32 devices in a mesh: parts: 2 (over y), row: 8 (over z, core), col: 2 (over x), sub: 1.
Axes of the slice: x: 2, y: 2, z: 4, core: 2. Of those that a mesh axis runs over, the one named last changes fastest.
Arguments:
- pair: float32 [192, 96, 128], P(('parts', 'row'), ('col', 'sub')), parts along dimension 0, may hold values from -250 to 250, as said below
- residue_mask: int32 [192], P('parts'), parts along dimension 0, may hold values from 0 to 1, as said below
- tri_norm_gain: float32 [128], replicated, may hold values from 0.25 to 1.75
- tri_in_weight: bfloat16 [128, 4, 128], replicated, may hold values from -0.5 to 0.5
- tri_gate_weight: bfloat16 [128, 128], replicated, may hold values from -0.5 to 0.5
- tri_out_norm_gain: float32 [128], replicated, may hold values from 0.25 to 1.75
- tri_out_weight: bfloat16 [128, 128], replicated, may hold values from -0.5 to 0.5
- att_norm_gain: float32 [128], replicated, may hold values from 0.25 to 1.75
- att_proj_weight: bfloat16 [128, 4, 128], replicated, may hold values from -0.5 to 0.5
- att_bias_weight: bfloat16 [128, 4], replicated, may hold values from -15 to 15
- att_out_weight: bfloat16 [128, 128], replicated, may hold values from -0.5 to 0.5
Outputs:
- pair_out: float32 [192, 96, 128], P(('parts', 'row'), ('col', 'sub')), parts along dimension 0
The draws below stay inside these ranges and needn't reach their ends.
There are 2 independent parts, one for each index of `parts`. The reference program is written for one: setup_inputs(seed, part) draws one part's arguments, and reference() takes and returns one part's arrays. A program takes and returns all parts, laid end to end along the dimension named above; an argument that names none is the same for every part. Nothing has to cross between parts.
Inputs may be any that keep to these rules, and one draw needn't show every extreme that they name: The pair entries are finite. `residue_mask`: 0 on every residue at or above a length of at least 48 and less than 96; below it 1, except some unresolved residues that are 0; residue 0 is always 1.
All inputs are finite; a program needn't handle non-finite values.
Results may differ from the reference program's by a relative error of at most 0.0032.
Values may be sent and summed in bfloat16 or wider, within the bound.
No kernel may reach another device: no remote copies, remote signals or barrier semaphores. Data moves between devices by JAX's collectives and lax.ppermute only.
A program may use at most 64 MiB of HBM per device.

```python
import math
import jax
import jax.numpy as jnp
from jax import lax

PAIR_CH = 128
TRI_HID = 128
HEADS = 4
HEAD_DIM = 32
RESIDUES = 96


def draw_pair(key, part):
    base_draw = jnp.clip(jax.random.normal(key, (RESIDUES, RESIDUES, PAIR_CH), jnp.float32), -6.0, 6.0)
    return base_draw


def draw_residue_mask(key, part):
    length = jax.random.randint(jax.random.fold_in(key, 7), (), RESIDUES // 2, RESIDUES)
    kept = jax.random.randint(jax.random.fold_in(key, 8), (RESIDUES,), 0, 8) != 0
    positions = jnp.arange(RESIDUES)
    live = (positions < length) & (kept | (positions == 0))
    return live.astype(jnp.int32)


def draw_att_bias_weight(key, part):
    base_draw = jnp.clip(jax.random.normal(key, (PAIR_CH, HEADS), jnp.float32), -4.0, 4.0)
    spread = 2.0
    return jnp.clip(base_draw * (spread / math.sqrt(PAIR_CH)), -15.0, 15.0).astype(jnp.bfloat16)


def gaussian(own_key, extent, scale, most, dtype=jnp.bfloat16):
    entries = jax.random.normal(own_key, extent, jnp.float32) * scale
    return jnp.minimum(jnp.maximum(entries, -most), most).astype(dtype)


def setup_inputs(seed: int = 0, part: int = 0) -> dict:
    streams_of = jax.random.split(jax.random.key(seed), 12)
    part_keys = jax.random.split(jax.random.fold_in(streams_of[11], part), 12)
    return {
        "pair": draw_pair(jax.random.fold_in(jax.random.fold_in(streams_of[11], part), 71), part),
        "residue_mask": draw_residue_mask(jax.random.fold_in(jax.random.fold_in(streams_of[11], part), 71), part),
        "tri_norm_gain": jnp.clip(1.0 + 0.15 * jax.random.normal(streams_of[2], (PAIR_CH,), jnp.float32), 0.25, 1.75),
        "tri_in_weight": gaussian(streams_of[3], (PAIR_CH, 4, TRI_HID), PAIR_CH ** -0.5, 0.5),
        "tri_gate_weight": gaussian(streams_of[4], (PAIR_CH, PAIR_CH), PAIR_CH ** -0.5, 0.5),
        "tri_out_norm_gain": jnp.clip(1.0 + 0.15 * jax.random.normal(streams_of[5], (TRI_HID,), jnp.float32), 0.25, 1.75),
        "tri_out_weight": gaussian(streams_of[6], (TRI_HID, PAIR_CH), TRI_HID ** -0.5, 0.5),
        "att_norm_gain": jnp.clip(1.0 + 0.15 * jax.random.normal(streams_of[7], (PAIR_CH,), jnp.float32), 0.25, 1.75),
        "att_proj_weight": gaussian(streams_of[8], (PAIR_CH, 4, HEADS * HEAD_DIM), PAIR_CH ** -0.5, 0.5),
        "att_bias_weight": draw_att_bias_weight(jax.random.fold_in(streams_of[11], 71), part),
        "att_out_weight": gaussian(streams_of[10], (HEADS * HEAD_DIM, PAIR_CH), (HEADS * HEAD_DIM) ** -0.5, 0.5),
    }


epsilon = 1e-05
mask_penalty = 1000000000.0

def norm_last(values_in, gain):
    center = lax.optimization_barrier(jnp.mean(values_in, axis=-1, keepdims=True))
    centered = values_in - center
    variance = lax.optimization_barrier(jnp.mean(centered * centered, axis=-1, keepdims=True))
    return centered * lax.rsqrt(variance + epsilon) * gain

def project(normed, weight):
    flat_rows = normed.reshape(-1, normed.shape[-1])
    product = jnp.dot(flat_rows, weight, preferred_element_type=jnp.float32)
    return product.reshape(normed.shape[:-1] + (weight.shape[1],))

def reference(pair, residue_mask, tri_norm_gain, tri_in_weight, tri_gate_weight, tri_out_norm_gain, tri_out_weight, att_norm_gain, att_proj_weight, att_bias_weight, att_out_weight):
    residue_live = residue_mask.astype(jnp.float32)
    pair_live = (residue_live[:, None] * residue_live[None, :])[:, :, None]
    tri_normed = norm_last(pair, tri_norm_gain).astype(jnp.bfloat16)
    left_factor = (jax.nn.sigmoid(project(tri_normed, tri_in_weight[:, 0])) * project(tri_normed, tri_in_weight[:, 1]) * pair_live).astype(jnp.bfloat16)
    right_factor = (jax.nn.sigmoid(project(tri_normed, tri_in_weight[:, 2])) * project(tri_normed, tri_in_weight[:, 3]) * pair_live).astype(jnp.bfloat16)
    tri_sum = jnp.einsum('ikh,jkh->ijh', left_factor.astype(jnp.float32), right_factor.astype(jnp.float32))
    hidden_normed = norm_last(tri_sum, tri_out_norm_gain).astype(jnp.bfloat16)
    tri_gate = jax.nn.sigmoid(project(tri_normed, tri_gate_weight))
    pair_mid = pair + tri_gate * project(hidden_normed, tri_out_weight)
    att_normed = norm_last(pair_mid, att_norm_gain).astype(jnp.bfloat16)
    head_shape = (RESIDUES, RESIDUES, HEADS, HEAD_DIM)
    queries = (project(att_normed, att_proj_weight[:, 0]) * HEAD_DIM ** (-0.5)).astype(jnp.bfloat16).reshape(head_shape)
    key_rows = project(att_normed, att_proj_weight[:, 1]).astype(jnp.bfloat16).reshape(head_shape)
    value_rows = project(att_normed, att_proj_weight[:, 2]).astype(jnp.bfloat16).reshape(head_shape)
    att_gate = jax.nn.sigmoid(project(att_normed, att_proj_weight[:, 3]))
    pair_bias = project(att_normed, att_bias_weight).astype(jnp.bfloat16)
    mask_row = (residue_live - 1.0) * mask_penalty
    head_bias = jnp.transpose(pair_bias.astype(jnp.float32), (2, 0, 1)) + mask_row[None, None, :]

    def one_row(row_item):
        query_row, key_row, value_row = row_item
        scores = jnp.einsum('jhd,khd->hjk', query_row.astype(jnp.float32), key_row.astype(jnp.float32)) + head_bias
        row_max = lax.optimization_barrier(jnp.max(scores, axis=-1, keepdims=True))
        raised = jnp.exp(scores - row_max)
        weights = (raised / lax.optimization_barrier(jnp.sum(raised, axis=-1, keepdims=True))).astype(jnp.bfloat16)
        return jnp.einsum('hjk,khd->jhd', weights.astype(jnp.float32), value_row.astype(jnp.float32))
    attended = lax.map(one_row, (queries, key_rows, value_rows))
    gated = (attended.reshape(RESIDUES, RESIDUES, HEADS * HEAD_DIM) * att_gate).astype(jnp.bfloat16)
    return pair_mid + project(gated, att_out_weight)
```

```python
import functools
import math

import jax
import jax.numpy as jnp
from jax import lax
from jax.experimental import pallas as pl
from jax.experimental.pallas import tpu as pltpu
from jax.sharding import PartitionSpec as P

epsilon = 1e-05
mask_penalty = 1000000000.0
LANES = 128
f32 = jnp.float32
bf16 = jnp.bfloat16


def norm_last(values_in, gain):
    center = jnp.mean(values_in, axis=-1, keepdims=True)
    centered = values_in - center
    variance = jnp.mean(centered * centered, axis=-1, keepdims=True)
    return centered * lax.rsqrt(variance + epsilon) * gain


def sigmoid(v):
    return 0.5 * jnp.tanh(0.5 * v) + 0.5


def project(normed, weight):
    flat_rows = normed.reshape(-1, normed.shape[-1])
    product = jnp.dot(flat_rows, weight, preferred_element_type=jnp.float32)
    return product.reshape(normed.shape[:-1] + (weight.shape[1],))


def body_general(
    pair,
    residue_mask,
    tri_norm_gain,
    tri_in_weight,
    tri_gate_weight,
    tri_out_norm_gain,
    tri_out_weight,
    att_norm_gain,
    att_proj_weight,
    att_bias_weight,
    att_out_weight,
):
    rows_here, cols_here, chan_here = pair.shape
    residues = cols_here * lax.axis_size(("col", "sub"))
    row_offset = lax.axis_index("row") * rows_here
    col_offset = lax.axis_index(("col", "sub")) * cols_here
    residue_live = residue_mask.astype(jnp.float32)
    live_rows = lax.dynamic_slice_in_dim(residue_live, row_offset, rows_here)
    live_cols = lax.dynamic_slice_in_dim(residue_live, col_offset, cols_here)
    pair_live = (live_rows[:, None] * live_cols[None, :])[:, :, None]
    tri_normed = norm_last(pair, tri_norm_gain).astype(jnp.bfloat16)
    in_width = tri_in_weight.shape[2]
    projected = project(tri_normed, tri_in_weight.reshape(tri_in_weight.shape[0], -1)).reshape(
        rows_here, cols_here, 4, in_width
    )
    left_factor = (jax.nn.sigmoid(projected[:, :, 0]) * projected[:, :, 1] * pair_live).astype(
        jnp.bfloat16
    )
    right_factor = (jax.nn.sigmoid(projected[:, :, 2]) * projected[:, :, 3] * pair_live).astype(
        jnp.bfloat16
    )
    left_all, right_all = (
        lax.all_gather(left_factor, ("col", "sub"), axis=1, tiled=True),
        lax.all_gather(right_factor, ("col", "sub"), axis=1, tiled=True),
    )
    exchanged = lax.all_to_all(right_all, "row", split_axis=1, concat_axis=0, tiled=True)
    own_rows = lax.dynamic_slice_in_dim(exchanged, col_offset, cols_here, 0)
    tri_sum = jnp.einsum(
        "ikh,jkh->ijh",
        left_all,
        lax.all_gather(own_rows, "row", axis=1, tiled=True),
        preferred_element_type=jnp.float32,
    )
    hidden_normed = norm_last(tri_sum, tri_out_norm_gain).astype(jnp.bfloat16)
    tri_gate = jax.nn.sigmoid(project(tri_normed, tri_gate_weight))
    pair_mid = pair + tri_gate * project(hidden_normed, tri_out_weight)
    att_normed = norm_last(pair_mid, att_norm_gain).astype(jnp.bfloat16)
    head_width = att_proj_weight.shape[2]
    heads_here = att_bias_weight.shape[1]
    head_size = head_width // heads_here
    projected = project(att_normed, att_proj_weight.reshape(att_proj_weight.shape[0], -1)).reshape(
        rows_here, cols_here, 4, head_width
    )
    queries = (projected[:, :, 0] * head_size ** (-0.5)).astype(jnp.bfloat16)
    key_rows = projected[:, :, 1].astype(jnp.bfloat16)
    value_rows = projected[:, :, 2].astype(jnp.bfloat16)
    att_gate = jax.nn.sigmoid(projected[:, :, 3])
    pair_bias = project(att_normed, att_bias_weight).astype(jnp.bfloat16)
    key_all, value_all = (
        lax.all_gather(key_rows, ("col", "sub"), axis=1, tiled=True),
        lax.all_gather(value_rows, ("col", "sub"), axis=1, tiled=True),
    )
    bias_all_rows = lax.all_gather(pair_bias, "row", axis=0, tiled=True)
    bias_panel = lax.all_to_all(
        bias_all_rows, ("col", "sub"), split_axis=0, concat_axis=1, tiled=True
    )
    mask_row = (residue_live - 1.0) * mask_penalty
    head_bias = jnp.transpose(bias_panel.astype(jnp.float32), (2, 0, 1)) + mask_row[None, None, :]
    block_rows = math.gcd(rows_here, max(1, 512 // cols_here))
    blocks = rows_here // block_rows

    def attend(block_items):
        query_block, key_block, value_block = block_items
        scores = (
            jnp.einsum(
                "ijhd,ikhd->ihjk", query_block, key_block, preferred_element_type=jnp.float32
            )
            + head_bias[None]
        )
        row_max = jnp.max(scores, axis=-1, keepdims=True)
        raised = jnp.exp(scores - row_max)
        weights = (raised / jnp.sum(raised, axis=-1, keepdims=True)).astype(jnp.bfloat16)
        return jnp.einsum(
            "ihjk,ikhd->ijhd", weights, value_block, preferred_element_type=jnp.float32
        )

    attended = lax.map(
        attend,
        (
            queries.reshape(blocks, block_rows, cols_here, heads_here, head_size),
            key_all.reshape(blocks, block_rows, residues, heads_here, head_size),
            value_all.reshape(blocks, block_rows, residues, heads_here, head_size),
        ),
    )
    gated = (attended.reshape(rows_here, cols_here, head_width) * att_gate).astype(jnp.bfloat16)
    return pair_mid + project(gated, att_out_weight)


def dot_nn(a, b):
    return lax.dot_general(a, b, (((1,), (0,)), ((), ())), preferred_element_type=f32)


def dot_nt(a, b):
    return lax.dot_general(a, b, (((1,), (1,)), ((), ())), preferred_element_type=f32)


def split_weight(w_ref, w_scratch):
    w_scratch[...] = w_ref[...].astype(f32)
    return [w_scratch[:, p, :] for p in range(w_ref.shape[1])]


def factors_kernel(devices, pair_ref, gain_ref, w_ref, lr_ref, normed_ref, w_scratch):
    cells, chan = pair_ref.shape
    hidden = w_ref.shape[2]
    own = hidden // devices
    normed = norm_last(pair_ref[...], gain_ref[...]).astype(bf16)
    normed_ref[...] = normed
    w_t = [jnp.transpose(w).astype(bf16) for w in split_weight(w_ref, w_scratch)]
    spare = (-cells) % LANES
    tiles = (cells + spare) // LANES
    if spare:
        tail = normed[:spare]
        rhs_left = jnp.concatenate([normed, tail], axis=0)
        rhs_right = jnp.concatenate([tail, normed], axis=0)
    else:
        rhs_left = rhs_right = normed
    left = sigmoid(dot_nt(w_t[0], rhs_left)) * dot_nt(w_t[1], rhs_left)
    right = sigmoid(dot_nt(w_t[2], rhs_right)) * dot_nt(w_t[3], rhs_right)
    panels = [left[:, t * LANES : (t + 1) * LANES] for t in range(tiles)]
    right_panels = [right[:, t * LANES : (t + 1) * LANES] for t in range(tiles)]
    if spare:
        lane = lax.broadcasted_iota(jnp.int32, (hidden, LANES), 1)
        panels[-1] = jnp.where(lane < LANES - spare, panels[-1], right_panels[0])
        panels += right_panels[1:]
    else:
        panels += right_panels
    for t, panel in enumerate(panels):
        lr_ref[:, t] = panel.reshape(devices, own, LANES).astype(bf16)


def segment(panels, start, target):
    tile, at = divmod(start, LANES)
    here = panels[tile]
    if at and tile + 1 < len(panels):
        lane = lax.broadcasted_iota(jnp.int32, here.shape, 1)
        here = jnp.where(lane >= at, here, panels[tile + 1])
    shift = (target - at) % LANES
    return pltpu.roll(here, shift, 1) if shift else here


def triangle_kernel(
    rows_here, cols_here, live_ref, lr_ref, sum_ref, left_scratch, right_scratch, sum_scratch
):
    devices, panels_in, own, _ = lr_ref.shape
    residues = live_ref.shape[1]
    cols = residues // cols_here
    rows = residues // rows_here
    cells = rows_here * cols_here
    lane = lax.broadcasted_iota(jnp.int32, (own, LANES), 1)
    for r in range(rows):
        parts = [
            [lr_ref[r * cols + c, t].astype(f32) for t in range(panels_in)] for c in range(cols)
        ]
        for side, scratch in ((0, left_scratch), (1, right_scratch)):
            for i in range(rows_here):
                start = side * cells + i * cols_here
                line = segment(parts[0], start, 0)
                for c in range(1, cols):
                    moved = segment(parts[c], start, c * cols_here)
                    line = jnp.where(lane < c * cols_here, line, moved)
                scratch[r * rows_here + i] = line
    live = live_ref[...].astype(f32)
    live_wide = jnp.concatenate([live, jnp.zeros((1, LANES - residues), f32)], axis=1)
    live_square = jnp.broadcast_to(live_wide, (LANES, LANES))
    both = live_square * jnp.transpose(live_square)
    both = both[:residues]
    keep = live_wide > 0
    for h in range(own):
        left = jnp.where(keep, left_scratch[:, h, :], 0.0).astype(bf16)
        right = jnp.where(keep, right_scratch[:, h, :], 0.0).astype(bf16)
        right = jnp.concatenate([right, jnp.zeros((LANES - residues, LANES), bf16)], axis=0)
        sum_scratch[:, h, :] = dot_nt(left, right) * both
    tiles = sum_ref.shape[1]
    for r in range(rows):
        lines = [sum_scratch[r * rows_here + i] for i in range(rows_here)]
        for c in range(cols):
            for t in range(tiles):
                panel = None
                for i in range(rows_here):
                    low, high = i * cols_here - t * LANES, (i + 1) * cols_here - t * LANES
                    if high <= 0 or low >= LANES:
                        continue
                    shift = (low - c * cols_here) % LANES
                    line = pltpu.roll(lines[i], shift, 1) if shift else lines[i]
                    panel = line if panel is None else jnp.where(lane >= low, line, panel)
                sum_ref[r * cols + c, t] = panel.astype(bf16)


def middle_kernel(
    pair_ref,
    normed_ref,
    sum_ref,
    out_gain_ref,
    out_w_ref,
    gate_w_ref,
    att_gain_ref,
    bias_w_ref,
    mid_ref,
    att_ref,
    bias_ref,
):
    devices, tiles, own, _ = sum_ref.shape
    cells, chan = pair_ref.shape
    hidden = devices * own
    gain_col = jnp.transpose(jnp.broadcast_to(out_gain_ref[...], (LANES, hidden)))
    gate = sigmoid(dot_nn(normed_ref[...], gate_w_ref[...]))
    bias_w = jnp.transpose(bias_w_ref[...].astype(f32)).astype(bf16)
    for t in range(tiles):
        total = sum_ref[:, t].astype(f32).reshape(hidden, LANES)
        center = jnp.mean(total, axis=0, keepdims=True)
        centered = total - center
        variance = jnp.mean(centered * centered, axis=0, keepdims=True)
        hidden_normed = centered * lax.rsqrt(variance + epsilon) * gain_col
        hidden_rows = jnp.transpose(hidden_normed).astype(bf16)
        low, high = t * LANES, min((t + 1) * LANES, cells)
        update = dot_nn(hidden_rows[: high - low], out_w_ref[...])
        mid = pair_ref[low:high] + gate[low:high] * update
        mid_ref[low:high] = mid
        att = norm_last(mid, att_gain_ref[...]).astype(bf16)
        att_ref[low:high] = att
        bias_ref[:, low:high] = dot_nt(bias_w, att).astype(bf16)


def attention_kernel(
    rows_here,
    place_ref,
    live_ref,
    bias_a_ref,
    bias_b_ref,
    att_ref,
    att_far_ref,
    mid_ref,
    proj_w_ref,
    out_w_ref,
    out_ref,
    w_scratch,
    bias_scratch,
):
    cells, chan = att_ref.shape
    cols_here = cells // rows_here
    blocks, heads, _ = bias_a_ref.shape
    residues = live_ref.shape[1]
    width = proj_w_ref.shape[2]
    size = width // heads
    block_at, col, same = place_ref[0], place_ref[1], place_ref[2]
    lane_row = lax.broadcasted_iota(jnp.int32, (1, LANES), 1)
    live = live_ref[...].astype(f32)
    live_wide = jnp.concatenate([live, jnp.zeros((1, LANES - residues), f32)], axis=1)
    swapped = jnp.where(
        lane_row < cols_here,
        pltpu.roll(live_wide, LANES - cols_here, 1),
        pltpu.roll(live_wide, cols_here, 1),
    )
    live_order = jnp.where(col == 0, live_wide, swapped)
    penalty = (live_order - 1.0) * mask_penalty
    lane = lax.broadcasted_iota(jnp.int32, (heads, LANES), 1)
    pad = (-cells) % LANES

    def panels(v):
        v = v.astype(f32)
        v = jnp.concatenate([v, jnp.zeros((heads, pad), f32)], axis=1) if pad else v
        return [v[:, t * LANES : (t + 1) * LANES] for t in range((cells + pad) // LANES)]

    for m in range(blocks):
        first, second = bias_a_ref[m].astype(f32), bias_b_ref[m].astype(f32)
        near = panels(jnp.where(same == 1, first, second))
        far = panels(jnp.where(same == 1, second, first))
        base = jnp.bitwise_xor(block_at, m) * rows_here
        for j in range(rows_here):
            line = jnp.where(
                lane < cols_here,
                segment(near, j * cols_here, 0),
                segment(far, j * cols_here, cols_here),
            )
            bias_scratch[base + j] = line
    penalty = penalty[:, :residues]
    head_bias = [bias_scratch[:, h, :][:, :residues] + penalty for h in range(heads)]
    head_bias = jnp.concatenate(head_bias, axis=0)

    w = [m.astype(bf16) for m in split_weight(proj_w_ref, w_scratch)]
    att, att_far = att_ref[...], att_far_ref[...]
    queries = (dot_nn(att, w[0]) * size ** (-0.5)).astype(bf16)
    keys = dot_nn(att, w[1]).astype(bf16)
    values = dot_nn(att, w[2]).astype(bf16)
    keys_far = dot_nn(att_far, w[1]).astype(bf16)
    values_far = dot_nn(att_far, w[2]).astype(bf16)
    gate = sigmoid(dot_nn(att, w[3]))
    head_of = lax.broadcasted_iota(jnp.int32, (cols_here, width), 1) // size
    for i in range(rows_here):
        at = slice(i * cols_here, (i + 1) * cols_here)
        q = queries[at]
        q_heads = jnp.concatenate(
            [jnp.where(head_of == h, q, jnp.zeros_like(q)) for h in range(heads)], axis=0
        )
        k = jnp.concatenate([keys[at], keys_far[at]], axis=0)
        v = jnp.concatenate([values[at], values_far[at]], axis=0)
        scores = dot_nt(q_heads, k) + head_bias
        raised = jnp.exp(scores - jnp.max(scores, axis=-1, keepdims=True))
        weights = (raised / jnp.sum(raised, axis=-1, keepdims=True)).astype(bf16)
        mixed = dot_nn(weights, v)
        attended = mixed[:cols_here]
        for h in range(1, heads):
            attended = jnp.where(head_of == h, mixed[h * cols_here : (h + 1) * cols_here], attended)
        gated = (attended * gate[at]).astype(bf16)
        out_ref[at] = mid_ref[at] + dot_nn(gated, out_w_ref[...])


def body_channels(
    pair,
    residue_mask,
    tri_norm_gain,
    tri_in_weight,
    tri_gate_weight,
    tri_out_norm_gain,
    tri_out_weight,
    att_norm_gain,
    att_proj_weight,
    att_bias_weight,
    att_out_weight,
):
    rows_here, cols_here, chan = pair.shape
    rows, cols = lax.axis_size("row"), lax.axis_size(("col", "sub"))
    group = ("row", "col", "sub")
    devices = rows * cols
    residues = cols_here * cols
    cells = rows_here * cols_here
    hidden = tri_in_weight.shape[2]
    own = hidden // devices
    heads = att_bias_weight.shape[1]
    blocks = rows // cols
    tiles = -(-cells // LANES)
    lr_panels = -(-2 * cells // LANES) if (-cells) % LANES * 2 == LANES else 2 * tiles
    flat = pair.reshape(cells, chan)
    live = residue_mask.reshape(1, residues)

    lr, normed = pl.pallas_call(
        functools.partial(factors_kernel, devices),
        out_shape=(
            jax.ShapeDtypeStruct((devices, lr_panels, own, LANES), bf16),
            jax.ShapeDtypeStruct((cells, chan), bf16),
        ),
        scratch_shapes=[pltpu.VMEM(tri_in_weight.shape, f32)],
        name="factors",
    )(flat, tri_norm_gain.reshape(1, chan), tri_in_weight)
    lr = lax.all_to_all(lr, group, 0, 0, tiled=True)
    sums = pl.pallas_call(
        functools.partial(triangle_kernel, rows_here, cols_here),
        out_shape=jax.ShapeDtypeStruct((devices, tiles, own, LANES), bf16),
        scratch_shapes=[pltpu.VMEM((residues, own, LANES), f32) for _ in range(3)],
        name="triangle",
    )(live, lr)
    sums = lax.all_to_all(sums, group, 0, 0, tiled=True)
    mid, att, bias = pl.pallas_call(
        middle_kernel,
        out_shape=(
            jax.ShapeDtypeStruct((cells, chan), f32),
            jax.ShapeDtypeStruct((cells, chan), bf16),
            jax.ShapeDtypeStruct((heads, cells), bf16),
        ),
        name="middle",
    )(
        flat,
        normed,
        sums,
        tri_out_norm_gain.reshape(1, hidden),
        tri_out_weight,
        tri_gate_weight,
        att_norm_gain.reshape(1, chan),
        att_bias_weight,
    )
    att_far = lax.ppermute(att, ("col", "sub"), [(c, c ^ 1) for c in range(cols)])
    held = bias[None]
    step = 1
    while step < blocks:
        other = lax.ppermute(held, "row", [(r, r ^ step) for r in range(rows)])
        held = jnp.concatenate([held, other], axis=0)
        step *= 2
    spread = []
    for shift in range(cols):
        pairs = []
        for part in range(cols):
            for q in range(blocks):
                for c in range(cols):
                    source = (c * blocks + q) * cols + (part + shift) % cols
                    pairs.append((source, (part * blocks + q) * cols + c))
        spread.append(lax.ppermute(held, group, pairs))
    row, col = lax.axis_index("row"), lax.axis_index(("col", "sub"))
    place = jnp.stack([row % blocks, col, (row // blocks == col).astype(jnp.int32)])
    out = pl.pallas_call(
        functools.partial(attention_kernel, rows_here),
        out_shape=jax.ShapeDtypeStruct((cells, chan), f32),
        in_specs=[pl.BlockSpec(memory_space=pltpu.SMEM)]
        + [pl.BlockSpec(memory_space=pltpu.VMEM)] * 8,
        scratch_shapes=[
            pltpu.VMEM(att_proj_weight.shape, f32),
            pltpu.VMEM((cols_here, heads, LANES), f32),
        ],
        name="attention",
    )(place, live, *spread, att, att_far, mid, att_proj_weight, att_out_weight)
    return out.reshape(pair.shape)


def solution(mesh):
    placed = (
        P(("parts", "row"), ("col", "sub"), None),
        P("parts"),
        P(),
        P(),
        P(),
        P(),
        P(),
        P(),
        P(),
        P(),
        P(),
    )

    def body(pair, residue_mask, tri_norm_gain, tri_in_weight, *others):
        rows, cols = mesh.shape["row"], mesh.shape["col"] * mesh.shape["sub"]
        hidden = tri_in_weight.shape[2]
        fits = (
            cols == 2
            and rows % cols == 0
            and (rows // cols) & (rows // cols - 1) == 0
            and hidden % (8 * rows * cols) == 0
            and hidden == pair.shape[2] == LANES
            and residue_mask.shape[0] <= LANES
            and pair.shape[0] * cols * pair.shape[1] % 16 == 0
        )
        chosen = body_channels if fits else body_general
        return chosen(pair, residue_mask, tri_norm_gain, tri_in_weight, *others)

    return jax.shard_map(
        body,
        mesh=mesh,
        in_specs=placed,
        out_specs=P(("parts", "row"), ("col", "sub"), None),
        check_vma=False,
    )
```

```python
import functools
import math

import jax
import jax.numpy as jnp
from jax import lax
from jax.experimental import pallas as pl
from jax.experimental.pallas import tpu as pltpu
from jax.sharding import PartitionSpec as P

epsilon = 1e-05
mask_penalty = 1000000000.0
LANES = 128
f32 = jnp.float32
bf16 = jnp.bfloat16


def norm_last(values_in, gain):
    center = jnp.mean(values_in, axis=-1, keepdims=True)
    centered = values_in - center
    variance = jnp.mean(centered * centered, axis=-1, keepdims=True)
    return centered * lax.rsqrt(variance + epsilon) * gain


def sigmoid(v):
    return 0.5 * jnp.tanh(0.5 * v) + 0.5


def project(normed, weight):
    flat_rows = normed.reshape(-1, normed.shape[-1])
    product = jnp.dot(flat_rows, weight, preferred_element_type=jnp.float32)
    return product.reshape(normed.shape[:-1] + (weight.shape[1],))


def body_general(
    pair,
    residue_mask,
    tri_norm_gain,
    tri_in_weight,
    tri_gate_weight,
    tri_out_norm_gain,
    tri_out_weight,
    att_norm_gain,
    att_proj_weight,
    att_bias_weight,
    att_out_weight,
):
    rows_here, cols_here, chan_here = pair.shape
    residues = cols_here * lax.axis_size(("col", "sub"))
    row_offset = lax.axis_index("row") * rows_here
    col_offset = lax.axis_index(("col", "sub")) * cols_here
    residue_live = residue_mask.astype(jnp.float32)
    live_rows = lax.dynamic_slice_in_dim(residue_live, row_offset, rows_here)
    live_cols = lax.dynamic_slice_in_dim(residue_live, col_offset, cols_here)
    pair_live = (live_rows[:, None] * live_cols[None, :])[:, :, None]
    tri_normed = norm_last(pair, tri_norm_gain).astype(jnp.bfloat16)
    in_width = tri_in_weight.shape[2]
    projected = project(tri_normed, tri_in_weight.reshape(tri_in_weight.shape[0], -1)).reshape(
        rows_here, cols_here, 4, in_width
    )
    left_factor = (jax.nn.sigmoid(projected[:, :, 0]) * projected[:, :, 1] * pair_live).astype(
        jnp.bfloat16
    )
    right_factor = (jax.nn.sigmoid(projected[:, :, 2]) * projected[:, :, 3] * pair_live).astype(
        jnp.bfloat16
    )
    left_all, right_all = (
        lax.all_gather(left_factor, ("col", "sub"), axis=1, tiled=True),
        lax.all_gather(right_factor, ("col", "sub"), axis=1, tiled=True),
    )
    exchanged = lax.all_to_all(right_all, "row", split_axis=1, concat_axis=0, tiled=True)
    own_rows = lax.dynamic_slice_in_dim(exchanged, col_offset, cols_here, 0)
    tri_sum = jnp.einsum(
        "ikh,jkh->ijh",
        left_all,
        lax.all_gather(own_rows, "row", axis=1, tiled=True),
        preferred_element_type=jnp.float32,
    )
    hidden_normed = norm_last(tri_sum, tri_out_norm_gain).astype(jnp.bfloat16)
    tri_gate = jax.nn.sigmoid(project(tri_normed, tri_gate_weight))
    pair_mid = pair + tri_gate * project(hidden_normed, tri_out_weight)
    att_normed = norm_last(pair_mid, att_norm_gain).astype(jnp.bfloat16)
    head_width = att_proj_weight.shape[2]
    heads_here = att_bias_weight.shape[1]
    head_size = head_width // heads_here
    projected = project(att_normed, att_proj_weight.reshape(att_proj_weight.shape[0], -1)).reshape(
        rows_here, cols_here, 4, head_width
    )
    queries = (projected[:, :, 0] * head_size ** (-0.5)).astype(jnp.bfloat16)
    key_rows = projected[:, :, 1].astype(jnp.bfloat16)
    value_rows = projected[:, :, 2].astype(jnp.bfloat16)
    att_gate = jax.nn.sigmoid(projected[:, :, 3])
    pair_bias = project(att_normed, att_bias_weight).astype(jnp.bfloat16)
    key_all, value_all = (
        lax.all_gather(key_rows, ("col", "sub"), axis=1, tiled=True),
        lax.all_gather(value_rows, ("col", "sub"), axis=1, tiled=True),
    )
    bias_all_rows = lax.all_gather(pair_bias, "row", axis=0, tiled=True)
    bias_panel = lax.all_to_all(
        bias_all_rows, ("col", "sub"), split_axis=0, concat_axis=1, tiled=True
    )
    mask_row = (residue_live - 1.0) * mask_penalty
    head_bias = jnp.transpose(bias_panel.astype(jnp.float32), (2, 0, 1)) + mask_row[None, None, :]
    block_rows = math.gcd(rows_here, max(1, 512 // cols_here))
    blocks = rows_here // block_rows

    def attend(block_items):
        query_block, key_block, value_block = block_items
        scores = (
            jnp.einsum(
                "ijhd,ikhd->ihjk", query_block, key_block, preferred_element_type=jnp.float32
            )
            + head_bias[None]
        )
        row_max = jnp.max(scores, axis=-1, keepdims=True)
        raised = jnp.exp(scores - row_max)
        weights = (raised / jnp.sum(raised, axis=-1, keepdims=True)).astype(jnp.bfloat16)
        return jnp.einsum(
            "ihjk,ikhd->ijhd", weights, value_block, preferred_element_type=jnp.float32
        )

    attended = lax.map(
        attend,
        (
            queries.reshape(blocks, block_rows, cols_here, heads_here, head_size),
            key_all.reshape(blocks, block_rows, residues, heads_here, head_size),
            value_all.reshape(blocks, block_rows, residues, heads_here, head_size),
        ),
    )
    gated = (attended.reshape(rows_here, cols_here, head_width) * att_gate).astype(jnp.bfloat16)
    return pair_mid + project(gated, att_out_weight)


def dot_nn(a, b):
    return lax.dot_general(a, b, (((1,), (0,)), ((), ())), preferred_element_type=f32)


def dot_nt(a, b):
    return lax.dot_general(a, b, (((1,), (1,)), ((), ())), preferred_element_type=f32)


def near(v):
    return pltpu.with_memory_space_constraint(v, pltpu.VMEM)


def split_weight(w_ref, w_scratch):
    w_scratch[...] = w_ref[...].astype(f32)
    return [w_scratch[:, p, :] for p in range(w_ref.shape[1])]


def factors_kernel(
    devices,
    pair_ref,
    gain_ref,
    w_ref,
    live_ref,
    out_gain_ref,
    att_gain_ref,
    lr_ref,
    normed_ref,
    rows_ref,
    w_scratch,
):
    cells, chan = pair_ref.shape
    live = live_ref[...].astype(f32)
    rows_ref[0:1] = jnp.concatenate([live, jnp.zeros((1, LANES - live.shape[1]), f32)], axis=1)
    rows_ref[1:2] = out_gain_ref[...]
    rows_ref[2:3] = att_gain_ref[...]
    hidden = w_ref.shape[2]
    own = hidden // devices
    normed = norm_last(pair_ref[...], gain_ref[...]).astype(bf16)
    normed_ref[...] = normed
    w_t = [jnp.transpose(w).astype(bf16) for w in split_weight(w_ref, w_scratch)]
    spare = (-cells) % LANES
    tiles = (cells + spare) // LANES
    if spare:
        tail = normed[:spare]
        rhs_left = jnp.concatenate([normed, tail], axis=0)
        rhs_right = jnp.concatenate([tail, normed], axis=0)
    else:
        rhs_left = rhs_right = normed
    left = sigmoid(dot_nt(w_t[0], rhs_left)) * dot_nt(w_t[1], rhs_left)
    right = sigmoid(dot_nt(w_t[2], rhs_right)) * dot_nt(w_t[3], rhs_right)
    panels = [left[:, t * LANES : (t + 1) * LANES] for t in range(tiles)]
    right_panels = [right[:, t * LANES : (t + 1) * LANES] for t in range(tiles)]
    if spare:
        lane = lax.broadcasted_iota(jnp.int32, (hidden, LANES), 1)
        panels[-1] = jnp.where(lane < LANES - spare, panels[-1], right_panels[0])
        panels += right_panels[1:]
    else:
        panels += right_panels
    for t, panel in enumerate(panels):
        lr_ref[:, t] = panel.reshape(devices, own, LANES).astype(bf16)


def segment(panels, start, target):
    tile, at = divmod(start, LANES)
    here = panels[tile]
    if at and tile + 1 < len(panels):
        lane = lax.broadcasted_iota(jnp.int32, here.shape, 1)
        here = jnp.where(lane >= at, here, panels[tile + 1])
    shift = (target - at) % LANES
    return pltpu.roll(here, shift, 1) if shift else here


def triangle_kernel(
    rows_here, cols_here, vectors_ref, lr_ref, sum_ref, left_scratch, right_scratch, sum_scratch
):
    devices, panels_in, own, _ = lr_ref.shape
    residues = left_scratch.shape[0]
    cols = residues // cols_here
    rows = residues // rows_here
    cells = rows_here * cols_here
    lane = lax.broadcasted_iota(jnp.int32, (own, LANES), 1)
    for r in range(rows):
        parts = [
            [lr_ref[r * cols + c, t].astype(f32) for t in range(panels_in)] for c in range(cols)
        ]
        for side, scratch in ((0, left_scratch), (1, right_scratch)):
            for i in range(rows_here):
                start = side * cells + i * cols_here
                line = segment(parts[0], start, 0)
                for c in range(1, cols):
                    moved = segment(parts[c], start, c * cols_here)
                    line = jnp.where(lane < c * cols_here, line, moved)
                scratch[r * rows_here + i] = line
    live_wide = vectors_ref[0:1]
    live_square = jnp.broadcast_to(live_wide, (LANES, LANES))
    both = live_square * jnp.transpose(live_square)
    both = both[:residues]
    keep = live_wide > 0
    for h in range(own):
        left = jnp.where(keep, left_scratch[:, h, :], 0.0).astype(bf16)
        right = jnp.where(keep, right_scratch[:, h, :], 0.0).astype(bf16)
        right = jnp.concatenate([right, jnp.zeros((LANES - residues, LANES), bf16)], axis=0)
        sum_scratch[:, h, :] = dot_nt(left, right) * both
    tiles = sum_ref.shape[1]
    for r in range(rows):
        lines = [sum_scratch[r * rows_here + i] for i in range(rows_here)]
        for c in range(cols):
            for t in range(tiles):
                panel = None
                for i in range(rows_here):
                    low, high = i * cols_here - t * LANES, (i + 1) * cols_here - t * LANES
                    if high <= 0 or low >= LANES:
                        continue
                    shift = (low - c * cols_here) % LANES
                    line = pltpu.roll(lines[i], shift, 1) if shift else lines[i]
                    panel = line if panel is None else jnp.where(lane >= low, line, panel)
                sum_ref[r * cols + c, t] = panel.astype(bf16)


def middle_kernel(
    pair_ref,
    normed_ref,
    sum_ref,
    vectors_ref,
    out_w_ref,
    gate_w_ref,
    bias_w_ref,
    mid_ref,
    att_ref,
    bias_ref,
):
    devices, tiles, own, _ = sum_ref.shape
    cells, chan = pair_ref.shape
    hidden = devices * own
    gain_col = jnp.transpose(jnp.broadcast_to(vectors_ref[1:2], (LANES, hidden)))
    gate = sigmoid(dot_nn(normed_ref[...], gate_w_ref[...]))
    bias_w = jnp.transpose(bias_w_ref[...].astype(f32)).astype(bf16)
    for t in range(tiles):
        total = sum_ref[:, t].astype(f32).reshape(hidden, LANES)
        center = jnp.mean(total, axis=0, keepdims=True)
        centered = total - center
        variance = jnp.mean(centered * centered, axis=0, keepdims=True)
        hidden_normed = centered * lax.rsqrt(variance + epsilon) * gain_col
        hidden_rows = jnp.transpose(hidden_normed).astype(bf16)
        low, high = t * LANES, min((t + 1) * LANES, cells)
        update = dot_nn(hidden_rows[: high - low], out_w_ref[...])
        mid = pair_ref[low:high] + gate[low:high] * update
        mid_ref[low:high] = mid
        att = norm_last(mid, vectors_ref[2:3]).astype(bf16)
        att_ref[low:high] = att
        bias_ref[:, low:high] = dot_nt(bias_w, att).astype(bf16)


def attention_kernel(
    rows_here,
    vectors_ref,
    bias_a_ref,
    bias_b_ref,
    att_ref,
    att_far_ref,
    mid_ref,
    proj_w_ref,
    out_w_ref,
    out_ref,
    w_scratch,
    bias_scratch,
):
    cells, chan = att_ref.shape
    cols_here = cells // rows_here
    blocks, heads, _ = bias_a_ref.shape
    residues = 2 * cols_here
    width = proj_w_ref.shape[2]
    size = width // heads
    row, col = lax.axis_index("row"), lax.axis_index(("col", "sub"))
    block_at = lax.rem(row, blocks)
    same = (lax.div(row, blocks) == col).astype(jnp.int32)
    lane_row = lax.broadcasted_iota(jnp.int32, (1, LANES), 1)
    live_wide = vectors_ref[0:1]
    swapped = jnp.where(
        lane_row < cols_here,
        pltpu.roll(live_wide, LANES - cols_here, 1),
        pltpu.roll(live_wide, cols_here, 1),
    )
    live_order = jnp.where(col == 0, live_wide, swapped)
    penalty = (live_order - 1.0) * mask_penalty
    lane = lax.broadcasted_iota(jnp.int32, (heads, LANES), 1)
    pad = (-cells) % LANES

    def panels(v):
        v = v.astype(f32)
        v = jnp.concatenate([v, jnp.zeros((heads, pad), f32)], axis=1) if pad else v
        return [v[:, t * LANES : (t + 1) * LANES] for t in range((cells + pad) // LANES)]

    for m in range(blocks):
        first, second = bias_a_ref[m].astype(f32), bias_b_ref[m].astype(f32)
        mine = panels(jnp.where(same == 1, first, second))
        far = panels(jnp.where(same == 1, second, first))
        base = jnp.bitwise_xor(block_at, m) * rows_here
        for j in range(rows_here):
            line = jnp.where(
                lane < cols_here,
                segment(mine, j * cols_here, 0),
                segment(far, j * cols_here, cols_here),
            )
            bias_scratch[base + j] = line
    penalty = penalty[:, :residues]
    head_bias = [bias_scratch[:, h, :][:, :residues] + penalty for h in range(heads)]
    head_bias = jnp.concatenate(head_bias, axis=0)

    w = [m.astype(bf16) for m in split_weight(proj_w_ref, w_scratch)]
    att, att_far = att_ref[...], att_far_ref[...]
    queries = (dot_nn(att, w[0]) * size ** (-0.5)).astype(bf16)
    keys = dot_nn(att, w[1]).astype(bf16)
    values = dot_nn(att, w[2]).astype(bf16)
    keys_far = dot_nn(att_far, w[1]).astype(bf16)
    values_far = dot_nn(att_far, w[2]).astype(bf16)
    gate = sigmoid(dot_nn(att, w[3]))
    head_of = lax.broadcasted_iota(jnp.int32, (cols_here, width), 1) // size
    for i in range(rows_here):
        at = slice(i * cols_here, (i + 1) * cols_here)
        q = queries[at]
        q_heads = jnp.concatenate(
            [jnp.where(head_of == h, q, jnp.zeros_like(q)) for h in range(heads)], axis=0
        )
        k = jnp.concatenate([keys[at], keys_far[at]], axis=0)
        v = jnp.concatenate([values[at], values_far[at]], axis=0)
        scores = dot_nt(q_heads, k) + head_bias
        raised = jnp.exp(scores - jnp.max(scores, axis=-1, keepdims=True))
        weights = (raised / jnp.sum(raised, axis=-1, keepdims=True)).astype(bf16)
        mixed = dot_nn(weights, v)
        attended = mixed[:cols_here]
        for h in range(1, heads):
            attended = jnp.where(head_of == h, mixed[h * cols_here : (h + 1) * cols_here], attended)
        gated = (attended * gate[at]).astype(bf16)
        out_ref[at] = mid_ref[at] + dot_nn(gated, out_w_ref[...])


def body_channels(
    pair,
    residue_mask,
    tri_norm_gain,
    tri_in_weight,
    tri_gate_weight,
    tri_out_norm_gain,
    tri_out_weight,
    att_norm_gain,
    att_proj_weight,
    att_bias_weight,
    att_out_weight,
):
    rows_here, cols_here, chan = pair.shape
    rows, cols = lax.axis_size("row"), lax.axis_size(("col", "sub"))
    group = ("row", "col", "sub")
    devices = rows * cols
    residues = cols_here * cols
    cells = rows_here * cols_here
    hidden = tri_in_weight.shape[2]
    own = hidden // devices
    heads = att_bias_weight.shape[1]
    blocks = rows // cols
    tiles = -(-cells // LANES)
    lr_panels = -(-2 * cells // LANES) if (-cells) % LANES * 2 == LANES else 2 * tiles
    flat = pair.reshape(cells, chan)
    live = residue_mask.reshape(1, residues)

    lr, normed, vectors = pl.pallas_call(
        functools.partial(factors_kernel, devices),
        out_shape=(
            pltpu.VMEM((devices, lr_panels, own, LANES), bf16),
            pltpu.VMEM((cells, chan), bf16),
            pltpu.VMEM((8, LANES), f32),
        ),
        scratch_shapes=[pltpu.VMEM(tri_in_weight.shape, f32)],
        name="factors",
    )(
        flat,
        tri_norm_gain.reshape(1, chan),
        tri_in_weight,
        live,
        tri_out_norm_gain.reshape(1, hidden),
        att_norm_gain.reshape(1, chan),
    )
    lr = lax.all_to_all(lr, group, 0, 0, tiled=True)
    sums = pl.pallas_call(
        functools.partial(triangle_kernel, rows_here, cols_here),
        out_shape=pltpu.VMEM((devices, tiles, own, LANES), bf16),
        scratch_shapes=[pltpu.VMEM((residues, own, LANES), f32) for _ in range(3)],
        name="triangle",
    )(near(vectors), near(lr))
    sums = lax.all_to_all(sums, group, 0, 0, tiled=True)
    mid, att, bias = pl.pallas_call(
        middle_kernel,
        out_shape=(
            pltpu.VMEM((cells, chan), f32),
            pltpu.VMEM((cells, chan), bf16),
            pltpu.VMEM((heads, cells), bf16),
        ),
        name="middle",
    )(
        *map(
            near,
            (
                flat,
                normed,
                sums,
                vectors,
                tri_out_weight,
                tri_gate_weight,
                att_bias_weight,
            ),
        )
    )
    att_far = lax.ppermute(att, ("col", "sub"), [(c, c ^ 1) for c in range(cols)])
    held = bias[None]
    step = 1
    while step < blocks:
        other = lax.ppermute(held, "row", [(r, r ^ step) for r in range(rows)])
        held = jnp.concatenate([held, other], axis=0)
        step *= 2
    spread = []
    for shift in range(cols):
        pairs = []
        for part in range(cols):
            for q in range(blocks):
                for c in range(cols):
                    source = (c * blocks + q) * cols + (part + shift) % cols
                    pairs.append((source, (part * blocks + q) * cols + c))
        spread.append(lax.ppermute(held, group, pairs))
    out = pl.pallas_call(
        functools.partial(attention_kernel, rows_here),
        out_shape=jax.ShapeDtypeStruct((cells, chan), f32),
        scratch_shapes=[
            pltpu.VMEM(att_proj_weight.shape, f32),
            pltpu.VMEM((cols_here, heads, LANES), f32),
        ],
        name="attention",
    )(*map(near, (vectors, *spread, att, att_far, mid, att_proj_weight, att_out_weight)))
    return out.reshape(pair.shape)


def solution(mesh):
    placed = (
        P(("parts", "row"), ("col", "sub"), None),
        P("parts"),
        P(),
        P(),
        P(),
        P(),
        P(),
        P(),
        P(),
        P(),
        P(),
    )

    def body(pair, residue_mask, tri_norm_gain, tri_in_weight, *others):
        rows, cols = mesh.shape["row"], mesh.shape["col"] * mesh.shape["sub"]
        hidden = tri_in_weight.shape[2]
        fits = (
            cols == 2
            and rows % cols == 0
            and (rows // cols) & (rows // cols - 1) == 0
            and hidden % (8 * rows * cols) == 0
            and hidden == pair.shape[2] == LANES
            and residue_mask.shape[0] <= LANES
            and pair.shape[0] * cols * pair.shape[1] % 16 == 0
        )
        chosen = body_channels if fits else body_general
        return chosen(pair, residue_mask, tri_norm_gain, tri_in_weight, *others)

    return jax.shard_map(
        body,
        mesh=mesh,
        in_specs=placed,
        out_specs=P(("parts", "row"), ("col", "sub"), None),
        check_vma=False,
    )
```

```python
import functools
import math

import jax
import jax.numpy as jnp
from jax import lax
from jax.experimental import pallas as pl
from jax.experimental.pallas import tpu as pltpu
from jax.sharding import PartitionSpec as P


epsilon = 1e-05
mask_penalty = 1000000000.0
LANES = 128
f32 = jnp.float32
bf16 = jnp.bfloat16


def norm_last(values_in, gain):
    center = jnp.mean(values_in, axis=-1, keepdims=True)
    centered = values_in - center
    variance = jnp.mean(centered * centered, axis=-1, keepdims=True)
    return centered * lax.rsqrt(variance + epsilon) * gain


def sigmoid(v):
    return 0.5 * jnp.tanh(0.5 * v) + 0.5


def project(normed, weight):
    flat_rows = normed.reshape(-1, normed.shape[-1])
    product = jnp.dot(flat_rows, weight, preferred_element_type=jnp.float32)
    return product.reshape(normed.shape[:-1] + (weight.shape[1],))


def body_general(
    pair,
    residue_mask,
    tri_norm_gain,
    tri_in_weight,
    tri_gate_weight,
    tri_out_norm_gain,
    tri_out_weight,
    att_norm_gain,
    att_proj_weight,
    att_bias_weight,
    att_out_weight,
):
    rows_here, cols_here, _ = pair.shape
    residues = cols_here * lax.axis_size(("col", "sub"))
    row_offset = lax.axis_index("row") * rows_here
    col_offset = lax.axis_index(("col", "sub")) * cols_here
    residue_live = residue_mask.astype(jnp.float32)
    live_rows = lax.dynamic_slice_in_dim(residue_live, row_offset, rows_here)
    live_cols = lax.dynamic_slice_in_dim(residue_live, col_offset, cols_here)
    pair_live = (live_rows[:, None] * live_cols[None, :])[:, :, None]
    tri_normed = norm_last(pair, tri_norm_gain).astype(jnp.bfloat16)
    in_width = tri_in_weight.shape[2]
    projected = project(tri_normed, tri_in_weight.reshape(tri_in_weight.shape[0], -1)).reshape(
        rows_here, cols_here, 4, in_width
    )
    left_factor = (jax.nn.sigmoid(projected[:, :, 0]) * projected[:, :, 1] * pair_live).astype(
        jnp.bfloat16
    )
    right_factor = (jax.nn.sigmoid(projected[:, :, 2]) * projected[:, :, 3] * pair_live).astype(
        jnp.bfloat16
    )
    left_all, right_all = (
        lax.all_gather(left_factor, ("col", "sub"), axis=1, tiled=True),
        lax.all_gather(right_factor, ("col", "sub"), axis=1, tiled=True),
    )
    exchanged = lax.all_to_all(right_all, "row", split_axis=1, concat_axis=0, tiled=True)
    own_rows = lax.dynamic_slice_in_dim(exchanged, col_offset, cols_here, 0)
    tri_sum = jnp.einsum(
        "ikh,jkh->ijh",
        left_all,
        lax.all_gather(own_rows, "row", axis=1, tiled=True),
        preferred_element_type=jnp.float32,
    )
    hidden_normed = norm_last(tri_sum, tri_out_norm_gain).astype(jnp.bfloat16)
    tri_gate = jax.nn.sigmoid(project(tri_normed, tri_gate_weight))
    pair_mid = pair + tri_gate * project(hidden_normed, tri_out_weight)
    att_normed = norm_last(pair_mid, att_norm_gain).astype(jnp.bfloat16)
    head_width = att_proj_weight.shape[2]
    heads_here = att_bias_weight.shape[1]
    head_size = head_width // heads_here
    projected = project(att_normed, att_proj_weight.reshape(att_proj_weight.shape[0], -1)).reshape(
        rows_here, cols_here, 4, head_width
    )
    queries = (projected[:, :, 0] * head_size ** (-0.5)).astype(jnp.bfloat16)
    key_rows = projected[:, :, 1].astype(jnp.bfloat16)
    value_rows = projected[:, :, 2].astype(jnp.bfloat16)
    att_gate = jax.nn.sigmoid(projected[:, :, 3])
    pair_bias = project(att_normed, att_bias_weight).astype(jnp.bfloat16)
    key_all, value_all = (
        lax.all_gather(key_rows, ("col", "sub"), axis=1, tiled=True),
        lax.all_gather(value_rows, ("col", "sub"), axis=1, tiled=True),
    )
    bias_all_rows = lax.all_gather(pair_bias, "row", axis=0, tiled=True)
    bias_panel = lax.all_to_all(
        bias_all_rows, ("col", "sub"), split_axis=0, concat_axis=1, tiled=True
    )
    mask_row = (residue_live - 1.0) * mask_penalty
    head_bias = jnp.transpose(bias_panel.astype(jnp.float32), (2, 0, 1)) + mask_row[None, None, :]
    block_rows = math.gcd(rows_here, max(1, 512 // cols_here))
    blocks = rows_here // block_rows

    def attend(block_items):
        query_block, key_block, value_block = block_items
        scores = (
            jnp.einsum(
                "ijhd,ikhd->ihjk", query_block, key_block, preferred_element_type=jnp.float32
            )
            + head_bias[None]
        )
        row_max = jnp.max(scores, axis=-1, keepdims=True)
        raised = jnp.exp(scores - row_max)
        weights = (raised / jnp.sum(raised, axis=-1, keepdims=True)).astype(jnp.bfloat16)
        return jnp.einsum(
            "ihjk,ikhd->ijhd", weights, value_block, preferred_element_type=jnp.float32
        )

    attended = lax.map(
        attend,
        (
            queries.reshape(blocks, block_rows, cols_here, heads_here, head_size),
            key_all.reshape(blocks, block_rows, residues, heads_here, head_size),
            value_all.reshape(blocks, block_rows, residues, heads_here, head_size),
        ),
    )
    gated = (attended.reshape(rows_here, cols_here, head_width) * att_gate).astype(jnp.bfloat16)
    return pair_mid + project(gated, att_out_weight)


def dot_nn(a, b):
    return lax.dot_general(a, b, (((1,), (0,)), ((), ())), preferred_element_type=f32)


def dot_nt(a, b):
    return lax.dot_general(a, b, (((1,), (1,)), ((), ())), preferred_element_type=f32)


kernel_params = pltpu.CompilerParams(vmem_limit_bytes=16 << 20)


def near(v):
    return pltpu.with_memory_space_constraint(v, pltpu.VMEM)


def afar(v):
    return pltpu.with_memory_space_constraint(v, pltpu.HBM)


def split_weight(w_ref, w_scratch):
    w_scratch[...] = w_ref[...].astype(f32)
    return [w_scratch[:, p, :] for p in range(w_ref.shape[1])]


def factors_kernel(
    devices,
    pair_ref,
    gain_ref,
    w_ref,
    live_ref,
    out_gain_ref,
    att_gain_ref,
    lr_ref,
    normed_ref,
    rows_ref,
    w_scratch,
):
    cells, _ = pair_ref.shape
    live = live_ref[...].astype(f32)
    rows_ref[0:1] = jnp.concatenate([live, jnp.zeros((1, LANES - live.shape[1]), f32)], axis=1)
    rows_ref[1:2] = out_gain_ref[...]
    rows_ref[2:3] = att_gain_ref[...]
    hidden = w_ref.shape[2]
    own = hidden // devices
    normed = norm_last(pair_ref[...], gain_ref[...]).astype(bf16)
    normed_ref[...] = normed
    w_t = [jnp.transpose(w).astype(bf16) for w in split_weight(w_ref, w_scratch)]
    spare = (-cells) % LANES
    tiles = (cells + spare) // LANES
    if spare:
        tail = normed[:spare]
        rhs_left = jnp.concatenate([normed, tail], axis=0)
        rhs_right = jnp.concatenate([tail, normed], axis=0)
    else:
        rhs_left = rhs_right = normed
    left = sigmoid(dot_nt(w_t[0], rhs_left)) * dot_nt(w_t[1], rhs_left)
    right = sigmoid(dot_nt(w_t[2], rhs_right)) * dot_nt(w_t[3], rhs_right)
    panels = [left[:, t * LANES : (t + 1) * LANES] for t in range(tiles)]
    right_panels = [right[:, t * LANES : (t + 1) * LANES] for t in range(tiles)]
    if spare:
        lane = lax.broadcasted_iota(jnp.int32, (hidden, LANES), 1)
        panels[-1] = jnp.where(lane < LANES - spare, panels[-1], right_panels[0])
        panels += right_panels[1:]
    else:
        panels += right_panels
    for t, panel in enumerate(panels):
        lr_ref[:, t] = panel.reshape(devices, own, LANES).astype(bf16)


def segment(panels, start, target):
    tile, at = divmod(start, LANES)
    here = panels[tile]
    if at and tile + 1 < len(panels):
        lane = lax.broadcasted_iota(jnp.int32, here.shape, 1)
        here = jnp.where(lane >= at, here, panels[tile + 1])
    shift = (target - at) % LANES
    return pltpu.roll(here, shift, 1) if shift else here


def triangle_kernel(
    rows_here, cols_here, vectors_ref, lr_ref, sum_ref, left_scratch, right_scratch, sum_scratch
):
    _, panels_in, own, _ = lr_ref.shape
    residues = left_scratch.shape[0]
    cols = residues // cols_here
    rows = residues // rows_here
    cells = rows_here * cols_here
    lane = lax.broadcasted_iota(jnp.int32, (own, LANES), 1)
    for r in range(rows):
        parts = [
            [lr_ref[r * cols + c, t].astype(f32) for t in range(panels_in)] for c in range(cols)
        ]
        for side, scratch in ((0, left_scratch), (1, right_scratch)):
            for i in range(rows_here):
                start = side * cells + i * cols_here
                line = segment(parts[0], start, 0)
                for c in range(1, cols):
                    moved = segment(parts[c], start, c * cols_here)
                    line = jnp.where(lane < c * cols_here, line, moved)
                scratch[r * rows_here + i] = line
    live_wide = vectors_ref[0:1]
    live_square = jnp.broadcast_to(live_wide, (LANES, LANES))
    both = live_square * jnp.transpose(live_square)
    both = both[:residues]
    keep = live_wide > 0
    for h in range(own):
        left = jnp.where(keep, left_scratch[:, h, :], 0.0).astype(bf16)
        right = jnp.where(keep, right_scratch[:, h, :], 0.0).astype(bf16)
        right = jnp.concatenate([right, jnp.zeros((LANES - residues, LANES), bf16)], axis=0)
        sum_scratch[:, h, :] = dot_nt(left, right) * both
    tiles = sum_ref.shape[1]
    for r in range(rows):
        lines = [sum_scratch[r * rows_here + i] for i in range(rows_here)]
        for c in range(cols):
            for t in range(tiles):
                panel = None
                for i in range(rows_here):
                    low, high = i * cols_here - t * LANES, (i + 1) * cols_here - t * LANES
                    if high <= 0 or low >= LANES:
                        continue
                    shift = (low - c * cols_here) % LANES
                    line = pltpu.roll(lines[i], shift, 1) if shift else lines[i]
                    panel = line if panel is None else jnp.where(lane >= low, line, panel)
                sum_ref[r * cols + c, t] = panel.astype(bf16)


def middle_kernel(
    pair_ref,
    normed_ref,
    sum_ref,
    vectors_ref,
    out_w_ref,
    gate_w_ref,
    bias_w_ref,
    mid_ref,
    att_ref,
    bias_ref,
):
    devices, tiles, own, _ = sum_ref.shape
    cells, _ = pair_ref.shape
    hidden = devices * own
    gain_col = jnp.transpose(jnp.broadcast_to(vectors_ref[1:2], (LANES, hidden)))
    gate = sigmoid(dot_nn(normed_ref[...], gate_w_ref[...]))
    bias_w = bias_w_ref[...]
    for t in range(tiles):
        total = sum_ref[:, t].astype(f32).reshape(hidden, LANES)
        center = jnp.mean(total, axis=0, keepdims=True)
        centered = total - center
        variance = jnp.mean(centered * centered, axis=0, keepdims=True)
        hidden_normed = centered * lax.rsqrt(variance + epsilon) * gain_col
        hidden_rows = jnp.transpose(hidden_normed).astype(bf16)
        low, high = t * LANES, min((t + 1) * LANES, cells)
        update = dot_nn(hidden_rows[: high - low], out_w_ref[...])
        mid = pair_ref[low:high] + gate[low:high] * update
        mid_ref[low:high] = mid
        att = norm_last(mid, vectors_ref[2:3]).astype(bf16)
        att_ref[low:high] = att
        bias_ref[0, :, low:high] = dot_nt(bias_w, att).astype(bf16)


def own_kernel(heads, att_ref, w_ref, q_ref, k_ref, v_ref, gate_ref, kv_w_ref, w_scratch):
    rows_here, cols_here, chan = att_ref.shape
    width = w_ref.shape[2]
    shape = (rows_here, cols_here, width)
    att = att_ref[...].reshape(rows_here * cols_here, chan)
    w = [m.astype(bf16) for m in split_weight(w_ref, w_scratch)]
    kv_w_ref[0], kv_w_ref[1] = w[1], w[2]
    q_ref[...] = (dot_nn(att, w[0]) * (width // heads) ** (-0.5)).astype(bf16).reshape(shape)
    k_ref[...] = dot_nn(att, w[1]).astype(bf16).reshape(shape)
    v_ref[...] = dot_nn(att, w[2]).astype(bf16).reshape(shape)
    gate_ref[...] = sigmoid(dot_nn(att, w[3])).reshape(shape)


def scores_kernel(heads, q_ref, k_ref, far_ref, kv_w_ref, scores_ref, v_far_ref):
    rows_here, cols_here, width = q_ref.shape
    far = far_ref[...].reshape(rows_here * cols_here, width)
    k_far = dot_nn(far, kv_w_ref[0]).astype(bf16).reshape(q_ref.shape)
    v_far_ref[...] = dot_nn(far, kv_w_ref[1]).astype(bf16).reshape(q_ref.shape)
    head_of = lax.broadcasted_iota(jnp.int32, (cols_here, width), 1) // (width // heads)
    for i in range(rows_here):
        q = q_ref[i]
        q_heads = jnp.concatenate(
            [jnp.where(head_of == h, q, jnp.zeros_like(q)) for h in range(heads)], axis=0
        )
        scores_ref[i] = dot_nt(q_heads, jnp.concatenate([k_ref[i], k_far[i]], axis=0))


def attention_kernel(
    vectors_ref,
    fetched_ref,
    swapped_ref,
    scores_ref,
    v_ref,
    v_far_ref,
    gate_ref,
    mid_ref,
    out_w_ref,
    out_ref,
    bias_scratch,
):
    rows_here, cols_here, width = v_ref.shape
    blocks, heads, cells = fetched_ref.shape
    residues = 2 * cols_here
    row, col = lax.axis_index("row"), lax.axis_index(("col", "sub"))
    same = jnp.bitwise_and(row, 1) == col
    chip = lax.div(row, 2)
    lane_row = lax.broadcasted_iota(jnp.int32, (1, LANES), 1)
    live = vectors_ref[0:1]
    swapped = jnp.where(
        lane_row < cols_here,
        pltpu.roll(live, LANES - cols_here, 1),
        pltpu.roll(live, cols_here, 1),
    )
    penalty = (jnp.where(col == 0, live, swapped) - 1.0) * mask_penalty
    lane = lax.broadcasted_iota(jnp.int32, (heads, LANES), 1)
    pad = (-cells) % LANES

    def panels(v):
        v = jnp.concatenate([v, jnp.zeros((heads, pad), f32)], axis=1) if pad else v
        return [v[:, t * LANES : (t + 1) * LANES] for t in range((cells + pad) // LANES)]

    for m in range(blocks):
        p, n = m // 2, m % 2
        block = 2 * jnp.bitwise_xor(jnp.bitwise_and(chip, 1), p)
        block = block + jnp.bitwise_xor(n, lax.div(chip, 2))
        first, second = fetched_ref[m].astype(f32), swapped_ref[m].astype(f32)
        mine = panels(jnp.where(same, first, second))
        other = panels(jnp.where(same, second, first))
        for j in range(rows_here):
            bias_scratch[block * rows_here + j] = jnp.where(
                lane < cols_here,
                segment(mine, j * cols_here, 0),
                segment(other, j * cols_here, cols_here),
            )
    penalty = penalty[:, :residues]
    head_bias = [bias_scratch[:, h, :][:, :residues] + penalty for h in range(heads)]
    head_bias = jnp.concatenate(head_bias, axis=0)
    head_of = lax.broadcasted_iota(jnp.int32, (cols_here, width), 1) // (width // heads)
    for i in range(rows_here):
        v = jnp.concatenate([v_ref[i], v_far_ref[i]], axis=0)
        scores = scores_ref[i] + head_bias
        raised = jnp.exp(scores - jnp.max(scores, axis=-1, keepdims=True))
        weights = (raised / jnp.sum(raised, axis=-1, keepdims=True)).astype(bf16)
        mixed = dot_nn(weights, v)
        attended = mixed[:cols_here]
        for h in range(1, heads):
            attended = jnp.where(head_of == h, mixed[h * cols_here : (h + 1) * cols_here], attended)
        gated = (attended * gate_ref[i]).astype(bf16)
        out_ref[i] = mid_ref[i] + dot_nn(gated, out_w_ref[...])


def body_channels(
    pair,
    residue_mask,
    tri_norm_gain,
    tri_in_weight,
    tri_gate_weight,
    tri_out_norm_gain,
    tri_out_weight,
    att_norm_gain,
    att_proj_weight,
    att_bias_weight,
    att_out_weight,
):
    rows_here, cols_here, chan = pair.shape
    rows, cols = lax.axis_size("row"), lax.axis_size(("col", "sub"))
    group = ("row", "col", "sub")
    devices = rows * cols
    residues = cols_here * cols
    cells = rows_here * cols_here
    hidden = tri_in_weight.shape[2]
    own = hidden // devices
    heads = att_bias_weight.shape[1]
    tiles = -(-cells // LANES)
    lr_panels = -(-2 * cells // LANES) if (-cells) % LANES * 2 == LANES else 2 * tiles
    flat = pair.reshape(cells, chan)
    live = residue_mask.reshape(1, residues)

    lr, normed, vectors = pl.pallas_call(
        functools.partial(factors_kernel, devices),
        out_shape=(
            pltpu.VMEM((devices, lr_panels, own, LANES), bf16),
            pltpu.VMEM((cells, chan), bf16),
            pltpu.VMEM((8, LANES), f32),
        ),
        scratch_shapes=[pltpu.VMEM(tri_in_weight.shape, f32)],
        compiler_params=kernel_params,
        name="factors",
    )(
        *map(
            afar,
            (
                flat,
                tri_norm_gain.reshape(1, chan),
                tri_in_weight,
                live,
                tri_out_norm_gain.reshape(1, hidden),
                att_norm_gain.reshape(1, chan),
            ),
        )
    )
    lr = lax.all_to_all(lr, group, 0, 0, tiled=True)
    sums = pl.pallas_call(
        functools.partial(triangle_kernel, rows_here, cols_here),
        out_shape=pltpu.VMEM((devices, tiles, own, LANES), bf16),
        scratch_shapes=[pltpu.VMEM((residues, own, LANES), f32) for _ in range(3)],
        compiler_params=kernel_params,
        name="triangle",
    )(near(vectors), near(lr))
    sums = lax.all_to_all(sums, group, 0, 0, tiled=True)
    shape = (rows_here, cols_here, chan)
    mid, att, bias = pl.pallas_call(
        middle_kernel,
        out_shape=(
            pltpu.VMEM((cells, chan), f32),
            pltpu.VMEM((cells, chan), bf16),
            pltpu.VMEM((1, heads, cells), bf16),
        ),
        compiler_params=kernel_params,
        name="middle",
    )(
        *map(
            near,
            (
                flat,
                normed,
                sums,
                vectors,
                tri_out_weight,
                tri_gate_weight,
                att_bias_weight.T,
            ),
        )
    )
    att, mid = att.reshape(shape), mid.reshape(shape)

    def swap(v):
        return lax.ppermute(v, "row", [(r, r ^ 1) for r in range(rows)])

    joined = swap(bias)
    bias = jnp.concatenate([bias, joined], axis=0)
    fetched = []
    for p in range(2):
        pairs = []
        for z in range(rows // 2):
            for s in range(2):
                for x in range(cols):
                    target = (2 * s + ((z & 1) ^ p)) * 2 + x
                    pairs.append(((2 * z + s) * cols + x, target * cols + (z >> 1)))
        fetched.append(lax.ppermute(bias, group, pairs))
    far = lax.ppermute(att, ("col", "sub"), [(c, c ^ 1) for c in range(cols)])
    queries, keys, values, gate, kv_weight = pl.pallas_call(
        functools.partial(own_kernel, heads),
        out_shape=(
            pltpu.VMEM(shape, bf16),
            pltpu.VMEM(shape, bf16),
            pltpu.VMEM(shape, bf16),
            pltpu.VMEM(shape, f32),
            pltpu.VMEM((2, chan, chan), bf16),
        ),
        scratch_shapes=[pltpu.VMEM(att_proj_weight.shape, f32)],
        compiler_params=kernel_params,
        name="own",
    )(near(att), near(att_proj_weight))
    fetched = jnp.concatenate(fetched, axis=0)
    swapped = swap(fetched)
    scores, values_far = pl.pallas_call(
        functools.partial(scores_kernel, heads),
        out_shape=(
            pltpu.VMEM((rows_here, heads * cols_here, residues), f32),
            pltpu.VMEM(shape, bf16),
        ),
        compiler_params=kernel_params,
        name="scores",
    )(*map(near, (queries, keys, far, kv_weight)))
    return pl.pallas_call(
        attention_kernel,
        out_shape=jax.ShapeDtypeStruct(shape, f32),
        scratch_shapes=[pltpu.VMEM((cols_here, heads, LANES), f32)],
        compiler_params=kernel_params,
        name="attention",
    )(*map(near, (vectors, fetched, swapped, scores, values, values_far, gate, mid, att_out_weight)))


def solution(mesh):
    placed = (
        P(("parts", "row"), ("col", "sub"), None),
        P("parts"),
        P(),
        P(),
        P(),
        P(),
        P(),
        P(),
        P(),
        P(),
        P(),
    )

    def body(pair, residue_mask, tri_norm_gain, tri_in_weight, *others):
        rows, cols = mesh.shape["row"], mesh.shape["col"] * mesh.shape["sub"]
        hidden = tri_in_weight.shape[2]
        fits = (
            cols == 2
            and rows == 8
            and hidden % (8 * rows * cols) == 0
            and hidden == pair.shape[2] == LANES
            and residue_mask.shape[0] <= LANES
            and pair.shape[0] * cols * pair.shape[1] % 16 == 0
        )
        chosen = body_channels if fits else body_general
        return chosen(pair, residue_mask, tri_norm_gain, tri_in_weight, *others)

    return jax.shard_map(
        body,
        mesh=mesh,
        in_specs=placed,
        out_specs=P(("parts", "row"), ("col", "sub"), None),
        check_vma=False,
    )
```

```python
import functools
import math

import jax
import jax.numpy as jnp
from jax import lax
from jax.experimental import pallas as pl
from jax.experimental.pallas import tpu as pltpu
from jax.sharding import PartitionSpec as P


epsilon = 1e-05
mask_penalty = 1000000000.0
LANES = 128
f32 = jnp.float32
bf16 = jnp.bfloat16


def norm_last(values_in, gain):
    center = jnp.mean(values_in, axis=-1, keepdims=True)
    centered = values_in - center
    variance = jnp.mean(centered * centered, axis=-1, keepdims=True)
    return centered * lax.rsqrt(variance + epsilon) * gain


def sigmoid(v):
    return 0.5 * jnp.tanh(0.5 * v) + 0.5


def project(normed, weight):
    flat_rows = normed.reshape(-1, normed.shape[-1])
    product = jnp.dot(flat_rows, weight, preferred_element_type=jnp.float32)
    return product.reshape(normed.shape[:-1] + (weight.shape[1],))


def body_general(
    pair,
    residue_mask,
    tri_norm_gain,
    tri_in_weight,
    tri_gate_weight,
    tri_out_norm_gain,
    tri_out_weight,
    att_norm_gain,
    att_proj_weight,
    att_bias_weight,
    att_out_weight,
):
    rows_here, cols_here, _ = pair.shape
    residues = cols_here * lax.axis_size(("col", "sub"))
    row_offset = lax.axis_index("row") * rows_here
    col_offset = lax.axis_index(("col", "sub")) * cols_here
    residue_live = residue_mask.astype(jnp.float32)
    live_rows = lax.dynamic_slice_in_dim(residue_live, row_offset, rows_here)
    live_cols = lax.dynamic_slice_in_dim(residue_live, col_offset, cols_here)
    pair_live = (live_rows[:, None] * live_cols[None, :])[:, :, None]
    tri_normed = norm_last(pair, tri_norm_gain).astype(jnp.bfloat16)
    in_width = tri_in_weight.shape[2]
    projected = project(tri_normed, tri_in_weight.reshape(tri_in_weight.shape[0], -1)).reshape(
        rows_here, cols_here, 4, in_width
    )
    left_factor = (jax.nn.sigmoid(projected[:, :, 0]) * projected[:, :, 1] * pair_live).astype(
        jnp.bfloat16
    )
    right_factor = (jax.nn.sigmoid(projected[:, :, 2]) * projected[:, :, 3] * pair_live).astype(
        jnp.bfloat16
    )
    left_all, right_all = (
        lax.all_gather(left_factor, ("col", "sub"), axis=1, tiled=True),
        lax.all_gather(right_factor, ("col", "sub"), axis=1, tiled=True),
    )
    exchanged = lax.all_to_all(right_all, "row", split_axis=1, concat_axis=0, tiled=True)
    own_rows = lax.dynamic_slice_in_dim(exchanged, col_offset, cols_here, 0)
    tri_sum = jnp.einsum(
        "ikh,jkh->ijh",
        left_all,
        lax.all_gather(own_rows, "row", axis=1, tiled=True),
        preferred_element_type=jnp.float32,
    )
    hidden_normed = norm_last(tri_sum, tri_out_norm_gain).astype(jnp.bfloat16)
    tri_gate = jax.nn.sigmoid(project(tri_normed, tri_gate_weight))
    pair_mid = pair + tri_gate * project(hidden_normed, tri_out_weight)
    att_normed = norm_last(pair_mid, att_norm_gain).astype(jnp.bfloat16)
    head_width = att_proj_weight.shape[2]
    heads_here = att_bias_weight.shape[1]
    head_size = head_width // heads_here
    projected = project(att_normed, att_proj_weight.reshape(att_proj_weight.shape[0], -1)).reshape(
        rows_here, cols_here, 4, head_width
    )
    queries = (projected[:, :, 0] * head_size ** (-0.5)).astype(jnp.bfloat16)
    key_rows = projected[:, :, 1].astype(jnp.bfloat16)
    value_rows = projected[:, :, 2].astype(jnp.bfloat16)
    att_gate = jax.nn.sigmoid(projected[:, :, 3])
    pair_bias = project(att_normed, att_bias_weight).astype(jnp.bfloat16)
    key_all, value_all = (
        lax.all_gather(key_rows, ("col", "sub"), axis=1, tiled=True),
        lax.all_gather(value_rows, ("col", "sub"), axis=1, tiled=True),
    )
    bias_all_rows = lax.all_gather(pair_bias, "row", axis=0, tiled=True)
    bias_panel = lax.all_to_all(
        bias_all_rows, ("col", "sub"), split_axis=0, concat_axis=1, tiled=True
    )
    mask_row = (residue_live - 1.0) * mask_penalty
    head_bias = jnp.transpose(bias_panel.astype(jnp.float32), (2, 0, 1)) + mask_row[None, None, :]
    block_rows = math.gcd(rows_here, max(1, 512 // cols_here))
    blocks = rows_here // block_rows

    def attend(block_items):
        query_block, key_block, value_block = block_items
        scores = (
            jnp.einsum(
                "ijhd,ikhd->ihjk", query_block, key_block, preferred_element_type=jnp.float32
            )
            + head_bias[None]
        )
        row_max = jnp.max(scores, axis=-1, keepdims=True)
        raised = jnp.exp(scores - row_max)
        weights = (raised / jnp.sum(raised, axis=-1, keepdims=True)).astype(jnp.bfloat16)
        return jnp.einsum(
            "ihjk,ikhd->ijhd", weights, value_block, preferred_element_type=jnp.float32
        )

    attended = lax.map(
        attend,
        (
            queries.reshape(blocks, block_rows, cols_here, heads_here, head_size),
            key_all.reshape(blocks, block_rows, residues, heads_here, head_size),
            value_all.reshape(blocks, block_rows, residues, heads_here, head_size),
        ),
    )
    gated = (attended.reshape(rows_here, cols_here, head_width) * att_gate).astype(jnp.bfloat16)
    return pair_mid + project(gated, att_out_weight)


def dot_nn(a, b):
    return lax.dot_general(a, b, (((1,), (0,)), ((), ())), preferred_element_type=f32)


def dot_nt(a, b):
    return lax.dot_general(a, b, (((1,), (1,)), ((), ())), preferred_element_type=f32)


kernel_params = pltpu.CompilerParams(vmem_limit_bytes=16 << 20)


def near(v):
    return pltpu.with_memory_space_constraint(v, pltpu.VMEM)


def afar(v):
    return pltpu.with_memory_space_constraint(v, pltpu.HBM)


def split_weight(w_ref, w_scratch):
    w_scratch[...] = w_ref[...].astype(f32)
    return [w_scratch[:, p, :] for p in range(w_ref.shape[1])]


def factors_kernel(
    devices,
    pair_ref,
    gain_ref,
    w_ref,
    live_ref,
    out_gain_ref,
    att_gain_ref,
    lr_ref,
    normed_ref,
    rows_ref,
    w_scratch,
):
    cells, _ = pair_ref.shape
    live = live_ref[...].astype(f32)
    rows_ref[0:1] = jnp.concatenate([live, jnp.zeros((1, LANES - live.shape[1]), f32)], axis=1)
    rows_ref[1:2] = out_gain_ref[...]
    rows_ref[2:3] = att_gain_ref[...]
    hidden = w_ref.shape[2]
    own = hidden // devices
    normed = norm_last(pair_ref[...], gain_ref[...]).astype(bf16)
    normed_ref[...] = normed
    w_t = [jnp.transpose(w).astype(bf16) for w in split_weight(w_ref, w_scratch)]
    spare = (-cells) % LANES
    tiles = (cells + spare) // LANES
    if spare:
        tail = normed[:spare]
        rhs_left = jnp.concatenate([normed, tail], axis=0)
        rhs_right = jnp.concatenate([tail, normed], axis=0)
    else:
        rhs_left = rhs_right = normed
    left = sigmoid(dot_nt(w_t[0], rhs_left)) * dot_nt(w_t[1], rhs_left)
    right = sigmoid(dot_nt(w_t[2], rhs_right)) * dot_nt(w_t[3], rhs_right)
    panels = [left[:, t * LANES : (t + 1) * LANES] for t in range(tiles)]
    right_panels = [right[:, t * LANES : (t + 1) * LANES] for t in range(tiles)]
    if spare:
        lane = lax.broadcasted_iota(jnp.int32, (hidden, LANES), 1)
        panels[-1] = jnp.where(lane < LANES - spare, panels[-1], right_panels[0])
        panels += right_panels[1:]
    else:
        panels += right_panels
    for t, panel in enumerate(panels):
        lr_ref[:, t] = panel.reshape(devices, own, LANES).astype(bf16)


def segment(panels, start, target):
    tile, at = divmod(start, LANES)
    here = panels[tile]
    if at and tile + 1 < len(panels):
        lane = lax.broadcasted_iota(jnp.int32, here.shape, 1)
        here = jnp.where(lane >= at, here, panels[tile + 1])
    shift = (target - at) % LANES
    return pltpu.roll(here, shift, 1) if shift else here


def triangle_kernel(
    rows_here, cols_here, vectors_ref, lr_ref, sum_ref, left_scratch, right_scratch, sum_scratch
):
    _, panels_in, own, _ = lr_ref.shape
    residues = left_scratch.shape[0]
    cols = residues // cols_here
    rows = residues // rows_here
    cells = rows_here * cols_here
    lane = lax.broadcasted_iota(jnp.int32, (own, LANES), 1)
    for r in range(rows):
        parts = [
            [lr_ref[r * cols + c, t].astype(f32) for t in range(panels_in)] for c in range(cols)
        ]
        for side, scratch in ((0, left_scratch), (1, right_scratch)):
            for i in range(rows_here):
                start = side * cells + i * cols_here
                line = segment(parts[0], start, 0)
                for c in range(1, cols):
                    moved = segment(parts[c], start, c * cols_here)
                    line = jnp.where(lane < c * cols_here, line, moved)
                scratch[r * rows_here + i] = line
    live_wide = vectors_ref[0:1]
    live_square = jnp.broadcast_to(live_wide, (LANES, LANES))
    both = live_square * jnp.transpose(live_square)
    both = both[:residues]
    keep = live_wide > 0
    for h in range(own):
        left = jnp.where(keep, left_scratch[:, h, :], 0.0).astype(bf16)
        right = jnp.where(keep, right_scratch[:, h, :], 0.0).astype(bf16)
        right = jnp.concatenate([right, jnp.zeros((LANES - residues, LANES), bf16)], axis=0)
        sum_scratch[:, h, :] = dot_nt(left, right) * both
    tiles = sum_ref.shape[1]
    for r in range(rows):
        lines = [sum_scratch[r * rows_here + i] for i in range(rows_here)]
        for c in range(cols):
            for t in range(tiles):
                panel = None
                for i in range(rows_here):
                    low, high = i * cols_here - t * LANES, (i + 1) * cols_here - t * LANES
                    if high <= 0 or low >= LANES:
                        continue
                    shift = (low - c * cols_here) % LANES
                    line = pltpu.roll(lines[i], shift, 1) if shift else lines[i]
                    panel = line if panel is None else jnp.where(lane >= low, line, panel)
                sum_ref[r * cols + c, t] = panel.astype(bf16)


def middle_kernel(
    pair_ref,
    normed_ref,
    sum_ref,
    vectors_ref,
    out_w_ref,
    gate_w_ref,
    bias_w_ref,
    mid_ref,
    att_ref,
    bias_ref,
):
    devices, tiles, own, _ = sum_ref.shape
    cells, _ = pair_ref.shape
    hidden = devices * own
    gain_col = jnp.transpose(jnp.broadcast_to(vectors_ref[1:2], (LANES, hidden)))
    gate = sigmoid(dot_nn(normed_ref[...], gate_w_ref[...]))
    bias_w = bias_w_ref[...]
    hidden_rows = []
    for t in range(tiles):
        total = sum_ref[:, t].astype(f32).reshape(hidden, LANES)
        center = jnp.mean(total, axis=0, keepdims=True)
        centered = total - center
        variance = jnp.mean(centered * centered, axis=0, keepdims=True)
        hidden_normed = centered * lax.rsqrt(variance + epsilon) * gain_col
        hidden_rows.append(jnp.transpose(hidden_normed).astype(bf16))
    hidden_rows = jnp.concatenate(hidden_rows, axis=0)[:cells]
    mid = pair_ref[...] + gate * dot_nn(hidden_rows, out_w_ref[...])
    mid_ref[...] = mid
    att = norm_last(mid, vectors_ref[2:3]).astype(bf16)
    att_ref[...] = att
    bias_ref[0] = dot_nt(bias_w, att).astype(bf16)


def own_kernel(heads, att_ref, w_ref, q_ref, k_ref, v_ref, gate_ref, kv_w_ref, w_scratch):
    rows_here, cols_here, chan = att_ref.shape
    width = w_ref.shape[2]
    shape = (rows_here, cols_here, width)
    att = att_ref[...].reshape(rows_here * cols_here, chan)
    w = [m.astype(bf16) for m in split_weight(w_ref, w_scratch)]
    kv_w_ref[0], kv_w_ref[1] = w[1], w[2]
    q_ref[...] = (dot_nn(att, w[0]) * (width // heads) ** (-0.5)).astype(bf16).reshape(shape)
    k_ref[...] = dot_nn(att, w[1]).astype(bf16).reshape(shape)
    v_ref[...] = dot_nn(att, w[2]).astype(bf16).reshape(shape)
    gate_ref[...] = sigmoid(dot_nn(att, w[3])).reshape(shape)


def scores_kernel(heads, q_ref, k_ref, far_ref, kv_w_ref, scores_ref, v_far_ref):
    rows_here, cols_here, width = q_ref.shape
    far = far_ref[...].reshape(rows_here * cols_here, width)
    k_far = dot_nn(far, kv_w_ref[0]).astype(bf16).reshape(q_ref.shape)
    v_far_ref[...] = dot_nn(far, kv_w_ref[1]).astype(bf16).reshape(q_ref.shape)
    head_of = lax.broadcasted_iota(jnp.int32, (cols_here, width), 1) // (width // heads)
    for i in range(rows_here):
        q = q_ref[i]
        q_heads = jnp.concatenate(
            [jnp.where(head_of == h, q, jnp.zeros_like(q)) for h in range(heads)], axis=0
        )
        scores_ref[i] = dot_nt(q_heads, jnp.concatenate([k_ref[i], k_far[i]], axis=0))


def attention_kernel(
    vectors_ref,
    fetched_ref,
    swapped_ref,
    scores_ref,
    v_ref,
    v_far_ref,
    gate_ref,
    mid_ref,
    out_w_ref,
    out_ref,
    bias_scratch,
    result,
    done,
):
    rows_here, cols_here, width = v_ref.shape
    chunks = done.shape[0]
    blocks, heads, cells = fetched_ref.shape
    residues = 2 * cols_here
    row, col = lax.axis_index("row"), lax.axis_index(("col", "sub"))
    same = jnp.bitwise_and(row, 1) == col
    chip = lax.div(row, 2)
    lane_row = lax.broadcasted_iota(jnp.int32, (1, LANES), 1)
    live = vectors_ref[0:1]
    swapped = jnp.where(
        lane_row < cols_here,
        pltpu.roll(live, LANES - cols_here, 1),
        pltpu.roll(live, cols_here, 1),
    )
    penalty = (jnp.where(col == 0, live, swapped) - 1.0) * mask_penalty
    lane = lax.broadcasted_iota(jnp.int32, (heads, LANES), 1)
    pad = (-cells) % LANES

    def panels(v):
        v = jnp.concatenate([v, jnp.zeros((heads, pad), f32)], axis=1) if pad else v
        return [v[:, t * LANES : (t + 1) * LANES] for t in range((cells + pad) // LANES)]

    for m in range(blocks):
        p, n = m // 2, m % 2
        block = 2 * jnp.bitwise_xor(lax.div(chip, 2), 1 - p)
        block = block + jnp.bitwise_xor(n, jnp.bitwise_and(chip, 1))
        first, second = fetched_ref[m].astype(f32), swapped_ref[m].astype(f32)
        mine = panels(jnp.where(same, first, second))
        other = panels(jnp.where(same, second, first))
        for j in range(rows_here):
            bias_scratch[block * rows_here + j] = jnp.where(
                lane < cols_here,
                segment(mine, j * cols_here, 0),
                segment(other, j * cols_here, cols_here),
            )
    penalty = penalty[:, :residues]
    head_bias = [bias_scratch[:, h, :][:, :residues] + penalty for h in range(heads)]
    head_bias = jnp.concatenate(head_bias, axis=0)
    head_of = lax.broadcasted_iota(jnp.int32, (cols_here, width), 1) // (width // heads)
    ones = jnp.ones((residues, width), bf16)
    chunk = rows_here // chunks
    copies = []
    for c in range(chunks):
        gated = []
        for i in range(c * chunk, (c + 1) * chunk):
            v = jnp.concatenate([v_ref[i], v_far_ref[i]], axis=0)
            scores = scores_ref[i] + head_bias
            raised = jnp.exp(scores - jnp.max(scores, axis=-1, keepdims=True)).astype(bf16)
            mixed = dot_nn(raised, jnp.concatenate([v, ones], axis=1))
            attended = mixed[:cols_here]
            for h in range(1, heads):
                part = mixed[h * cols_here : (h + 1) * cols_here]
                attended = jnp.where(jnp.tile(head_of, (1, 2)) == h, part, attended)
            attended = attended[:, :width] / attended[:, width:]
            gated.append((attended * gate_ref[i]).astype(bf16))
        update = dot_nn(jnp.concatenate(gated, axis=0), out_w_ref[...])
        at = slice(c * chunk, (c + 1) * chunk)
        result[at] = mid_ref[at] + update.reshape(chunk, cols_here, width)
        copies.append(pltpu.make_async_copy(result.at[at], out_ref.at[at], done.at[c]))
        copies[-1].start()
    for copy in copies:
        copy.wait()


def body_channels(
    pair,
    residue_mask,
    tri_norm_gain,
    tri_in_weight,
    tri_gate_weight,
    tri_out_norm_gain,
    tri_out_weight,
    att_norm_gain,
    att_proj_weight,
    att_bias_weight,
    att_out_weight,
):
    rows_here, cols_here, chan = pair.shape
    rows, cols = lax.axis_size("row"), lax.axis_size(("col", "sub"))
    group = ("row", "col", "sub")
    devices = rows * cols
    residues = cols_here * cols
    cells = rows_here * cols_here
    hidden = tri_in_weight.shape[2]
    own = hidden // devices
    heads = att_bias_weight.shape[1]
    tiles = -(-cells // LANES)
    lr_panels = -(-2 * cells // LANES) if (-cells) % LANES * 2 == LANES else 2 * tiles
    flat = pair.reshape(cells, chan)
    live = residue_mask.reshape(1, residues)

    lr, normed, vectors = pl.pallas_call(
        functools.partial(factors_kernel, devices),
        out_shape=(
            pltpu.VMEM((devices, lr_panels, own, LANES), bf16),
            pltpu.VMEM((cells, chan), bf16),
            pltpu.VMEM((8, LANES), f32),
        ),
        scratch_shapes=[pltpu.VMEM(tri_in_weight.shape, f32)],
        compiler_params=kernel_params,
        name="factors",
    )(
        *map(
            afar,
            (
                flat,
                tri_norm_gain.reshape(1, chan),
                tri_in_weight,
                live,
                tri_out_norm_gain.reshape(1, hidden),
                att_norm_gain.reshape(1, chan),
            ),
        )
    )
    lr = lax.all_to_all(lr, group, 0, 0, tiled=True)
    sums = pl.pallas_call(
        functools.partial(triangle_kernel, rows_here, cols_here),
        out_shape=pltpu.VMEM((devices, tiles, own, LANES), bf16),
        scratch_shapes=[pltpu.VMEM((residues, own, LANES), f32) for _ in range(3)],
        compiler_params=kernel_params,
        name="triangle",
    )(near(vectors), near(lr))
    sums = lax.all_to_all(sums, group, 0, 0, tiled=True)
    shape = (rows_here, cols_here, chan)
    chunks = math.gcd(rows_here, 3)
    mid, att, bias = pl.pallas_call(
        middle_kernel,
        out_shape=(
            pltpu.VMEM((cells, chan), f32),
            pltpu.VMEM((cells, chan), bf16),
            pltpu.VMEM((1, heads, cells), bf16),
        ),
        compiler_params=kernel_params,
        name="middle",
    )(
        *map(
            near,
            (
                flat,
                normed,
                sums,
                vectors,
                tri_out_weight,
                tri_gate_weight,
                att_bias_weight.T,
            ),
        )
    )
    att, mid = att.reshape(shape), mid.reshape(shape)

    def swap(v):
        return lax.ppermute(v, "row", [(r, r ^ 1) for r in range(rows)])

    joined = swap(bias)
    bias = jnp.concatenate([bias, joined], axis=0)
    fetched = []
    for p in range(2):
        pairs = []
        for z in range(rows // 2):
            for s in range(2):
                for x in range(cols):
                    target = (2 * ((z & 1) ^ 1 ^ p) + s) * 2 + x
                    pairs.append(((2 * z + s) * cols + x, target * cols + (z >> 1)))
        fetched.append(lax.ppermute(bias, group, pairs))
    far = lax.ppermute(att, ("col", "sub"), [(c, c ^ 1) for c in range(cols)])
    queries, keys, values, gate, kv_weight = pl.pallas_call(
        functools.partial(own_kernel, heads),
        out_shape=(
            pltpu.VMEM(shape, bf16),
            pltpu.VMEM(shape, bf16),
            pltpu.VMEM(shape, bf16),
            pltpu.VMEM(shape, f32),
            pltpu.VMEM((2, chan, chan), bf16),
        ),
        scratch_shapes=[pltpu.VMEM(att_proj_weight.shape, f32)],
        compiler_params=kernel_params,
        name="own",
    )(near(att), near(att_proj_weight))
    fetched = jnp.concatenate(fetched, axis=0)
    swapped = swap(fetched)
    scores, values_far = pl.pallas_call(
        functools.partial(scores_kernel, heads),
        out_shape=(
            pltpu.VMEM((rows_here, heads * cols_here, residues), f32),
            pltpu.VMEM(shape, bf16),
        ),
        compiler_params=kernel_params,
        name="scores",
    )(*map(near, (queries, keys, far, kv_weight)))
    return pl.pallas_call(
        attention_kernel,
        out_shape=jax.ShapeDtypeStruct(shape, f32),
        out_specs=pl.BlockSpec(memory_space=pltpu.HBM),
        scratch_shapes=[
            pltpu.VMEM((cols_here, heads, LANES), f32),
            pltpu.VMEM(shape, f32),
            pltpu.SemaphoreType.DMA((chunks,)),
        ],
        compiler_params=kernel_params,
        name="attention",
    )(*map(near, (vectors, fetched, swapped, scores, values, values_far, gate, mid, att_out_weight)))


def solution(mesh):
    placed = (
        P(("parts", "row"), ("col", "sub"), None),
        P("parts"),
        P(),
        P(),
        P(),
        P(),
        P(),
        P(),
        P(),
        P(),
        P(),
    )

    def body(pair, residue_mask, tri_norm_gain, tri_in_weight, *others):
        rows, cols = mesh.shape["row"], mesh.shape["col"] * mesh.shape["sub"]
        hidden = tri_in_weight.shape[2]
        fits = (
            cols == 2
            and rows == 8
            and hidden % (8 * rows * cols) == 0
            and hidden == pair.shape[2] == LANES
            and residue_mask.shape[0] <= LANES
            and pair.shape[0] * cols * pair.shape[1] % 16 == 0
        )
        chosen = body_channels if fits else body_general
        return chosen(pair, residue_mask, tri_norm_gain, tri_in_weight, *others)

    return jax.shard_map(
        body,
        mesh=mesh,
        in_specs=placed,
        out_specs=P(("parts", "row"), ("col", "sub"), None),
        check_vma=False,
    )
```

```python
import functools
import math

import jax
import jax.numpy as jnp
from jax import lax
from jax.experimental import pallas as pl
from jax.experimental.pallas import tpu as pltpu
from jax.sharding import PartitionSpec as P


epsilon = 1e-05
mask_penalty = 1000000000.0
LANES = 128
f32 = jnp.float32
bf16 = jnp.bfloat16


def norm_last(values_in, gain):
    center = jnp.mean(values_in, axis=-1, keepdims=True)
    centered = values_in - center
    variance = jnp.mean(centered * centered, axis=-1, keepdims=True)
    return centered * lax.rsqrt(variance + epsilon) * gain


def sigmoid(v):
    return 0.5 * jnp.tanh(0.5 * v) + 0.5


def project(normed, weight):
    flat_rows = normed.reshape(-1, normed.shape[-1])
    product = jnp.dot(flat_rows, weight, preferred_element_type=jnp.float32)
    return product.reshape(normed.shape[:-1] + (weight.shape[1],))


def body_general(
    pair,
    residue_mask,
    tri_norm_gain,
    tri_in_weight,
    tri_gate_weight,
    tri_out_norm_gain,
    tri_out_weight,
    att_norm_gain,
    att_proj_weight,
    att_bias_weight,
    att_out_weight,
):
    rows_here, cols_here, _ = pair.shape
    residues = cols_here * lax.axis_size(("col", "sub"))
    row_offset = lax.axis_index("row") * rows_here
    col_offset = lax.axis_index(("col", "sub")) * cols_here
    residue_live = residue_mask.astype(jnp.float32)
    live_rows = lax.dynamic_slice_in_dim(residue_live, row_offset, rows_here)
    live_cols = lax.dynamic_slice_in_dim(residue_live, col_offset, cols_here)
    pair_live = (live_rows[:, None] * live_cols[None, :])[:, :, None]
    tri_normed = norm_last(pair, tri_norm_gain).astype(jnp.bfloat16)
    in_width = tri_in_weight.shape[2]
    projected = project(tri_normed, tri_in_weight.reshape(tri_in_weight.shape[0], -1)).reshape(
        rows_here, cols_here, 4, in_width
    )
    left_factor = (jax.nn.sigmoid(projected[:, :, 0]) * projected[:, :, 1] * pair_live).astype(
        jnp.bfloat16
    )
    right_factor = (jax.nn.sigmoid(projected[:, :, 2]) * projected[:, :, 3] * pair_live).astype(
        jnp.bfloat16
    )
    left_all, right_all = (
        lax.all_gather(left_factor, ("col", "sub"), axis=1, tiled=True),
        lax.all_gather(right_factor, ("col", "sub"), axis=1, tiled=True),
    )
    exchanged = lax.all_to_all(right_all, "row", split_axis=1, concat_axis=0, tiled=True)
    own_rows = lax.dynamic_slice_in_dim(exchanged, col_offset, cols_here, 0)
    tri_sum = jnp.einsum(
        "ikh,jkh->ijh",
        left_all,
        lax.all_gather(own_rows, "row", axis=1, tiled=True),
        preferred_element_type=jnp.float32,
    )
    hidden_normed = norm_last(tri_sum, tri_out_norm_gain).astype(jnp.bfloat16)
    tri_gate = jax.nn.sigmoid(project(tri_normed, tri_gate_weight))
    pair_mid = pair + tri_gate * project(hidden_normed, tri_out_weight)
    att_normed = norm_last(pair_mid, att_norm_gain).astype(jnp.bfloat16)
    head_width = att_proj_weight.shape[2]
    heads_here = att_bias_weight.shape[1]
    head_size = head_width // heads_here
    projected = project(att_normed, att_proj_weight.reshape(att_proj_weight.shape[0], -1)).reshape(
        rows_here, cols_here, 4, head_width
    )
    queries = (projected[:, :, 0] * head_size ** (-0.5)).astype(jnp.bfloat16)
    key_rows = projected[:, :, 1].astype(jnp.bfloat16)
    value_rows = projected[:, :, 2].astype(jnp.bfloat16)
    att_gate = jax.nn.sigmoid(projected[:, :, 3])
    pair_bias = project(att_normed, att_bias_weight).astype(jnp.bfloat16)
    key_all, value_all = (
        lax.all_gather(key_rows, ("col", "sub"), axis=1, tiled=True),
        lax.all_gather(value_rows, ("col", "sub"), axis=1, tiled=True),
    )
    bias_all_rows = lax.all_gather(pair_bias, "row", axis=0, tiled=True)
    bias_panel = lax.all_to_all(
        bias_all_rows, ("col", "sub"), split_axis=0, concat_axis=1, tiled=True
    )
    mask_row = (residue_live - 1.0) * mask_penalty
    head_bias = jnp.transpose(bias_panel.astype(jnp.float32), (2, 0, 1)) + mask_row[None, None, :]
    block_rows = math.gcd(rows_here, max(1, 512 // cols_here))
    blocks = rows_here // block_rows

    def attend(block_items):
        query_block, key_block, value_block = block_items
        scores = (
            jnp.einsum(
                "ijhd,ikhd->ihjk", query_block, key_block, preferred_element_type=jnp.float32
            )
            + head_bias[None]
        )
        row_max = jnp.max(scores, axis=-1, keepdims=True)
        raised = jnp.exp(scores - row_max)
        weights = (raised / jnp.sum(raised, axis=-1, keepdims=True)).astype(jnp.bfloat16)
        return jnp.einsum(
            "ihjk,ikhd->ijhd", weights, value_block, preferred_element_type=jnp.float32
        )

    attended = lax.map(
        attend,
        (
            queries.reshape(blocks, block_rows, cols_here, heads_here, head_size),
            key_all.reshape(blocks, block_rows, residues, heads_here, head_size),
            value_all.reshape(blocks, block_rows, residues, heads_here, head_size),
        ),
    )
    gated = (attended.reshape(rows_here, cols_here, head_width) * att_gate).astype(jnp.bfloat16)
    return pair_mid + project(gated, att_out_weight)


def dot_nn(a, b):
    return lax.dot_general(a, b, (((1,), (0,)), ((), ())), preferred_element_type=f32)


def dot_nt(a, b):
    return lax.dot_general(a, b, (((1,), (1,)), ((), ())), preferred_element_type=f32)


kernel_params = pltpu.CompilerParams(vmem_limit_bytes=16 << 20)


def near(v):
    return pltpu.with_memory_space_constraint(v, pltpu.VMEM)


def afar(v):
    return pltpu.with_memory_space_constraint(v, pltpu.HBM)


def split_weight(w_ref, w_scratch):
    rows, mats, out = w_ref.shape
    w_scratch[...] = w_ref[...].astype(f32).reshape(rows * mats, out)
    return [w_scratch[pl.ds(p, rows, stride=mats), :] for p in range(mats)]


def factors_kernel(
    devices,
    pair_ref,
    gain_ref,
    w_ref,
    live_ref,
    out_gain_ref,
    att_gain_ref,
    lr_ref,
    normed_ref,
    rows_ref,
    w_scratch,
):
    cells, _ = pair_ref.shape
    live = live_ref[...].astype(f32)
    rows_ref[0:1] = jnp.concatenate([live, jnp.zeros((1, LANES - live.shape[1]), f32)], axis=1)
    rows_ref[1:2] = out_gain_ref[...]
    rows_ref[2:3] = att_gain_ref[...]
    hidden = w_ref.shape[2]
    own = hidden // devices
    normed = norm_last(pair_ref[...], gain_ref[...]).astype(bf16)
    normed_ref[...] = normed
    w_t = [jnp.transpose(w).astype(bf16) for w in split_weight(w_ref, w_scratch)]
    spare = (-cells) % LANES
    tiles = (cells + spare) // LANES
    if spare:
        tail = normed[:spare]
        rhs_left = jnp.concatenate([normed, tail], axis=0)
        rhs_right = jnp.concatenate([tail, normed], axis=0)
    else:
        rhs_left = rhs_right = normed
    left = sigmoid(dot_nt(w_t[0], rhs_left)) * dot_nt(w_t[1], rhs_left)
    right = sigmoid(dot_nt(w_t[2], rhs_right)) * dot_nt(w_t[3], rhs_right)
    panels = [left[:, t * LANES : (t + 1) * LANES] for t in range(tiles)]
    right_panels = [right[:, t * LANES : (t + 1) * LANES] for t in range(tiles)]
    if spare:
        lane = lax.broadcasted_iota(jnp.int32, (hidden, LANES), 1)
        panels[-1] = jnp.where(lane < LANES - spare, panels[-1], right_panels[0])
        panels += right_panels[1:]
    else:
        panels += right_panels
    for t, panel in enumerate(panels):
        lr_ref[:, t] = panel.reshape(devices, own, LANES).astype(bf16)


def segment(panels, start, target):
    tile, at = divmod(start, LANES)
    here = panels[tile]
    if at and tile + 1 < len(panels):
        lane = lax.broadcasted_iota(jnp.int32, here.shape, 1)
        here = jnp.where(lane >= at, here, panels[tile + 1])
    shift = (target - at) % LANES
    return pltpu.roll(here, shift, 1) if shift else here


def triangle_kernel(
    rows_here, cols_here, vectors_ref, lr_ref, sum_ref, left_scratch, right_scratch, sum_scratch
):
    _, panels_in, own, _ = lr_ref.shape
    residues = left_scratch.shape[0] // own
    cols = residues // cols_here
    rows = residues // rows_here
    cells = rows_here * cols_here
    lane = lax.broadcasted_iota(jnp.int32, (own, LANES), 1)
    for r in range(rows):
        parts = [
            [lr_ref[r * cols + c, t].astype(f32) for t in range(panels_in)] for c in range(cols)
        ]
        for side, scratch in ((0, left_scratch), (1, right_scratch)):
            for i in range(rows_here):
                start = side * cells + i * cols_here
                line = segment(parts[0], start, 0)
                for c in range(1, cols):
                    moved = segment(parts[c], start, c * cols_here)
                    line = jnp.where(lane < c * cols_here, line, moved)
                scratch[pl.ds((r * rows_here + i) * own, own), :] = line
    live_wide = vectors_ref[0:1]
    live_square = jnp.broadcast_to(live_wide, (LANES, LANES))
    both = live_square * jnp.transpose(live_square)
    both = both[:residues]
    keep = live_wide > 0
    for h in range(own):
        left = jnp.where(keep, left_scratch[pl.ds(h, residues, stride=own), :], 0.0).astype(bf16)
        right = jnp.where(keep, right_scratch[pl.ds(h, residues, stride=own), :], 0.0).astype(bf16)
        right = jnp.concatenate([right, jnp.zeros((LANES - residues, LANES), bf16)], axis=0)
        sum_scratch[pl.ds(h, residues, stride=own), :] = dot_nt(left, right) * both
    tiles = sum_ref.shape[1]
    for r in range(rows):
        lines = [
            sum_scratch[pl.ds((r * rows_here + i) * own, own), :] for i in range(rows_here)
        ]
        for c in range(cols):
            for t in range(tiles):
                panel = None
                for i in range(rows_here):
                    low, high = i * cols_here - t * LANES, (i + 1) * cols_here - t * LANES
                    if high <= 0 or low >= LANES:
                        continue
                    shift = (low - c * cols_here) % LANES
                    line = pltpu.roll(lines[i], shift, 1) if shift else lines[i]
                    panel = line if panel is None else jnp.where(lane >= low, line, panel)
                sum_ref[r * cols + c, t] = panel.astype(bf16)


def middle_kernel(
    pair_ref,
    normed_ref,
    sum_ref,
    vectors_ref,
    out_w_ref,
    gate_w_ref,
    bias_w_ref,
    mid_ref,
    att_ref,
    bias_ref,
):
    devices, tiles, own, _ = sum_ref.shape
    cells, _ = pair_ref.shape
    hidden = devices * own
    gain_col = jnp.transpose(jnp.broadcast_to(vectors_ref[1:2], (LANES, hidden)))
    gate = sigmoid(dot_nn(normed_ref[...], gate_w_ref[...]))
    bias_w = bias_w_ref[...]
    hidden_rows = []
    for t in range(tiles):
        total = sum_ref[:, t].astype(f32).reshape(hidden, LANES)
        center = jnp.mean(total, axis=0, keepdims=True)
        centered = total - center
        variance = jnp.mean(centered * centered, axis=0, keepdims=True)
        hidden_normed = centered * lax.rsqrt(variance + epsilon) * gain_col
        hidden_rows.append(jnp.transpose(hidden_normed).astype(bf16))
    hidden_rows = jnp.concatenate(hidden_rows, axis=0)[:cells]
    mid = pair_ref[...] + gate * dot_nn(hidden_rows, out_w_ref[...])
    mid_ref[...] = mid
    att = norm_last(mid, vectors_ref[2:3]).astype(bf16)
    att_ref[...] = att
    bias_ref[0] = dot_nt(bias_w, att).astype(bf16)


def own_kernel(heads, att_ref, w_ref, q_ref, k_ref, v_ref, gate_ref, kv_w_ref, w_scratch):
    rows_here, cols_here, chan = att_ref.shape
    width = w_ref.shape[2]
    shape = (rows_here, cols_here, width)
    att = att_ref[...].reshape(rows_here * cols_here, chan)
    w = [m.astype(bf16) for m in split_weight(w_ref, w_scratch)]
    kv_w_ref[0], kv_w_ref[1] = w[1], w[2]
    q_ref[...] = (dot_nn(att, w[0]) * (width // heads) ** (-0.5)).astype(bf16).reshape(shape)
    k_ref[...] = dot_nn(att, w[1]).astype(bf16).reshape(shape)
    v_ref[...] = dot_nn(att, w[2]).astype(bf16).reshape(shape)
    gate_ref[...] = sigmoid(dot_nn(att, w[3])).reshape(shape)


def scores_kernel(heads, q_ref, k_ref, far_ref, kv_w_ref, scores_ref, v_far_ref):
    rows_here, cols_here, width = q_ref.shape
    far = far_ref[...].reshape(rows_here * cols_here, width)
    k_far = dot_nn(far, kv_w_ref[0]).astype(bf16).reshape(q_ref.shape)
    v_far_ref[...] = dot_nn(far, kv_w_ref[1]).astype(bf16).reshape(q_ref.shape)
    head_of = lax.broadcasted_iota(jnp.int32, (cols_here, width), 1) // (width // heads)
    for i in range(rows_here):
        q = q_ref[i]
        q_heads = jnp.concatenate(
            [jnp.where(head_of == h, q, jnp.zeros_like(q)) for h in range(heads)], axis=0
        )
        scores_ref[i] = dot_nt(q_heads, jnp.concatenate([k_ref[i], k_far[i]], axis=0))


def attention_kernel(
    vectors_ref,
    fetched_ref,
    swapped_ref,
    scores_ref,
    v_ref,
    v_far_ref,
    gate_ref,
    mid_ref,
    out_w_ref,
    out_ref,
    bias_scratch,
    result,
    done,
):
    rows_here, cols_here, width = v_ref.shape
    chunks = done.shape[0]
    blocks, heads, cells = fetched_ref.shape
    residues = 2 * cols_here
    row, col = lax.axis_index("row"), lax.axis_index(("col", "sub"))
    same = jnp.bitwise_and(row, 1) == 0
    chip = lax.div(row, 2)
    lane_row = lax.broadcasted_iota(jnp.int32, (1, LANES), 1)
    live = vectors_ref[0:1]
    swapped = jnp.where(
        lane_row < cols_here,
        pltpu.roll(live, LANES - cols_here, 1),
        pltpu.roll(live, cols_here, 1),
    )
    penalty = (jnp.where(col == 0, live, swapped) - 1.0) * mask_penalty
    lane = lax.broadcasted_iota(jnp.int32, (heads, LANES), 1)
    pad = (-cells) % LANES

    def panels(v):
        v = jnp.concatenate([v, jnp.zeros((heads, pad), f32)], axis=1) if pad else v
        return [v[:, t * LANES : (t + 1) * LANES] for t in range((cells + pad) // LANES)]

    for m in range(blocks):
        p, n = m // 2, m % 2
        block = 2 * jnp.bitwise_xor(lax.div(chip, 2), 1 - p)
        block = block + jnp.bitwise_xor(n, jnp.bitwise_xor(jnp.bitwise_and(chip, 1), col))
        first, second = fetched_ref[m].astype(f32), swapped_ref[m].astype(f32)
        mine = panels(jnp.where(same, first, second))
        other = panels(jnp.where(same, second, first))
        for j in range(rows_here):
            bias_scratch[pl.ds((block * rows_here + j) * heads, heads), :] = jnp.where(
                lane < cols_here,
                segment(mine, j * cols_here, 0),
                segment(other, j * cols_here, cols_here),
            )
    penalty = penalty[:, :residues]
    head_bias = [
        bias_scratch[pl.ds(h, cols_here, stride=heads), :][:, :residues] + penalty
        for h in range(heads)
    ]
    head_bias = jnp.concatenate(head_bias, axis=0)
    head_of = lax.broadcasted_iota(jnp.int32, (cols_here, width), 1) // (width // heads)
    ones = jnp.ones((residues, width), bf16)
    chunk = rows_here // chunks
    copies = []
    for c in range(chunks):
        gated = []
        for i in range(c * chunk, (c + 1) * chunk):
            v = jnp.concatenate([v_ref[i], v_far_ref[i]], axis=0)
            scores = scores_ref[i] + head_bias
            raised = jnp.exp(scores - jnp.max(scores, axis=-1, keepdims=True)).astype(bf16)
            mixed = dot_nn(raised, jnp.concatenate([v, ones], axis=1))
            attended = mixed[:cols_here]
            for h in range(1, heads):
                part = mixed[h * cols_here : (h + 1) * cols_here]
                attended = jnp.where(jnp.tile(head_of, (1, 2)) == h, part, attended)
            attended = attended[:, :width] / attended[:, width:]
            gated.append((attended * gate_ref[i]).astype(bf16))
        update = dot_nn(jnp.concatenate(gated, axis=0), out_w_ref[...])
        at = slice(c * chunk, (c + 1) * chunk)
        result[at] = mid_ref[at] + update.reshape(chunk, cols_here, width)
        copies.append(pltpu.make_async_copy(result.at[at], out_ref.at[at], done.at[c]))
        copies[-1].start()
    for copy in copies:
        copy.wait()


def body_channels(
    pair,
    residue_mask,
    tri_norm_gain,
    tri_in_weight,
    tri_gate_weight,
    tri_out_norm_gain,
    tri_out_weight,
    att_norm_gain,
    att_proj_weight,
    att_bias_weight,
    att_out_weight,
):
    rows_here, cols_here, chan = pair.shape
    rows, cols = lax.axis_size("row"), lax.axis_size(("col", "sub"))
    group = ("row", "col", "sub")
    devices = rows * cols
    residues = cols_here * cols
    cells = rows_here * cols_here
    hidden = tri_in_weight.shape[2]
    own = hidden // devices
    heads = att_bias_weight.shape[1]
    tiles = -(-cells // LANES)
    lr_panels = -(-2 * cells // LANES) if (-cells) % LANES * 2 == LANES else 2 * tiles
    flat = pair.reshape(cells, chan)
    live = residue_mask.reshape(1, residues)

    lr, normed, vectors = pl.pallas_call(
        functools.partial(factors_kernel, devices),
        out_shape=(
            pltpu.VMEM((devices, lr_panels, own, LANES), bf16),
            pltpu.VMEM((cells, chan), bf16),
            pltpu.VMEM((8, LANES), f32),
        ),
        scratch_shapes=[pltpu.VMEM((chan * tri_in_weight.shape[1], hidden), f32)],
        compiler_params=kernel_params,
        name="factors",
    )(
        *map(
            afar,
            (
                flat,
                tri_norm_gain.reshape(1, chan),
                tri_in_weight,
                live,
                tri_out_norm_gain.reshape(1, hidden),
                att_norm_gain.reshape(1, chan),
            ),
        )
    )
    lr = lax.all_to_all(lr, group, 0, 0, tiled=True)
    sums = pl.pallas_call(
        functools.partial(triangle_kernel, rows_here, cols_here),
        out_shape=pltpu.VMEM((devices, tiles, own, LANES), bf16),
        scratch_shapes=[pltpu.VMEM((residues * own, LANES), f32) for _ in range(3)],
        compiler_params=kernel_params,
        name="triangle",
    )(near(vectors), near(lr))
    sums = lax.all_to_all(sums, group, 0, 0, tiled=True)
    shape = (rows_here, cols_here, chan)
    chunks = math.gcd(rows_here, 3)
    mid, att, bias = pl.pallas_call(
        middle_kernel,
        out_shape=(
            pltpu.VMEM((cells, chan), f32),
            pltpu.VMEM((cells, chan), bf16),
            pltpu.VMEM((1, heads, cells), bf16),
        ),
        compiler_params=kernel_params,
        name="middle",
    )(
        *map(
            near,
            (
                flat,
                normed,
                sums,
                vectors,
                tri_out_weight,
                tri_gate_weight,
                att_bias_weight.T,
            ),
        )
    )
    att, mid = att.reshape(shape), mid.reshape(shape)

    def swap(v):
        return lax.ppermute(v, "row", [(r, r ^ 1) for r in range(rows)])

    joined = swap(bias)
    bias = jnp.concatenate([bias, joined], axis=0)
    fetched = []
    for p in range(2):
        pairs = []
        for z in range(rows // 2):
            for s in range(2):
                for x in range(cols):
                    half = z >> 1
                    target = (2 * ((z & 1) ^ 1 ^ p) + (s ^ half)) * 2 + (x ^ half)
                    pairs.append(((2 * z + s) * cols + x, target * cols + half))
        fetched.append(lax.ppermute(bias, group, pairs))
    far = lax.ppermute(att, ("col", "sub"), [(c, c ^ 1) for c in range(cols)])
    queries, keys, values, gate, kv_weight = pl.pallas_call(
        functools.partial(own_kernel, heads),
        out_shape=(
            pltpu.VMEM(shape, bf16),
            pltpu.VMEM(shape, bf16),
            pltpu.VMEM(shape, bf16),
            pltpu.VMEM(shape, f32),
            pltpu.VMEM((2, chan, chan), bf16),
        ),
        scratch_shapes=[pltpu.VMEM((chan * att_proj_weight.shape[1], chan), f32)],
        compiler_params=kernel_params,
        name="own",
    )(near(att), near(att_proj_weight))
    fetched = jnp.concatenate(fetched, axis=0)
    swapped = swap(fetched)
    scores, values_far = pl.pallas_call(
        functools.partial(scores_kernel, heads),
        out_shape=(
            pltpu.VMEM((rows_here, heads * cols_here, residues), f32),
            pltpu.VMEM(shape, bf16),
        ),
        compiler_params=kernel_params,
        name="scores",
    )(*map(near, (queries, keys, far, kv_weight)))
    return pl.pallas_call(
        attention_kernel,
        out_shape=jax.ShapeDtypeStruct(shape, f32),
        out_specs=pl.BlockSpec(memory_space=pltpu.HBM),
        scratch_shapes=[
            pltpu.VMEM((cols_here * heads, LANES), f32),
            pltpu.VMEM(shape, f32),
            pltpu.SemaphoreType.DMA((chunks,)),
        ],
        compiler_params=kernel_params,
        name="attention",
    )(*map(near, (vectors, fetched, swapped, scores, values, values_far, gate, mid, att_out_weight)))


def solution(mesh):
    placed = (
        P(("parts", "row"), ("col", "sub"), None),
        P("parts"),
        P(),
        P(),
        P(),
        P(),
        P(),
        P(),
        P(),
        P(),
        P(),
    )

    def body(pair, residue_mask, tri_norm_gain, tri_in_weight, *others):
        rows, cols = mesh.shape["row"], mesh.shape["col"] * mesh.shape["sub"]
        hidden = tri_in_weight.shape[2]
        fits = (
            cols == 2
            and rows == 8
            and hidden % (8 * rows * cols) == 0
            and hidden == pair.shape[2] == LANES
            and residue_mask.shape[0] <= LANES
            and pair.shape[0] * cols * pair.shape[1] % 16 == 0
        )
        chosen = body_channels if fits else body_general
        return chosen(pair, residue_mask, tri_norm_gain, tri_in_weight, *others)

    return jax.shard_map(
        body,
        mesh=mesh,
        in_specs=placed,
        out_specs=P(("parts", "row"), ("col", "sub"), None),
        check_vma=False,
    )
```

```python
import functools
import math

import jax
import jax.numpy as jnp
from jax import lax
from jax.experimental import pallas as pl
from jax.experimental.pallas import tpu as pltpu
from jax.sharding import PartitionSpec as P


epsilon = 1e-05
mask_penalty = 1000000000.0
LANES = 128
f32 = jnp.float32
bf16 = jnp.bfloat16


def norm_last(values_in, gain):
    center = jnp.mean(values_in, axis=-1, keepdims=True)
    centered = values_in - center
    variance = jnp.mean(centered * centered, axis=-1, keepdims=True)
    return centered * lax.rsqrt(variance + epsilon) * gain


def sigmoid(v):
    return 0.5 * jnp.tanh(0.5 * v) + 0.5


def project(normed, weight):
    flat_rows = normed.reshape(-1, normed.shape[-1])
    product = jnp.dot(flat_rows, weight, preferred_element_type=jnp.float32)
    return product.reshape(normed.shape[:-1] + (weight.shape[1],))


def body_general(
    pair,
    residue_mask,
    tri_norm_gain,
    tri_in_weight,
    tri_gate_weight,
    tri_out_norm_gain,
    tri_out_weight,
    att_norm_gain,
    att_proj_weight,
    att_bias_weight,
    att_out_weight,
):
    rows_here, cols_here, _ = pair.shape
    residues = cols_here * lax.axis_size(("col", "sub"))
    row_offset = lax.axis_index("row") * rows_here
    col_offset = lax.axis_index(("col", "sub")) * cols_here
    residue_live = residue_mask.astype(jnp.float32)
    live_rows = lax.dynamic_slice_in_dim(residue_live, row_offset, rows_here)
    live_cols = lax.dynamic_slice_in_dim(residue_live, col_offset, cols_here)
    pair_live = (live_rows[:, None] * live_cols[None, :])[:, :, None]
    tri_normed = norm_last(pair, tri_norm_gain).astype(jnp.bfloat16)
    in_width = tri_in_weight.shape[2]
    projected = project(tri_normed, tri_in_weight.reshape(tri_in_weight.shape[0], -1)).reshape(
        rows_here, cols_here, 4, in_width
    )
    left_factor = (jax.nn.sigmoid(projected[:, :, 0]) * projected[:, :, 1] * pair_live).astype(
        jnp.bfloat16
    )
    right_factor = (jax.nn.sigmoid(projected[:, :, 2]) * projected[:, :, 3] * pair_live).astype(
        jnp.bfloat16
    )
    left_all, right_all = (
        lax.all_gather(left_factor, ("col", "sub"), axis=1, tiled=True),
        lax.all_gather(right_factor, ("col", "sub"), axis=1, tiled=True),
    )
    exchanged = lax.all_to_all(right_all, "row", split_axis=1, concat_axis=0, tiled=True)
    own_rows = lax.dynamic_slice_in_dim(exchanged, col_offset, cols_here, 0)
    tri_sum = jnp.einsum(
        "ikh,jkh->ijh",
        left_all,
        lax.all_gather(own_rows, "row", axis=1, tiled=True),
        preferred_element_type=jnp.float32,
    )
    hidden_normed = norm_last(tri_sum, tri_out_norm_gain).astype(jnp.bfloat16)
    tri_gate = jax.nn.sigmoid(project(tri_normed, tri_gate_weight))
    pair_mid = pair + tri_gate * project(hidden_normed, tri_out_weight)
    att_normed = norm_last(pair_mid, att_norm_gain).astype(jnp.bfloat16)
    head_width = att_proj_weight.shape[2]
    heads_here = att_bias_weight.shape[1]
    head_size = head_width // heads_here
    projected = project(att_normed, att_proj_weight.reshape(att_proj_weight.shape[0], -1)).reshape(
        rows_here, cols_here, 4, head_width
    )
    queries = (projected[:, :, 0] * head_size ** (-0.5)).astype(jnp.bfloat16)
    key_rows = projected[:, :, 1].astype(jnp.bfloat16)
    value_rows = projected[:, :, 2].astype(jnp.bfloat16)
    att_gate = jax.nn.sigmoid(projected[:, :, 3])
    pair_bias = project(att_normed, att_bias_weight).astype(jnp.bfloat16)
    key_all, value_all = (
        lax.all_gather(key_rows, ("col", "sub"), axis=1, tiled=True),
        lax.all_gather(value_rows, ("col", "sub"), axis=1, tiled=True),
    )
    bias_all_rows = lax.all_gather(pair_bias, "row", axis=0, tiled=True)
    bias_panel = lax.all_to_all(
        bias_all_rows, ("col", "sub"), split_axis=0, concat_axis=1, tiled=True
    )
    mask_row = (residue_live - 1.0) * mask_penalty
    head_bias = jnp.transpose(bias_panel.astype(jnp.float32), (2, 0, 1)) + mask_row[None, None, :]
    block_rows = math.gcd(rows_here, max(1, 512 // cols_here))
    blocks = rows_here // block_rows

    def attend(block_items):
        query_block, key_block, value_block = block_items
        scores = (
            jnp.einsum(
                "ijhd,ikhd->ihjk", query_block, key_block, preferred_element_type=jnp.float32
            )
            + head_bias[None]
        )
        row_max = jnp.max(scores, axis=-1, keepdims=True)
        raised = jnp.exp(scores - row_max)
        weights = (raised / jnp.sum(raised, axis=-1, keepdims=True)).astype(jnp.bfloat16)
        return jnp.einsum(
            "ihjk,ikhd->ijhd", weights, value_block, preferred_element_type=jnp.float32
        )

    attended = lax.map(
        attend,
        (
            queries.reshape(blocks, block_rows, cols_here, heads_here, head_size),
            key_all.reshape(blocks, block_rows, residues, heads_here, head_size),
            value_all.reshape(blocks, block_rows, residues, heads_here, head_size),
        ),
    )
    gated = (attended.reshape(rows_here, cols_here, head_width) * att_gate).astype(jnp.bfloat16)
    return pair_mid + project(gated, att_out_weight)


def dot_nn(a, b):
    return lax.dot_general(a, b, (((1,), (0,)), ((), ())), preferred_element_type=f32)


def dot_nt(a, b):
    return lax.dot_general(a, b, (((1,), (1,)), ((), ())), preferred_element_type=f32)


kernel_params = pltpu.CompilerParams(vmem_limit_bytes=16 << 20)


def near(v):
    return pltpu.with_memory_space_constraint(v, pltpu.VMEM)


def afar(v):
    return pltpu.with_memory_space_constraint(v, pltpu.HBM)


def split_weight(w_ref, w_scratch):
    rows, mats, out = w_ref.shape
    w_scratch[...] = w_ref[...].astype(f32).reshape(rows * mats, out)
    return [w_scratch[pl.ds(p, rows, stride=mats), :] for p in range(mats)]


def factors_kernel(
    devices,
    pair_ref,
    gain_ref,
    w_ref,
    live_ref,
    out_gain_ref,
    att_gain_ref,
    lr_ref,
    normed_ref,
    rows_ref,
    w_scratch,
):
    cells, _ = pair_ref.shape
    live = live_ref[...].astype(f32)
    rows_ref[0:1] = jnp.concatenate([live, jnp.zeros((1, LANES - live.shape[1]), f32)], axis=1)
    rows_ref[1:2] = out_gain_ref[...]
    rows_ref[2:3] = att_gain_ref[...]
    hidden = w_ref.shape[2]
    own = hidden // devices
    normed = norm_last(pair_ref[...], gain_ref[...]).astype(bf16)
    normed_ref[...] = normed
    w_t = [jnp.transpose(w).astype(bf16) for w in split_weight(w_ref, w_scratch)]
    spare = (-cells) % LANES
    tiles = (cells + spare) // LANES
    if spare:
        tail = normed[:spare]
        rhs_left = jnp.concatenate([normed, tail], axis=0)
        rhs_right = jnp.concatenate([tail, normed], axis=0)
    else:
        rhs_left = rhs_right = normed
    left = sigmoid(dot_nt(w_t[0], rhs_left)) * dot_nt(w_t[1], rhs_left)
    right = sigmoid(dot_nt(w_t[2], rhs_right)) * dot_nt(w_t[3], rhs_right)
    panels = [left[:, t * LANES : (t + 1) * LANES] for t in range(tiles)]
    right_panels = [right[:, t * LANES : (t + 1) * LANES] for t in range(tiles)]
    if spare:
        lane = lax.broadcasted_iota(jnp.int32, (hidden, LANES), 1)
        panels[-1] = jnp.where(lane < LANES - spare, panels[-1], right_panels[0])
        panels += right_panels[1:]
    else:
        panels += right_panels
    for t, panel in enumerate(panels):
        lr_ref[:, t] = panel.reshape(devices, own, LANES).astype(bf16)


def segment(panels, start, target):
    tile, at = divmod(start, LANES)
    here = panels[tile]
    if at and tile + 1 < len(panels):
        lane = lax.broadcasted_iota(jnp.int32, here.shape, 1)
        here = jnp.where(lane >= at, here, panels[tile + 1])
    shift = (target - at) % LANES
    return pltpu.roll(here, shift, 1) if shift else here


def triangle_kernel(
    rows_here, cols_here, vectors_ref, lr_ref, sum_ref, left_scratch, right_scratch, sum_scratch
):
    _, panels_in, own, _ = lr_ref.shape
    residues = left_scratch.shape[0] // own
    cols = residues // cols_here
    rows = residues // rows_here
    cells = rows_here * cols_here
    lane = lax.broadcasted_iota(jnp.int32, (own, LANES), 1)
    for r in range(rows):
        parts = [
            [lr_ref[r * cols + c, t].astype(f32) for t in range(panels_in)] for c in range(cols)
        ]
        for side, scratch in ((0, left_scratch), (1, right_scratch)):
            for i in range(rows_here):
                start = side * cells + i * cols_here
                line = segment(parts[0], start, 0)
                for c in range(1, cols):
                    moved = segment(parts[c], start, c * cols_here)
                    line = jnp.where(lane < c * cols_here, line, moved)
                scratch[pl.ds((r * rows_here + i) * own, own), :] = line
    live_wide = vectors_ref[0:1]
    live_square = jnp.broadcast_to(live_wide, (LANES, LANES))
    both = live_square * jnp.transpose(live_square)
    both = both[:residues]
    keep = live_wide > 0
    for h in range(own):
        left = jnp.where(keep, left_scratch[pl.ds(h, residues, stride=own), :], 0.0).astype(bf16)
        right = jnp.where(keep, right_scratch[pl.ds(h, residues, stride=own), :], 0.0).astype(bf16)
        right = jnp.concatenate([right, jnp.zeros((LANES - residues, LANES), bf16)], axis=0)
        sum_scratch[pl.ds(h, residues, stride=own), :] = dot_nt(left, right) * both
    tiles = sum_ref.shape[1]
    for r in range(rows):
        lines = [
            sum_scratch[pl.ds((r * rows_here + i) * own, own), :] for i in range(rows_here)
        ]
        for c in range(cols):
            for t in range(tiles):
                panel = None
                for i in range(rows_here):
                    low, high = i * cols_here - t * LANES, (i + 1) * cols_here - t * LANES
                    if high <= 0 or low >= LANES:
                        continue
                    shift = (low - c * cols_here) % LANES
                    line = pltpu.roll(lines[i], shift, 1) if shift else lines[i]
                    panel = line if panel is None else jnp.where(lane >= low, line, panel)
                sum_ref[r * cols + c, t] = panel.astype(bf16)


def middle_kernel(
    pair_ref,
    normed_ref,
    sum_ref,
    vectors_ref,
    out_w_ref,
    gate_w_ref,
    bias_w_ref,
    mid_ref,
    att_ref,
    bias_ref,
):
    devices, tiles, own, _ = sum_ref.shape
    cells, _ = pair_ref.shape
    hidden = devices * own
    gain_col = jnp.transpose(jnp.broadcast_to(vectors_ref[1:2], (LANES, hidden)))
    gate = sigmoid(dot_nn(normed_ref[...], gate_w_ref[...]))
    bias_w = bias_w_ref[...]
    hidden_rows = []
    for t in range(tiles):
        total = sum_ref[:, t].astype(f32).reshape(hidden, LANES)
        center = jnp.mean(total, axis=0, keepdims=True)
        centered = total - center
        variance = jnp.mean(centered * centered, axis=0, keepdims=True)
        hidden_normed = centered * lax.rsqrt(variance + epsilon) * gain_col
        hidden_rows.append(jnp.transpose(hidden_normed).astype(bf16))
    hidden_rows = jnp.concatenate(hidden_rows, axis=0)[:cells]
    mid = pair_ref[...] + gate * dot_nn(hidden_rows, out_w_ref[...])
    mid_ref[...] = mid
    att = norm_last(mid, vectors_ref[2:3]).astype(bf16)
    att_ref[...] = att
    bias_ref[0] = dot_nt(bias_w, att).astype(bf16)


def own_kernel(heads, att_ref, w_ref, q_ref, k_ref, v_ref, gate_ref, kv_w_ref, w_scratch):
    rows_here, cols_here, chan = att_ref.shape
    width = w_ref.shape[2]
    shape = (rows_here, cols_here, width)
    att = att_ref[...].reshape(rows_here * cols_here, chan)
    w = [m.astype(bf16) for m in split_weight(w_ref, w_scratch)]
    kv_w_ref[0], kv_w_ref[1] = w[1], w[2]
    q_ref[...] = (dot_nn(att, w[0]) * (width // heads) ** (-0.5)).astype(bf16).reshape(shape)
    k_ref[...] = dot_nn(att, w[1]).astype(bf16).reshape(shape)
    v_ref[...] = dot_nn(att, w[2]).astype(bf16).reshape(shape)
    gate_ref[...] = sigmoid(dot_nn(att, w[3])).reshape(shape)


def fetch_plan():
    trips, codes = ([], []), [0] * 16
    for h in range(2):
        for x in range(2):
            for p in range(2):
                for b in range(2):
                    chips = [t for t in range(4) if (t in FIRST[h][x]) == (b == p)]
                    for n, target in enumerate(chips):
                        source_core = n ^ TURNED[2 * h + b][x][p]
                        core = x ^ (target in SWAPPED[h])
                        source = ((2 * h + b) * 2 + source_core) * 2 + x
                        device = (target * 2 + core) * 2 + h
                        trips[p].append((source, device))
                        codes[device] |= (b if p == 0 else 0) | source_core << (1 + p)
                        codes[device] |= (x == h) << 3
    return trips, codes


FIRST = (((1, 3), (2, 3)), ((2, 3), (2, 3)))
SWAPPED = ((), (0, 1, 3))
TURNED = (((1, 0), (1, 1)), ((1, 0), (1, 0)), ((0, 1), (0, 1)), ((0, 0), (0, 1)))


def fetch_code(codes, row, col):
    index = row * 2 + col
    code = jnp.int32(0)
    for device, entry in enumerate(codes):
        code = jnp.where(index == device, jnp.int32(entry), code)
    return [jnp.bitwise_and(lax.shift_right_logical(code, jnp.int32(n)), 1) for n in range(4)]


def head_bias_half(ref, scratch, rows_here, cols_here, code, target):
    blocks, heads, cells = ref.shape
    first, *cores, _ = code
    pad = (-cells) % LANES
    for m in range(blocks):
        p, n = m // 2, m % 2
        block = 2 * jnp.bitwise_xor(first, p) + jnp.bitwise_xor(n, cores[p])
        v = ref[m].astype(f32)
        v = jnp.concatenate([v, jnp.zeros((heads, pad), f32)], axis=1) if pad else v
        panels = [v[:, t * LANES : (t + 1) * LANES] for t in range((cells + pad) // LANES)]
        for j in range(rows_here):
            line = segment(panels, j * cols_here, target)
            scratch[pl.ds((block * rows_here + j) * heads, heads), :] = line
    return jnp.concatenate(
        [scratch[pl.ds(h, cols_here, stride=heads), :] for h in range(heads)], axis=0
    )


def scores_kernel(
    codes,
    vectors_ref,
    fetched_ref,
    q_ref,
    k_ref,
    far_ref,
    v_ref,
    kv_w_ref,
    scores_ref,
    v_all_ref,
    bias_ref,
    bias_scratch,
):
    rows_here, cols_here, width = q_ref.shape
    heads = fetched_ref.shape[1]
    far = far_ref[...].reshape(rows_here * cols_here, width)
    k_far = dot_nn(far, kv_w_ref[0]).astype(bf16).reshape(q_ref.shape)
    v_far = dot_nn(far, kv_w_ref[1]).astype(bf16).reshape(q_ref.shape)
    row, col = lax.axis_index("row"), lax.axis_index(("col", "sub"))
    code = fetch_code(codes, row, col)
    own_first = code[3] == 1

    def in_order(own, other):
        return jnp.concatenate(
            [jnp.where(own_first, own, other), jnp.where(own_first, other, own)], axis=0
        )

    head_of = lax.broadcasted_iota(jnp.int32, (cols_here, width), 1) // (width // heads)
    for i in range(rows_here):
        q = q_ref[i]
        q_heads = jnp.concatenate(
            [jnp.where(head_of == h, q, jnp.zeros_like(q)) for h in range(heads)], axis=0
        )
        scores_ref[i] = dot_nt(q_heads, in_order(k_ref[i], k_far[i]))
        v_all_ref[i] = in_order(v_ref[i], v_far[i])
    lane_row = lax.broadcasted_iota(jnp.int32, (1, LANES), 1)
    live = vectors_ref[0:1]
    swapped = jnp.where(
        lane_row < cols_here,
        pltpu.roll(live, LANES - cols_here, 1),
        pltpu.roll(live, cols_here, 1),
    )
    natural = (col == 0) == own_first
    penalty = (jnp.where(natural, live, swapped) - 1.0) * mask_penalty
    half = head_bias_half(fetched_ref, bias_scratch, rows_here, cols_here, code, 0)
    bias_ref[...] = jnp.where(lane_row < cols_here, half, 0.0) + penalty


def attention_kernel(
    codes,
    bias_ref,
    swapped_ref,
    scores_ref,
    v_all_ref,
    gate_ref,
    mid_ref,
    out_w_ref,
    out_ref,
    bias_scratch,
    result,
    done,
):
    rows_here, cols_here, width = gate_ref.shape
    chunks = done.shape[0]
    heads = swapped_ref.shape[1]
    residues = 2 * cols_here
    row, col = lax.axis_index("row"), lax.axis_index(("col", "sub"))
    code = fetch_code(codes, jnp.bitwise_xor(row, 1), col)
    half = head_bias_half(swapped_ref, bias_scratch, rows_here, cols_here, code, cols_here)
    lane_row = lax.broadcasted_iota(jnp.int32, (1, LANES), 1)
    head_bias = (bias_ref[...] + jnp.where(lane_row < cols_here, 0.0, half))[:, :residues]
    head_of = lax.broadcasted_iota(jnp.int32, (cols_here, width), 1) // (width // heads)
    ones = jnp.ones((residues, width), bf16)
    chunk = rows_here // chunks
    copies = []
    for c in range(chunks):
        gated = []
        for i in range(c * chunk, (c + 1) * chunk):
            scores = scores_ref[i] + head_bias
            raised = jnp.exp(scores - jnp.max(scores, axis=-1, keepdims=True)).astype(bf16)
            mixed = dot_nn(raised, jnp.concatenate([v_all_ref[i], ones], axis=1))
            attended = mixed[:cols_here]
            for h in range(1, heads):
                part = mixed[h * cols_here : (h + 1) * cols_here]
                attended = jnp.where(jnp.tile(head_of, (1, 2)) == h, part, attended)
            attended = attended[:, :width] / attended[:, width:]
            gated.append((attended * gate_ref[i]).astype(bf16))
        update = dot_nn(jnp.concatenate(gated, axis=0), out_w_ref[...])
        at = slice(c * chunk, (c + 1) * chunk)
        result[at] = mid_ref[at] + update.reshape(chunk, cols_here, width)
        copies.append(pltpu.make_async_copy(result.at[at], out_ref.at[at], done.at[c]))
        copies[-1].start()
    for copy in copies:
        copy.wait()


def body_channels(
    pair,
    residue_mask,
    tri_norm_gain,
    tri_in_weight,
    tri_gate_weight,
    tri_out_norm_gain,
    tri_out_weight,
    att_norm_gain,
    att_proj_weight,
    att_bias_weight,
    att_out_weight,
):
    rows_here, cols_here, chan = pair.shape
    rows, cols = lax.axis_size("row"), lax.axis_size(("col", "sub"))
    group = ("row", "col", "sub")
    devices = rows * cols
    residues = cols_here * cols
    cells = rows_here * cols_here
    hidden = tri_in_weight.shape[2]
    own = hidden // devices
    heads = att_bias_weight.shape[1]
    tiles = -(-cells // LANES)
    lr_panels = -(-2 * cells // LANES) if (-cells) % LANES * 2 == LANES else 2 * tiles
    flat = pair.reshape(cells, chan)
    live = residue_mask.reshape(1, residues)

    lr, normed, vectors = pl.pallas_call(
        functools.partial(factors_kernel, devices),
        out_shape=(
            pltpu.VMEM((devices, lr_panels, own, LANES), bf16),
            pltpu.VMEM((cells, chan), bf16),
            pltpu.VMEM((8, LANES), f32),
        ),
        scratch_shapes=[pltpu.VMEM((chan * tri_in_weight.shape[1], hidden), f32)],
        compiler_params=kernel_params,
        name="factors",
    )(
        *map(
            afar,
            (
                flat,
                tri_norm_gain.reshape(1, chan),
                tri_in_weight,
                live,
                tri_out_norm_gain.reshape(1, hidden),
                att_norm_gain.reshape(1, chan),
            ),
        )
    )
    lr = lax.all_to_all(lr, group, 0, 0, tiled=True)
    sums = pl.pallas_call(
        functools.partial(triangle_kernel, rows_here, cols_here),
        out_shape=pltpu.VMEM((devices, tiles, own, LANES), bf16),
        scratch_shapes=[pltpu.VMEM((residues * own, LANES), f32) for _ in range(3)],
        compiler_params=kernel_params,
        name="triangle",
    )(near(vectors), near(lr))
    sums = lax.all_to_all(sums, group, 0, 0, tiled=True)
    shape = (rows_here, cols_here, chan)
    chunks = math.gcd(rows_here, 3)
    mid, att, bias = pl.pallas_call(
        middle_kernel,
        out_shape=(
            pltpu.VMEM((cells, chan), f32),
            pltpu.VMEM((cells, chan), bf16),
            pltpu.VMEM((1, heads, cells), bf16),
        ),
        compiler_params=kernel_params,
        name="middle",
    )(
        *map(
            near,
            (
                flat,
                normed,
                sums,
                vectors,
                tri_out_weight,
                tri_gate_weight,
                att_bias_weight.T,
            ),
        )
    )
    att, mid = att.reshape(shape), mid.reshape(shape)

    def swap(v):
        return lax.ppermute(v, "row", [(r, r ^ 1) for r in range(rows)])

    trips, codes = fetch_plan()
    joined = swap(bias)
    bias = jnp.concatenate([bias, joined], axis=0)
    fetched = []
    for p in range(2):
        fetched.append(lax.ppermute(bias, group, trips[p]))
    far = lax.ppermute(att, ("col", "sub"), [(c, c ^ 1) for c in range(cols)])
    queries, keys, values, gate, kv_weight = pl.pallas_call(
        functools.partial(own_kernel, heads),
        out_shape=(
            pltpu.VMEM(shape, bf16),
            pltpu.VMEM(shape, bf16),
            pltpu.VMEM(shape, bf16),
            pltpu.VMEM(shape, f32),
            pltpu.VMEM((2, chan, chan), bf16),
        ),
        scratch_shapes=[pltpu.VMEM((chan * att_proj_weight.shape[1], chan), f32)],
        compiler_params=kernel_params,
        name="own",
    )(near(att), near(att_proj_weight))
    fetched = jnp.concatenate(fetched, axis=0)
    swapped = swap(fetched)
    scores, values, bias = pl.pallas_call(
        functools.partial(scores_kernel, codes),
        out_shape=(
            pltpu.VMEM((rows_here, heads * cols_here, residues), f32),
            pltpu.VMEM((rows_here, residues, chan), bf16),
            pltpu.VMEM((heads * cols_here, LANES), f32),
        ),
        scratch_shapes=[pltpu.VMEM((cols_here * heads, LANES), f32)],
        compiler_params=kernel_params,
        name="scores",
    )(*map(near, (vectors, fetched, queries, keys, far, values, kv_weight)))
    return pl.pallas_call(
        functools.partial(attention_kernel, codes),
        out_shape=jax.ShapeDtypeStruct(shape, f32),
        out_specs=pl.BlockSpec(memory_space=pltpu.HBM),
        scratch_shapes=[
            pltpu.VMEM((cols_here * heads, LANES), f32),
            pltpu.VMEM(shape, f32),
            pltpu.SemaphoreType.DMA((chunks,)),
        ],
        compiler_params=kernel_params,
        name="attention",
    )(*map(near, (bias, swapped, scores, values, gate, mid, att_out_weight)))


def solution(mesh):
    placed = (
        P(("parts", "row"), ("col", "sub"), None),
        P("parts"),
        P(),
        P(),
        P(),
        P(),
        P(),
        P(),
        P(),
        P(),
        P(),
    )

    def body(pair, residue_mask, tri_norm_gain, tri_in_weight, *others):
        rows, cols = mesh.shape["row"], mesh.shape["col"] * mesh.shape["sub"]
        hidden = tri_in_weight.shape[2]
        fits = (
            cols == 2
            and rows == 8
            and hidden % (8 * rows * cols) == 0
            and hidden == pair.shape[2] == LANES
            and residue_mask.shape[0] <= LANES
            and pair.shape[0] * cols * pair.shape[1] % 16 == 0
        )
        chosen = body_channels if fits else body_general
        return chosen(pair, residue_mask, tri_norm_gain, tri_in_weight, *others)

    return jax.shard_map(
        body,
        mesh=mesh,
        in_specs=placed,
        out_specs=P(("parts", "row"), ("col", "sub"), None),
        check_vma=False,
    )
```

```python
import functools
import math

import jax
import jax.numpy as jnp
from jax import lax
from jax.experimental import pallas as pl
from jax.experimental.pallas import tpu as pltpu
from jax.sharding import PartitionSpec as P


epsilon = 1e-05
mask_penalty = 1000000000.0
LANES = 128
f32 = jnp.float32
bf16 = jnp.bfloat16


def norm_last(values_in, gain):
    center = jnp.mean(values_in, axis=-1, keepdims=True)
    centered = values_in - center
    variance = jnp.mean(centered * centered, axis=-1, keepdims=True)
    return centered * lax.rsqrt(variance + epsilon) * gain


def sigmoid(v):
    return 0.5 * jnp.tanh(0.5 * v) + 0.5


def project(normed, weight):
    flat_rows = normed.reshape(-1, normed.shape[-1])
    product = jnp.dot(flat_rows, weight, preferred_element_type=jnp.float32)
    return product.reshape(normed.shape[:-1] + (weight.shape[1],))


def body_general(
    pair,
    residue_mask,
    tri_norm_gain,
    tri_in_weight,
    tri_gate_weight,
    tri_out_norm_gain,
    tri_out_weight,
    att_norm_gain,
    att_proj_weight,
    att_bias_weight,
    att_out_weight,
):
    rows_here, cols_here, _ = pair.shape
    residues = cols_here * lax.axis_size(("col", "sub"))
    row_offset = lax.axis_index("row") * rows_here
    col_offset = lax.axis_index(("col", "sub")) * cols_here
    residue_live = residue_mask.astype(jnp.float32)
    live_rows = lax.dynamic_slice_in_dim(residue_live, row_offset, rows_here)
    live_cols = lax.dynamic_slice_in_dim(residue_live, col_offset, cols_here)
    pair_live = (live_rows[:, None] * live_cols[None, :])[:, :, None]
    tri_normed = norm_last(pair, tri_norm_gain).astype(jnp.bfloat16)
    in_width = tri_in_weight.shape[2]
    projected = project(tri_normed, tri_in_weight.reshape(tri_in_weight.shape[0], -1)).reshape(
        rows_here, cols_here, 4, in_width
    )
    left_factor = (jax.nn.sigmoid(projected[:, :, 0]) * projected[:, :, 1] * pair_live).astype(
        jnp.bfloat16
    )
    right_factor = (jax.nn.sigmoid(projected[:, :, 2]) * projected[:, :, 3] * pair_live).astype(
        jnp.bfloat16
    )
    left_all, right_all = (
        lax.all_gather(left_factor, ("col", "sub"), axis=1, tiled=True),
        lax.all_gather(right_factor, ("col", "sub"), axis=1, tiled=True),
    )
    exchanged = lax.all_to_all(right_all, "row", split_axis=1, concat_axis=0, tiled=True)
    own_rows = lax.dynamic_slice_in_dim(exchanged, col_offset, cols_here, 0)
    tri_sum = jnp.einsum(
        "ikh,jkh->ijh",
        left_all,
        lax.all_gather(own_rows, "row", axis=1, tiled=True),
        preferred_element_type=jnp.float32,
    )
    hidden_normed = norm_last(tri_sum, tri_out_norm_gain).astype(jnp.bfloat16)
    tri_gate = jax.nn.sigmoid(project(tri_normed, tri_gate_weight))
    pair_mid = pair + tri_gate * project(hidden_normed, tri_out_weight)
    att_normed = norm_last(pair_mid, att_norm_gain).astype(jnp.bfloat16)
    head_width = att_proj_weight.shape[2]
    heads_here = att_bias_weight.shape[1]
    head_size = head_width // heads_here
    projected = project(att_normed, att_proj_weight.reshape(att_proj_weight.shape[0], -1)).reshape(
        rows_here, cols_here, 4, head_width
    )
    queries = (projected[:, :, 0] * head_size ** (-0.5)).astype(jnp.bfloat16)
    key_rows = projected[:, :, 1].astype(jnp.bfloat16)
    value_rows = projected[:, :, 2].astype(jnp.bfloat16)
    att_gate = jax.nn.sigmoid(projected[:, :, 3])
    pair_bias = project(att_normed, att_bias_weight).astype(jnp.bfloat16)
    key_all, value_all = (
        lax.all_gather(key_rows, ("col", "sub"), axis=1, tiled=True),
        lax.all_gather(value_rows, ("col", "sub"), axis=1, tiled=True),
    )
    bias_all_rows = lax.all_gather(pair_bias, "row", axis=0, tiled=True)
    bias_panel = lax.all_to_all(
        bias_all_rows, ("col", "sub"), split_axis=0, concat_axis=1, tiled=True
    )
    mask_row = (residue_live - 1.0) * mask_penalty
    head_bias = jnp.transpose(bias_panel.astype(jnp.float32), (2, 0, 1)) + mask_row[None, None, :]
    block_rows = math.gcd(rows_here, max(1, 512 // cols_here))
    blocks = rows_here // block_rows

    def attend(block_items):
        query_block, key_block, value_block = block_items
        scores = (
            jnp.einsum(
                "ijhd,ikhd->ihjk", query_block, key_block, preferred_element_type=jnp.float32
            )
            + head_bias[None]
        )
        row_max = jnp.max(scores, axis=-1, keepdims=True)
        raised = jnp.exp(scores - row_max)
        weights = (raised / jnp.sum(raised, axis=-1, keepdims=True)).astype(jnp.bfloat16)
        return jnp.einsum(
            "ihjk,ikhd->ijhd", weights, value_block, preferred_element_type=jnp.float32
        )

    attended = lax.map(
        attend,
        (
            queries.reshape(blocks, block_rows, cols_here, heads_here, head_size),
            key_all.reshape(blocks, block_rows, residues, heads_here, head_size),
            value_all.reshape(blocks, block_rows, residues, heads_here, head_size),
        ),
    )
    gated = (attended.reshape(rows_here, cols_here, head_width) * att_gate).astype(jnp.bfloat16)
    return pair_mid + project(gated, att_out_weight)


def dot_nn(a, b):
    return lax.dot_general(a, b, (((1,), (0,)), ((), ())), preferred_element_type=f32)


def dot_nt(a, b):
    return lax.dot_general(a, b, (((1,), (1,)), ((), ())), preferred_element_type=f32)


kernel_params = pltpu.CompilerParams(vmem_limit_bytes=16 << 20)


def near(v):
    return pltpu.with_memory_space_constraint(v, pltpu.VMEM)


def afar(v):
    return pltpu.with_memory_space_constraint(v, pltpu.HBM)


def split_weight(w_ref, w_scratch):
    rows, mats, out = w_ref.shape
    w_scratch[...] = w_ref[...].astype(f32).reshape(rows * mats, out)
    return [w_scratch[pl.ds(p, rows, stride=mats), :] for p in range(mats)]


def factors_kernel(
    devices,
    pair_ref,
    gain_ref,
    w_ref,
    live_ref,
    out_gain_ref,
    att_gain_ref,
    lr_ref,
    normed_ref,
    rows_ref,
    w_scratch,
):
    cells, _ = pair_ref.shape
    live = live_ref[...].astype(f32)
    rows_ref[0:1] = jnp.concatenate([live, jnp.zeros((1, LANES - live.shape[1]), f32)], axis=1)
    rows_ref[1:2] = out_gain_ref[...]
    rows_ref[2:3] = att_gain_ref[...]
    hidden = w_ref.shape[2]
    own = hidden // devices
    normed = norm_last(pair_ref[...], gain_ref[...]).astype(bf16)
    normed_ref[...] = normed
    w_t = [jnp.transpose(w).astype(bf16) for w in split_weight(w_ref, w_scratch)]
    spare = (-cells) % LANES
    tiles = (cells + spare) // LANES
    if spare:
        tail = normed[:spare]
        rhs_left = jnp.concatenate([normed, tail], axis=0)
        rhs_right = jnp.concatenate([tail, normed], axis=0)
    else:
        rhs_left = rhs_right = normed
    left = sigmoid(dot_nt(w_t[0], rhs_left)) * dot_nt(w_t[1], rhs_left)
    right = sigmoid(dot_nt(w_t[2], rhs_right)) * dot_nt(w_t[3], rhs_right)
    panels = [left[:, t * LANES : (t + 1) * LANES] for t in range(tiles)]
    right_panels = [right[:, t * LANES : (t + 1) * LANES] for t in range(tiles)]
    if spare:
        lane = lax.broadcasted_iota(jnp.int32, (hidden, LANES), 1)
        panels[-1] = jnp.where(lane < LANES - spare, panels[-1], right_panels[0])
        panels += right_panels[1:]
    else:
        panels += right_panels
    for t, panel in enumerate(panels):
        lr_ref[:, t] = panel.reshape(devices, own, LANES).astype(bf16)


def segment(panels, start, target):
    tile, at = divmod(start, LANES)
    here = panels[tile]
    if at and tile + 1 < len(panels):
        lane = lax.broadcasted_iota(jnp.int32, here.shape, 1)
        here = jnp.where(lane >= at, here, panels[tile + 1])
    shift = (target - at) % LANES
    return pltpu.roll(here, shift, 1) if shift else here


def triangle_kernel(
    rows_here, cols_here, vectors_ref, lr_ref, sum_ref, left_scratch, right_scratch, sum_scratch
):
    _, panels_in, own, _ = lr_ref.shape
    residues = left_scratch.shape[0] // own
    cols = residues // cols_here
    rows = residues // rows_here
    cells = rows_here * cols_here
    lane = lax.broadcasted_iota(jnp.int32, (own, LANES), 1)
    for r in range(rows):
        parts = [
            [lr_ref[r * cols + c, t].astype(f32) for t in range(panels_in)] for c in range(cols)
        ]
        for side, scratch in ((0, left_scratch), (1, right_scratch)):
            for i in range(rows_here):
                start = side * cells + i * cols_here
                line = segment(parts[0], start, 0)
                for c in range(1, cols):
                    moved = segment(parts[c], start, c * cols_here)
                    line = jnp.where(lane < c * cols_here, line, moved)
                scratch[pl.ds((r * rows_here + i) * own, own), :] = line
    live_wide = vectors_ref[0:1]
    live_square = jnp.broadcast_to(live_wide, (LANES, LANES))
    both = live_square * jnp.transpose(live_square)
    both = both[:residues]
    keep = live_wide > 0
    for h in range(own):
        left = jnp.where(keep, left_scratch[pl.ds(h, residues, stride=own), :], 0.0).astype(bf16)
        right = jnp.where(keep, right_scratch[pl.ds(h, residues, stride=own), :], 0.0).astype(bf16)
        right = jnp.concatenate([right, jnp.zeros((LANES - residues, LANES), bf16)], axis=0)
        sum_scratch[pl.ds(h, residues, stride=own), :] = dot_nt(left, right) * both
    tiles = sum_ref.shape[1]
    for r in range(rows):
        lines = [
            sum_scratch[pl.ds((r * rows_here + i) * own, own), :] for i in range(rows_here)
        ]
        for c in range(cols):
            for t in range(tiles):
                panel = None
                for i in range(rows_here):
                    low, high = i * cols_here - t * LANES, (i + 1) * cols_here - t * LANES
                    if high <= 0 or low >= LANES:
                        continue
                    shift = (low - c * cols_here) % LANES
                    line = pltpu.roll(lines[i], shift, 1) if shift else lines[i]
                    panel = line if panel is None else jnp.where(lane >= low, line, panel)
                sum_ref[r * cols + c, t] = panel.astype(bf16)


def middle_kernel(
    pair_ref,
    normed_ref,
    sum_ref,
    vectors_ref,
    out_w_ref,
    gate_w_ref,
    bias_w_ref,
    mid_ref,
    att_ref,
    bias_ref,
):
    devices, tiles, own, _ = sum_ref.shape
    cells, _ = pair_ref.shape
    hidden = devices * own
    gain_col = jnp.transpose(jnp.broadcast_to(vectors_ref[1:2], (LANES, hidden)))
    gate = sigmoid(dot_nn(normed_ref[...], gate_w_ref[...]))
    bias_w = bias_w_ref[...]
    hidden_rows = []
    for t in range(tiles):
        total = sum_ref[:, t].astype(f32).reshape(hidden, LANES)
        center = jnp.mean(total, axis=0, keepdims=True)
        centered = total - center
        variance = jnp.mean(centered * centered, axis=0, keepdims=True)
        hidden_normed = centered * lax.rsqrt(variance + epsilon) * gain_col
        hidden_rows.append(jnp.transpose(hidden_normed).astype(bf16))
    hidden_rows = jnp.concatenate(hidden_rows, axis=0)[:cells]
    mid = pair_ref[...] + gate * dot_nn(hidden_rows, out_w_ref[...])
    mid_ref[...] = mid
    att = norm_last(mid, vectors_ref[2:3]).astype(bf16)
    att_ref[...] = att
    bias_ref[0] = dot_nt(bias_w, att).astype(bf16)


def own_kernel(heads, att_ref, w_ref, q_ref, k_ref, v_ref, gate_ref, kv_w_ref, w_scratch):
    rows_here, cols_here, chan = att_ref.shape
    width = w_ref.shape[2]
    shape = (rows_here, cols_here, width)
    att = att_ref[...].reshape(rows_here * cols_here, chan)
    w = [m.astype(bf16) for m in split_weight(w_ref, w_scratch)]
    kv_w_ref[0], kv_w_ref[1] = w[1], w[2]
    q_ref[...] = (dot_nn(att, w[0]) * (width // heads) ** (-0.5)).astype(bf16).reshape(shape)
    k_ref[...] = dot_nn(att, w[1]).astype(bf16).reshape(shape)
    v_ref[...] = dot_nn(att, w[2]).astype(bf16).reshape(shape)
    gate_ref[...] = sigmoid(dot_nn(att, w[3])).reshape(shape)


def fetch_plan():
    trips, codes = ([], []), [0] * 16
    for h in range(2):
        for x in range(2):
            for p in range(2):
                for b in range(2):
                    chips = [t for t in range(4) if (t in FIRST[h][x]) == (b == p)]
                    for n, target in enumerate(chips):
                        source_core = n ^ TURNED[2 * h + b][x][p]
                        core = x ^ (target in SWAPPED[h])
                        source = ((2 * h + b) * 2 + source_core) * 2 + x
                        device = (target * 2 + core) * 2 + h
                        trips[p].append((source, device))
                        codes[device] |= (b if p == 0 else 0) | source_core << (1 + p)
                        codes[device] |= (x == h) << 3
    return trips, codes


FIRST = (((0, 1), (0, 2)), ((0, 1), (1, 2)))
SWAPPED = ((1,), (0, 1, 2, 3))
TURNED = (((1, 0), (1, 0)), ((0, 1), (1, 1)), ((1, 0), (0, 0)), ((0, 1), (0, 0)))


def fetch_code(codes, row, col):
    index = row * 2 + col
    code = jnp.int32(0)
    for device, entry in enumerate(codes):
        code = jnp.where(index == device, jnp.int32(entry), code)
    return [jnp.bitwise_and(lax.shift_right_logical(code, jnp.int32(n)), 1) for n in range(4)]


def head_bias_half(ref, scratch, rows_here, cols_here, code, target):
    blocks, heads, cells = ref.shape
    first, *cores, _ = code
    pad = (-cells) % LANES
    for m in range(blocks):
        p, n = m // 2, m % 2
        block = 2 * jnp.bitwise_xor(first, p) + jnp.bitwise_xor(n, cores[p])
        v = ref[m].astype(f32)
        v = jnp.concatenate([v, jnp.zeros((heads, pad), f32)], axis=1) if pad else v
        panels = [v[:, t * LANES : (t + 1) * LANES] for t in range((cells + pad) // LANES)]
        for j in range(rows_here):
            line = segment(panels, j * cols_here, target)
            scratch[pl.ds((block * rows_here + j) * heads, heads), :] = line
    return jnp.concatenate(
        [scratch[pl.ds(h, cols_here, stride=heads), :] for h in range(heads)], axis=0
    )


def scores_kernel(
    codes,
    vectors_ref,
    fetched_ref,
    q_ref,
    k_ref,
    far_ref,
    v_ref,
    kv_w_ref,
    scores_ref,
    v_all_ref,
    bias_ref,
    bias_scratch,
):
    rows_here, cols_here, width = q_ref.shape
    heads = fetched_ref.shape[1]
    far = far_ref[...].reshape(rows_here * cols_here, width)
    k_far = dot_nn(far, kv_w_ref[0]).astype(bf16).reshape(q_ref.shape)
    v_far = dot_nn(far, kv_w_ref[1]).astype(bf16).reshape(q_ref.shape)
    row, col = lax.axis_index("row"), lax.axis_index(("col", "sub"))
    code = fetch_code(codes, row, col)
    own_first = code[3] == 1

    def in_order(own, other):
        return jnp.concatenate(
            [jnp.where(own_first, own, other), jnp.where(own_first, other, own)], axis=0
        )

    head_of = lax.broadcasted_iota(jnp.int32, (cols_here, width), 1) // (width // heads)
    for i in range(rows_here):
        q = q_ref[i]
        q_heads = jnp.concatenate(
            [jnp.where(head_of == h, q, jnp.zeros_like(q)) for h in range(heads)], axis=0
        )
        scores_ref[i] = dot_nt(q_heads, in_order(k_ref[i], k_far[i]))
        v_all_ref[i] = in_order(v_ref[i], v_far[i])
    lane_row = lax.broadcasted_iota(jnp.int32, (1, LANES), 1)
    live = vectors_ref[0:1]
    swapped = jnp.where(
        lane_row < cols_here,
        pltpu.roll(live, LANES - cols_here, 1),
        pltpu.roll(live, cols_here, 1),
    )
    natural = (col == 0) == own_first
    penalty = (jnp.where(natural, live, swapped) - 1.0) * mask_penalty
    half = head_bias_half(fetched_ref, bias_scratch, rows_here, cols_here, code, 0)
    bias_ref[...] = jnp.where(lane_row < cols_here, half, 0.0) + penalty


def attention_kernel(
    codes,
    bias_ref,
    swapped_ref,
    scores_ref,
    v_all_ref,
    gate_ref,
    mid_ref,
    out_w_ref,
    out_ref,
    bias_scratch,
    result,
    done,
):
    rows_here, cols_here, width = gate_ref.shape
    chunks = done.shape[0]
    heads = swapped_ref.shape[1]
    residues = 2 * cols_here
    row, col = lax.axis_index("row"), lax.axis_index(("col", "sub"))
    code = fetch_code(codes, jnp.bitwise_xor(row, 1), col)
    half = head_bias_half(swapped_ref, bias_scratch, rows_here, cols_here, code, cols_here)
    lane_row = lax.broadcasted_iota(jnp.int32, (1, LANES), 1)
    head_bias = (bias_ref[...] + jnp.where(lane_row < cols_here, 0.0, half))[:, :residues]
    head_of = lax.broadcasted_iota(jnp.int32, (cols_here, width), 1) // (width // heads)
    ones = jnp.ones((residues, width), bf16)
    chunk = rows_here // chunks
    copies = []
    for c in range(chunks):
        gated = []
        for i in range(c * chunk, (c + 1) * chunk):
            scores = scores_ref[i] + head_bias
            raised = jnp.exp(scores - jnp.max(scores, axis=-1, keepdims=True)).astype(bf16)
            mixed = dot_nn(raised, jnp.concatenate([v_all_ref[i], ones], axis=1))
            attended = mixed[:cols_here]
            for h in range(1, heads):
                part = mixed[h * cols_here : (h + 1) * cols_here]
                attended = jnp.where(jnp.tile(head_of, (1, 2)) == h, part, attended)
            attended = attended[:, :width] / attended[:, width:]
            gated.append((attended * gate_ref[i]).astype(bf16))
        update = dot_nn(jnp.concatenate(gated, axis=0), out_w_ref[...])
        at = slice(c * chunk, (c + 1) * chunk)
        result[at] = mid_ref[at] + update.reshape(chunk, cols_here, width)
        copies.append(pltpu.make_async_copy(result.at[at], out_ref.at[at], done.at[c]))
        copies[-1].start()
    for copy in copies:
        copy.wait()


def body_channels(
    pair,
    residue_mask,
    tri_norm_gain,
    tri_in_weight,
    tri_gate_weight,
    tri_out_norm_gain,
    tri_out_weight,
    att_norm_gain,
    att_proj_weight,
    att_bias_weight,
    att_out_weight,
):
    rows_here, cols_here, chan = pair.shape
    rows, cols = lax.axis_size("row"), lax.axis_size(("col", "sub"))
    group = ("row", "col", "sub")
    devices = rows * cols
    residues = cols_here * cols
    cells = rows_here * cols_here
    hidden = tri_in_weight.shape[2]
    own = hidden // devices
    heads = att_bias_weight.shape[1]
    tiles = -(-cells // LANES)
    lr_panels = -(-2 * cells // LANES) if (-cells) % LANES * 2 == LANES else 2 * tiles
    flat = pair.reshape(cells, chan)
    live = residue_mask.reshape(1, residues)

    lr, normed, vectors = pl.pallas_call(
        functools.partial(factors_kernel, devices),
        out_shape=(
            pltpu.VMEM((devices, lr_panels, own, LANES), bf16),
            pltpu.VMEM((cells, chan), bf16),
            pltpu.VMEM((8, LANES), f32),
        ),
        scratch_shapes=[pltpu.VMEM((chan * tri_in_weight.shape[1], hidden), f32)],
        compiler_params=kernel_params,
        name="factors",
    )(
        *map(
            afar,
            (
                flat,
                tri_norm_gain.reshape(1, chan),
                tri_in_weight,
                live,
                tri_out_norm_gain.reshape(1, hidden),
                att_norm_gain.reshape(1, chan),
            ),
        )
    )
    lr = lax.all_to_all(lr, group, 0, 0, tiled=True)
    sums = pl.pallas_call(
        functools.partial(triangle_kernel, rows_here, cols_here),
        out_shape=pltpu.VMEM((devices, tiles, own, LANES), bf16),
        scratch_shapes=[pltpu.VMEM((residues * own, LANES), f32) for _ in range(3)],
        compiler_params=kernel_params,
        name="triangle",
    )(near(vectors), near(lr))
    sums = lax.all_to_all(sums, group, 0, 0, tiled=True)
    shape = (rows_here, cols_here, chan)
    chunks = math.gcd(rows_here, 3)
    mid, att, bias = pl.pallas_call(
        middle_kernel,
        out_shape=(
            pltpu.VMEM((cells, chan), f32),
            pltpu.VMEM((cells, chan), bf16),
            pltpu.VMEM((1, heads, cells), bf16),
        ),
        compiler_params=kernel_params,
        name="middle",
    )(
        *map(
            near,
            (
                flat,
                normed,
                sums,
                vectors,
                tri_out_weight,
                tri_gate_weight,
                att_bias_weight.T,
            ),
        )
    )
    att, mid = att.reshape(shape), mid.reshape(shape)

    def swap(v):
        return lax.ppermute(v, "row", [(r, r ^ 1) for r in range(rows)])

    trips, codes = fetch_plan()
    joined = swap(bias)
    bias = jnp.concatenate([bias, joined], axis=0)
    fetched = []
    for p in range(2):
        fetched.append(lax.ppermute(bias, group, trips[p]))
    far = lax.ppermute(att, ("col", "sub"), [(c, c ^ 1) for c in range(cols)])
    queries, keys, values, gate, kv_weight = pl.pallas_call(
        functools.partial(own_kernel, heads),
        out_shape=(
            pltpu.VMEM(shape, bf16),
            pltpu.VMEM(shape, bf16),
            pltpu.VMEM(shape, bf16),
            pltpu.VMEM(shape, f32),
            pltpu.VMEM((2, chan, chan), bf16),
        ),
        scratch_shapes=[pltpu.VMEM((chan * att_proj_weight.shape[1], chan), f32)],
        compiler_params=kernel_params,
        name="own",
    )(near(att), near(att_proj_weight))
    fetched = jnp.concatenate(fetched, axis=0)
    swapped = swap(fetched)
    scores, values, bias = pl.pallas_call(
        functools.partial(scores_kernel, codes),
        out_shape=(
            pltpu.VMEM((rows_here, heads * cols_here, residues), f32),
            pltpu.VMEM((rows_here, residues, chan), bf16),
            pltpu.VMEM((heads * cols_here, LANES), f32),
        ),
        scratch_shapes=[pltpu.VMEM((cols_here * heads, LANES), f32)],
        compiler_params=kernel_params,
        name="scores",
    )(*map(near, (vectors, fetched, queries, keys, far, values, kv_weight)))
    return pl.pallas_call(
        functools.partial(attention_kernel, codes),
        out_shape=jax.ShapeDtypeStruct(shape, f32),
        out_specs=pl.BlockSpec(memory_space=pltpu.HBM),
        scratch_shapes=[
            pltpu.VMEM((cols_here * heads, LANES), f32),
            pltpu.VMEM(shape, f32),
            pltpu.SemaphoreType.DMA((chunks,)),
        ],
        compiler_params=kernel_params,
        name="attention",
    )(*map(near, (bias, swapped, scores, values, gate, mid, att_out_weight)))


def solution(mesh):
    placed = (
        P(("parts", "row"), ("col", "sub"), None),
        P("parts"),
        P(),
        P(),
        P(),
        P(),
        P(),
        P(),
        P(),
        P(),
        P(),
    )

    def body(pair, residue_mask, tri_norm_gain, tri_in_weight, *others):
        rows, cols = mesh.shape["row"], mesh.shape["col"] * mesh.shape["sub"]
        hidden = tri_in_weight.shape[2]
        fits = (
            cols == 2
            and rows == 8
            and hidden % (8 * rows * cols) == 0
            and hidden == pair.shape[2] == LANES
            and residue_mask.shape[0] <= LANES
            and pair.shape[0] * cols * pair.shape[1] % 16 == 0
        )
        chosen = body_channels if fits else body_general
        return chosen(pair, residue_mask, tri_norm_gain, tri_in_weight, *others)

    return jax.shard_map(
        body,
        mesh=mesh,
        in_specs=placed,
        out_specs=P(("parts", "row"), ("col", "sub"), None),
        check_vma=False,
    )
```

```python
import functools
import math

import jax
import jax.numpy as jnp
from jax import lax
from jax.experimental import pallas as pl
from jax.experimental.pallas import tpu as pltpu
from jax.sharding import PartitionSpec as P


epsilon = 1e-05
mask_penalty = 1000000000.0
LANES = 128
f32 = jnp.float32
bf16 = jnp.bfloat16


def norm_last(values_in, gain):
    center = jnp.mean(values_in, axis=-1, keepdims=True)
    centered = values_in - center
    variance = jnp.mean(centered * centered, axis=-1, keepdims=True)
    return centered * lax.rsqrt(variance + epsilon) * gain


def sigmoid(v):
    return 0.5 * jnp.tanh(0.5 * v) + 0.5


def project(normed, weight):
    flat_rows = normed.reshape(-1, normed.shape[-1])
    product = jnp.dot(flat_rows, weight, preferred_element_type=jnp.float32)
    return product.reshape(normed.shape[:-1] + (weight.shape[1],))


def body_general(
    pair,
    residue_mask,
    tri_norm_gain,
    tri_in_weight,
    tri_gate_weight,
    tri_out_norm_gain,
    tri_out_weight,
    att_norm_gain,
    att_proj_weight,
    att_bias_weight,
    att_out_weight,
):
    rows_here, cols_here, _ = pair.shape
    residues = cols_here * lax.axis_size(("col", "sub"))
    row_offset = lax.axis_index("row") * rows_here
    col_offset = lax.axis_index(("col", "sub")) * cols_here
    residue_live = residue_mask.astype(jnp.float32)
    live_rows = lax.dynamic_slice_in_dim(residue_live, row_offset, rows_here)
    live_cols = lax.dynamic_slice_in_dim(residue_live, col_offset, cols_here)
    pair_live = (live_rows[:, None] * live_cols[None, :])[:, :, None]
    tri_normed = norm_last(pair, tri_norm_gain).astype(jnp.bfloat16)
    in_width = tri_in_weight.shape[2]
    projected = project(tri_normed, tri_in_weight.reshape(tri_in_weight.shape[0], -1)).reshape(
        rows_here, cols_here, 4, in_width
    )
    left_factor = (jax.nn.sigmoid(projected[:, :, 0]) * projected[:, :, 1] * pair_live).astype(
        jnp.bfloat16
    )
    right_factor = (jax.nn.sigmoid(projected[:, :, 2]) * projected[:, :, 3] * pair_live).astype(
        jnp.bfloat16
    )
    left_all, right_all = (
        lax.all_gather(left_factor, ("col", "sub"), axis=1, tiled=True),
        lax.all_gather(right_factor, ("col", "sub"), axis=1, tiled=True),
    )
    exchanged = lax.all_to_all(right_all, "row", split_axis=1, concat_axis=0, tiled=True)
    own_rows = lax.dynamic_slice_in_dim(exchanged, col_offset, cols_here, 0)
    tri_sum = jnp.einsum(
        "ikh,jkh->ijh",
        left_all,
        lax.all_gather(own_rows, "row", axis=1, tiled=True),
        preferred_element_type=jnp.float32,
    )
    hidden_normed = norm_last(tri_sum, tri_out_norm_gain).astype(jnp.bfloat16)
    tri_gate = jax.nn.sigmoid(project(tri_normed, tri_gate_weight))
    pair_mid = pair + tri_gate * project(hidden_normed, tri_out_weight)
    att_normed = norm_last(pair_mid, att_norm_gain).astype(jnp.bfloat16)
    head_width = att_proj_weight.shape[2]
    heads_here = att_bias_weight.shape[1]
    head_size = head_width // heads_here
    projected = project(att_normed, att_proj_weight.reshape(att_proj_weight.shape[0], -1)).reshape(
        rows_here, cols_here, 4, head_width
    )
    queries = (projected[:, :, 0] * head_size ** (-0.5)).astype(jnp.bfloat16)
    key_rows = projected[:, :, 1].astype(jnp.bfloat16)
    value_rows = projected[:, :, 2].astype(jnp.bfloat16)
    att_gate = jax.nn.sigmoid(projected[:, :, 3])
    pair_bias = project(att_normed, att_bias_weight).astype(jnp.bfloat16)
    key_all, value_all = (
        lax.all_gather(key_rows, ("col", "sub"), axis=1, tiled=True),
        lax.all_gather(value_rows, ("col", "sub"), axis=1, tiled=True),
    )
    bias_all_rows = lax.all_gather(pair_bias, "row", axis=0, tiled=True)
    bias_panel = lax.all_to_all(
        bias_all_rows, ("col", "sub"), split_axis=0, concat_axis=1, tiled=True
    )
    mask_row = (residue_live - 1.0) * mask_penalty
    head_bias = jnp.transpose(bias_panel.astype(jnp.float32), (2, 0, 1)) + mask_row[None, None, :]
    block_rows = math.gcd(rows_here, max(1, 512 // cols_here))
    blocks = rows_here // block_rows

    def attend(block_items):
        query_block, key_block, value_block = block_items
        scores = (
            jnp.einsum(
                "ijhd,ikhd->ihjk", query_block, key_block, preferred_element_type=jnp.float32
            )
            + head_bias[None]
        )
        row_max = jnp.max(scores, axis=-1, keepdims=True)
        raised = jnp.exp(scores - row_max)
        weights = (raised / jnp.sum(raised, axis=-1, keepdims=True)).astype(jnp.bfloat16)
        return jnp.einsum(
            "ihjk,ikhd->ijhd", weights, value_block, preferred_element_type=jnp.float32
        )

    attended = lax.map(
        attend,
        (
            queries.reshape(blocks, block_rows, cols_here, heads_here, head_size),
            key_all.reshape(blocks, block_rows, residues, heads_here, head_size),
            value_all.reshape(blocks, block_rows, residues, heads_here, head_size),
        ),
    )
    gated = (attended.reshape(rows_here, cols_here, head_width) * att_gate).astype(jnp.bfloat16)
    return pair_mid + project(gated, att_out_weight)


def dot_nn(a, b):
    return lax.dot_general(a, b, (((1,), (0,)), ((), ())), preferred_element_type=f32)


def dot_nt(a, b):
    return lax.dot_general(a, b, (((1,), (1,)), ((), ())), preferred_element_type=f32)


kernel_params = pltpu.CompilerParams(vmem_limit_bytes=16 << 20)


def near(v):
    return pltpu.with_memory_space_constraint(v, pltpu.VMEM)


def afar(v):
    return pltpu.with_memory_space_constraint(v, pltpu.HBM)


def split_weight(w_ref, w_scratch):
    rows, mats, out = w_ref.shape
    w_scratch[...] = w_ref[...].astype(f32).reshape(rows * mats, out)
    return [w_scratch[pl.ds(p, rows, stride=mats), :] for p in range(mats)]


def factors_kernel(
    devices,
    pair_ref,
    gain_ref,
    w_ref,
    live_ref,
    out_gain_ref,
    att_gain_ref,
    lr_ref,
    normed_ref,
    rows_ref,
    kept_ref,
    w_scratch,
):
    cells, _ = pair_ref.shape
    kept_ref[...] = pair_ref[...]
    live = live_ref[...].astype(f32)
    rows_ref[0:1] = jnp.concatenate([live, jnp.zeros((1, LANES - live.shape[1]), f32)], axis=1)
    rows_ref[1:2] = out_gain_ref[...]
    rows_ref[2:3] = att_gain_ref[...]
    hidden = w_ref.shape[2]
    own = hidden // devices
    normed = norm_last(pair_ref[...], gain_ref[...]).astype(bf16)
    normed_ref[...] = normed
    w = [w.astype(bf16) for w in split_weight(w_ref, w_scratch)]
    spare = (-cells) % LANES
    tiles = (cells + spare) // LANES
    if spare:
        tail = normed[:spare]
        rows_left = jnp.concatenate([normed, tail], axis=0)
        rows_right = jnp.concatenate([tail, normed], axis=0)
    else:
        rows_left = rows_right = normed
    left = jnp.transpose(sigmoid(dot_nn(rows_left, w[0])) * dot_nn(rows_left, w[1]))
    right = jnp.transpose(sigmoid(dot_nn(rows_right, w[2])) * dot_nn(rows_right, w[3]))
    panels = [left[:, t * LANES : (t + 1) * LANES] for t in range(tiles)]
    right_panels = [right[:, t * LANES : (t + 1) * LANES] for t in range(tiles)]
    if spare:
        lane = lax.broadcasted_iota(jnp.int32, (hidden, LANES), 1)
        panels[-1] = jnp.where(lane < LANES - spare, panels[-1], right_panels[0])
        panels += right_panels[1:]
    else:
        panels += right_panels
    for t, panel in enumerate(panels):
        lr_ref[:, t] = panel.reshape(devices, own, LANES).astype(bf16)


def segment(panels, start, target):
    tile, at = divmod(start, LANES)
    here = panels[tile]
    if at and tile + 1 < len(panels):
        lane = lax.broadcasted_iota(jnp.int32, here.shape, 1)
        here = jnp.where(lane >= at, here, panels[tile + 1])
    shift = (target - at) % LANES
    return pltpu.roll(here, shift, 1) if shift else here


def triangle_kernel(
    rows_here, cols_here, vectors_ref, lr_ref, sum_ref, left_scratch, right_scratch, sum_scratch
):
    _, panels_in, own, _ = lr_ref.shape
    residues = left_scratch.shape[0] // own
    cols = residues // cols_here
    rows = residues // rows_here
    cells = rows_here * cols_here
    lane = lax.broadcasted_iota(jnp.int32, (own, LANES), 1)
    for r in range(rows):
        parts = [
            [lr_ref[r * cols + c, t].astype(f32) for t in range(panels_in)] for c in range(cols)
        ]
        for side, scratch in ((0, left_scratch), (1, right_scratch)):
            for i in range(rows_here):
                start = side * cells + i * cols_here
                line = segment(parts[0], start, 0)
                for c in range(1, cols):
                    moved = segment(parts[c], start, c * cols_here)
                    line = jnp.where(lane < c * cols_here, line, moved)
                scratch[pl.ds((r * rows_here + i) * own, own), :] = line
    live_wide = vectors_ref[0:1]
    live_square = jnp.broadcast_to(live_wide, (LANES, LANES))
    both = live_square * jnp.transpose(live_square)
    both = both[:residues]
    keep = live_wide > 0
    for h in range(own):
        left = jnp.where(keep, left_scratch[pl.ds(h, residues, stride=own), :], 0.0).astype(bf16)
        right = right_scratch[pl.ds(h, residues, stride=own), :].astype(bf16)
        right = jnp.concatenate([right, jnp.zeros((LANES - residues, LANES), bf16)], axis=0)
        sum_scratch[pl.ds(h, residues, stride=own), :] = dot_nt(left, right) * both
    tiles = sum_ref.shape[1]
    for r in range(rows):
        lines = [
            sum_scratch[pl.ds((r * rows_here + i) * own, own), :] for i in range(rows_here)
        ]
        for c in range(cols):
            for t in range(tiles):
                panel = None
                for i in range(rows_here):
                    low, high = i * cols_here - t * LANES, (i + 1) * cols_here - t * LANES
                    if high <= 0 or low >= LANES:
                        continue
                    shift = (low - c * cols_here) % LANES
                    line = pltpu.roll(lines[i], shift, 1) if shift else lines[i]
                    panel = line if panel is None else jnp.where(lane >= low, line, panel)
                sum_ref[r * cols + c, t] = panel.astype(bf16)


def middle_kernel(
    pair_ref,
    normed_ref,
    sum_ref,
    vectors_ref,
    out_w_ref,
    gate_w_ref,
    bias_w_ref,
    mid_ref,
    att_ref,
    bias_ref,
):
    devices, tiles, own, _ = sum_ref.shape
    cells, _ = pair_ref.shape
    hidden = devices * own
    gain_col = jnp.transpose(jnp.broadcast_to(vectors_ref[1:2], (LANES, hidden)))
    gate = sigmoid(dot_nn(normed_ref[...], gate_w_ref[...]))
    bias_w = bias_w_ref[...]
    hidden_rows = []
    for t in range(tiles):
        total = sum_ref[:, t].astype(f32).reshape(hidden, LANES)
        center = jnp.mean(total, axis=0, keepdims=True)
        centered = total - center
        variance = jnp.mean(centered * centered, axis=0, keepdims=True)
        hidden_normed = centered * lax.rsqrt(variance + epsilon) * gain_col
        hidden_rows.append(jnp.transpose(hidden_normed).astype(bf16))
    hidden_rows = jnp.concatenate(hidden_rows, axis=0)[:cells]
    mid = pair_ref[...] + gate * dot_nn(hidden_rows, out_w_ref[...])
    mid_ref[...] = mid
    att = norm_last(mid, vectors_ref[2:3]).astype(bf16)
    att_ref[...] = att
    bias_ref[0] = dot_nt(bias_w, att).astype(bf16)


def own_kernel(heads, att_ref, w_ref, q_ref, k_ref, v_ref, gate_ref, kv_w_ref, w_scratch):
    rows_here, cols_here, chan = att_ref.shape
    width = w_ref.shape[2]
    shape = (rows_here, cols_here, width)
    att = att_ref[...].reshape(rows_here * cols_here, chan)
    w = [m.astype(bf16) for m in split_weight(w_ref, w_scratch)]
    kv_w_ref[0], kv_w_ref[1] = w[1], w[2]
    q_ref[...] = (dot_nn(att, w[0]) * (width // heads) ** (-0.5)).astype(bf16).reshape(shape)
    k_ref[...] = dot_nn(att, w[1]).astype(bf16).reshape(shape)
    v_ref[...] = dot_nn(att, w[2]).astype(bf16).reshape(shape)
    gate_ref[...] = sigmoid(dot_nn(att, w[3])).reshape(shape)


def fetch_plan():
    trips, codes = ([], []), [0] * 16
    for h in range(2):
        for x in range(2):
            for p in range(2):
                for b in range(2):
                    chips = [t for t in range(4) if (t in FIRST[h][x]) == (b == p)]
                    for n, target in enumerate(chips):
                        source_core = n ^ TURNED[2 * h + b][x][p]
                        core = x ^ (target in SWAPPED[h])
                        source = ((2 * h + b) * 2 + source_core) * 2 + x
                        device = (target * 2 + core) * 2 + h
                        trips[p].append((source, device))
                        codes[device] |= (b if p == 0 else 0) | source_core << (1 + p)
                        codes[device] |= (x == h) << 3
    return trips, codes


FIRST = (((0, 1), (0, 2)), ((0, 1), (1, 2)))
SWAPPED = ((1,), (0, 1, 2, 3))
TURNED = (((1, 0), (1, 0)), ((0, 1), (1, 1)), ((1, 0), (0, 0)), ((0, 1), (0, 0)))


def fetch_code(codes, row, col):
    index = row * 2 + col
    code = jnp.int32(0)
    for device, entry in enumerate(codes):
        code = jnp.where(index == device, jnp.int32(entry), code)
    return [jnp.bitwise_and(lax.shift_right_logical(code, jnp.int32(n)), 1) for n in range(4)]


def head_bias_half(ref, scratch, rows_here, cols_here, code, target):
    blocks, heads, cells = ref.shape
    first, *cores, _ = code
    pad = (-cells) % LANES
    for m in range(blocks):
        p, n = m // 2, m % 2
        block = 2 * jnp.bitwise_xor(first, p) + jnp.bitwise_xor(n, cores[p])
        v = ref[m].astype(f32)
        v = jnp.concatenate([v, jnp.zeros((heads, pad), f32)], axis=1) if pad else v
        panels = [v[:, t * LANES : (t + 1) * LANES] for t in range((cells + pad) // LANES)]
        for j in range(rows_here):
            line = segment(panels, j * cols_here, target)
            scratch[pl.ds((block * rows_here + j) * heads, heads), :] = line
    return jnp.concatenate(
        [scratch[pl.ds(h, cols_here, stride=heads), :] for h in range(heads)], axis=0
    )


def scores_kernel(
    codes,
    vectors_ref,
    fetched_ref,
    q_ref,
    k_ref,
    far_ref,
    v_ref,
    kv_w_ref,
    scores_ref,
    v_all_ref,
    bias_ref,
    bias_scratch,
):
    rows_here, cols_here, width = q_ref.shape
    heads = fetched_ref.shape[1]
    far = far_ref[...].reshape(rows_here * cols_here, width)
    k_far = dot_nn(far, kv_w_ref[0]).astype(bf16).reshape(q_ref.shape)
    v_far = dot_nn(far, kv_w_ref[1]).astype(bf16).reshape(q_ref.shape)
    row, col = lax.axis_index("row"), lax.axis_index(("col", "sub"))
    code = fetch_code(codes, row, col)
    own_first = code[3] == 1

    def in_order(own, other):
        return jnp.concatenate(
            [jnp.where(own_first, own, other), jnp.where(own_first, other, own)], axis=0
        )

    head_of = lax.broadcasted_iota(jnp.int32, (cols_here, width), 1) // (width // heads)
    for i in range(rows_here):
        q = q_ref[i]
        q_heads = jnp.concatenate(
            [jnp.where(head_of == h, q, jnp.zeros_like(q)) for h in range(heads)], axis=0
        )
        scores_ref[i] = dot_nt(q_heads, in_order(k_ref[i], k_far[i]))
        v_all_ref[i] = in_order(v_ref[i], v_far[i])
    lane_row = lax.broadcasted_iota(jnp.int32, (1, LANES), 1)
    live = vectors_ref[0:1]
    swapped = jnp.where(
        lane_row < cols_here,
        pltpu.roll(live, LANES - cols_here, 1),
        pltpu.roll(live, cols_here, 1),
    )
    natural = (col == 0) == own_first
    penalty = (jnp.where(natural, live, swapped) - 1.0) * mask_penalty
    half = head_bias_half(fetched_ref, bias_scratch, rows_here, cols_here, code, 0)
    bias_ref[...] = jnp.where(lane_row < cols_here, half, 0.0) + penalty


def attention_kernel(
    codes,
    bias_ref,
    swapped_ref,
    scores_ref,
    v_all_ref,
    gate_ref,
    mid_ref,
    out_w_ref,
    out_ref,
    bias_scratch,
    result,
    done,
):
    rows_here, cols_here, width = gate_ref.shape
    chunks = done.shape[0]
    heads = swapped_ref.shape[1]
    residues = 2 * cols_here
    row, col = lax.axis_index("row"), lax.axis_index(("col", "sub"))
    code = fetch_code(codes, jnp.bitwise_xor(row, 1), col)
    half = head_bias_half(swapped_ref, bias_scratch, rows_here, cols_here, code, cols_here)
    lane_row = lax.broadcasted_iota(jnp.int32, (1, LANES), 1)
    head_bias = (bias_ref[...] + jnp.where(lane_row < cols_here, 0.0, half))[:, :residues]
    head_of = lax.broadcasted_iota(jnp.int32, (cols_here, width), 1) // (width // heads)
    ones = jnp.ones((residues, width), bf16)
    chunk = rows_here // chunks
    copies = []
    for c in range(chunks):
        gated = []
        for i in range(c * chunk, (c + 1) * chunk):
            scores = scores_ref[i] + head_bias
            raised = jnp.exp(scores - jnp.max(scores, axis=-1, keepdims=True)).astype(bf16)
            mixed = dot_nn(raised, jnp.concatenate([v_all_ref[i], ones], axis=1))
            attended = mixed[:cols_here]
            for h in range(1, heads):
                part = mixed[h * cols_here : (h + 1) * cols_here]
                attended = jnp.where(jnp.tile(head_of, (1, 2)) == h, part, attended)
            attended = attended[:, :width] / attended[:, width:]
            gated.append((attended * gate_ref[i]).astype(bf16))
        update = dot_nn(jnp.concatenate(gated, axis=0), out_w_ref[...])
        at = slice(c * chunk, (c + 1) * chunk)
        result[at] = mid_ref[at] + update.reshape(chunk, cols_here, width)
        copies.append(pltpu.make_async_copy(result.at[at], out_ref.at[at], done.at[c]))
        copies[-1].start()
    for copy in copies:
        copy.wait()


def body_channels(
    pair,
    residue_mask,
    tri_norm_gain,
    tri_in_weight,
    tri_gate_weight,
    tri_out_norm_gain,
    tri_out_weight,
    att_norm_gain,
    att_proj_weight,
    att_bias_weight,
    att_out_weight,
):
    rows_here, cols_here, chan = pair.shape
    rows, cols = lax.axis_size("row"), lax.axis_size(("col", "sub"))
    group = ("row", "col", "sub")
    devices = rows * cols
    residues = cols_here * cols
    cells = rows_here * cols_here
    hidden = tri_in_weight.shape[2]
    own = hidden // devices
    heads = att_bias_weight.shape[1]
    tiles = -(-cells // LANES)
    lr_panels = -(-2 * cells // LANES) if (-cells) % LANES * 2 == LANES else 2 * tiles
    flat = pair.reshape(cells, chan)
    live = residue_mask.reshape(1, residues)

    lr, normed, vectors, kept = pl.pallas_call(
        functools.partial(factors_kernel, devices),
        out_shape=(
            pltpu.VMEM((devices, lr_panels, own, LANES), bf16),
            pltpu.VMEM((cells, chan), bf16),
            pltpu.VMEM((8, LANES), f32),
            pltpu.VMEM((cells, chan), f32),
        ),
        scratch_shapes=[pltpu.VMEM((chan * tri_in_weight.shape[1], hidden), f32)],
        compiler_params=kernel_params,
        name="factors",
    )(
        *map(
            afar,
            (
                flat,
                tri_norm_gain.reshape(1, chan),
                tri_in_weight,
                live,
                tri_out_norm_gain.reshape(1, hidden),
                att_norm_gain.reshape(1, chan),
            ),
        )
    )
    lr = lax.all_to_all(lr, group, 0, 0, tiled=True)
    sums = pl.pallas_call(
        functools.partial(triangle_kernel, rows_here, cols_here),
        out_shape=pltpu.VMEM((devices, tiles, own, LANES), bf16),
        scratch_shapes=[pltpu.VMEM((residues * own, LANES), f32) for _ in range(3)],
        compiler_params=kernel_params,
        name="triangle",
    )(near(vectors), near(lr))
    sums = lax.all_to_all(sums, group, 0, 0, tiled=True)
    shape = (rows_here, cols_here, chan)
    chunks = math.gcd(rows_here, 2)
    mid, att, bias = pl.pallas_call(
        middle_kernel,
        out_shape=(
            pltpu.VMEM((cells, chan), f32),
            pltpu.VMEM((cells, chan), bf16),
            pltpu.VMEM((1, heads, cells), bf16),
        ),
        compiler_params=kernel_params,
        name="middle",
    )(
        *map(
            near,
            (
                kept,
                normed,
                sums,
                vectors,
                tri_out_weight,
                tri_gate_weight,
                att_bias_weight.T,
            ),
        )
    )
    att, mid = att.reshape(shape), mid.reshape(shape)

    def swap(v):
        return lax.ppermute(v, "row", [(r, r ^ 1) for r in range(rows)])

    trips, codes = fetch_plan()
    joined = swap(bias)
    bias = jnp.concatenate([bias, joined], axis=0)
    fetched = []
    for p in range(2):
        fetched.append(lax.ppermute(bias, group, trips[p]))
    far = lax.ppermute(att, ("col", "sub"), [(c, c ^ 1) for c in range(cols)])
    queries, keys, values, gate, kv_weight = pl.pallas_call(
        functools.partial(own_kernel, heads),
        out_shape=(
            pltpu.VMEM(shape, bf16),
            pltpu.VMEM(shape, bf16),
            pltpu.VMEM(shape, bf16),
            pltpu.VMEM(shape, f32),
            pltpu.VMEM((2, chan, chan), bf16),
        ),
        scratch_shapes=[pltpu.VMEM((chan * att_proj_weight.shape[1], chan), f32)],
        compiler_params=kernel_params,
        name="own",
    )(near(att), near(att_proj_weight))
    fetched = jnp.concatenate(fetched, axis=0)
    swapped = swap(fetched)
    scores, values, bias = pl.pallas_call(
        functools.partial(scores_kernel, codes),
        out_shape=(
            pltpu.VMEM((rows_here, heads * cols_here, residues), f32),
            pltpu.VMEM((rows_here, residues, chan), bf16),
            pltpu.VMEM((heads * cols_here, LANES), f32),
        ),
        scratch_shapes=[pltpu.VMEM((cols_here * heads, LANES), f32)],
        compiler_params=kernel_params,
        name="scores",
    )(*map(near, (vectors, fetched, queries, keys, far, values, kv_weight)))
    return pl.pallas_call(
        functools.partial(attention_kernel, codes),
        out_shape=jax.ShapeDtypeStruct(shape, f32),
        out_specs=pl.BlockSpec(memory_space=pltpu.HBM),
        scratch_shapes=[
            pltpu.VMEM((cols_here * heads, LANES), f32),
            pltpu.VMEM(shape, f32),
            pltpu.SemaphoreType.DMA((chunks,)),
        ],
        compiler_params=kernel_params,
        name="attention",
    )(*map(near, (bias, swapped, scores, values, gate, mid, att_out_weight)))


def solution(mesh):
    placed = (
        P(("parts", "row"), ("col", "sub"), None),
        P("parts"),
        P(),
        P(),
        P(),
        P(),
        P(),
        P(),
        P(),
        P(),
        P(),
    )

    def body(pair, residue_mask, tri_norm_gain, tri_in_weight, *others):
        rows, cols = mesh.shape["row"], mesh.shape["col"] * mesh.shape["sub"]
        hidden = tri_in_weight.shape[2]
        fits = (
            cols == 2
            and rows == 8
            and hidden % (8 * rows * cols) == 0
            and hidden == pair.shape[2] == LANES
            and residue_mask.shape[0] <= LANES
            and pair.shape[0] * cols * pair.shape[1] % 16 == 0
        )
        chosen = body_channels if fits else body_general
        return chosen(pair, residue_mask, tri_norm_gain, tri_in_weight, *others)

    return jax.shard_map(
        body,
        mesh=mesh,
        in_specs=placed,
        out_specs=P(("parts", "row"), ("col", "sub"), None),
        check_vma=False,
    )
```

```python
import functools
import math

import jax
import jax.numpy as jnp
from jax import lax
from jax.experimental import pallas as pl
from jax.experimental.pallas import tpu as pltpu
from jax.sharding import PartitionSpec as P


epsilon = 1e-05
mask_penalty = 1000000000.0
LANES = 128
f32 = jnp.float32
bf16 = jnp.bfloat16


def norm_last(values_in, gain):
    center = jnp.mean(values_in, axis=-1, keepdims=True)
    centered = values_in - center
    variance = jnp.mean(centered * centered, axis=-1, keepdims=True)
    return centered * lax.rsqrt(variance + epsilon) * gain


def sigmoid(v):
    return 0.5 * jnp.tanh(0.5 * v) + 0.5


def project(normed, weight):
    flat_rows = normed.reshape(-1, normed.shape[-1])
    product = jnp.dot(flat_rows, weight, preferred_element_type=jnp.float32)
    return product.reshape(normed.shape[:-1] + (weight.shape[1],))


def body_general(
    pair,
    residue_mask,
    tri_norm_gain,
    tri_in_weight,
    tri_gate_weight,
    tri_out_norm_gain,
    tri_out_weight,
    att_norm_gain,
    att_proj_weight,
    att_bias_weight,
    att_out_weight,
):
    rows_here, cols_here, _ = pair.shape
    residues = cols_here * lax.axis_size(("col", "sub"))
    row_offset = lax.axis_index("row") * rows_here
    col_offset = lax.axis_index(("col", "sub")) * cols_here
    residue_live = residue_mask.astype(jnp.float32)
    live_rows = lax.dynamic_slice_in_dim(residue_live, row_offset, rows_here)
    live_cols = lax.dynamic_slice_in_dim(residue_live, col_offset, cols_here)
    pair_live = (live_rows[:, None] * live_cols[None, :])[:, :, None]
    tri_normed = norm_last(pair, tri_norm_gain).astype(jnp.bfloat16)
    in_width = tri_in_weight.shape[2]
    projected = project(tri_normed, tri_in_weight.reshape(tri_in_weight.shape[0], -1)).reshape(
        rows_here, cols_here, 4, in_width
    )
    left_factor = (jax.nn.sigmoid(projected[:, :, 0]) * projected[:, :, 1] * pair_live).astype(
        jnp.bfloat16
    )
    right_factor = (jax.nn.sigmoid(projected[:, :, 2]) * projected[:, :, 3] * pair_live).astype(
        jnp.bfloat16
    )
    left_all, right_all = (
        lax.all_gather(left_factor, ("col", "sub"), axis=1, tiled=True),
        lax.all_gather(right_factor, ("col", "sub"), axis=1, tiled=True),
    )
    exchanged = lax.all_to_all(right_all, "row", split_axis=1, concat_axis=0, tiled=True)
    own_rows = lax.dynamic_slice_in_dim(exchanged, col_offset, cols_here, 0)
    tri_sum = jnp.einsum(
        "ikh,jkh->ijh",
        left_all,
        lax.all_gather(own_rows, "row", axis=1, tiled=True),
        preferred_element_type=jnp.float32,
    )
    hidden_normed = norm_last(tri_sum, tri_out_norm_gain).astype(jnp.bfloat16)
    tri_gate = jax.nn.sigmoid(project(tri_normed, tri_gate_weight))
    pair_mid = pair + tri_gate * project(hidden_normed, tri_out_weight)
    att_normed = norm_last(pair_mid, att_norm_gain).astype(jnp.bfloat16)
    head_width = att_proj_weight.shape[2]
    heads_here = att_bias_weight.shape[1]
    head_size = head_width // heads_here
    projected = project(att_normed, att_proj_weight.reshape(att_proj_weight.shape[0], -1)).reshape(
        rows_here, cols_here, 4, head_width
    )
    queries = (projected[:, :, 0] * head_size ** (-0.5)).astype(jnp.bfloat16)
    key_rows = projected[:, :, 1].astype(jnp.bfloat16)
    value_rows = projected[:, :, 2].astype(jnp.bfloat16)
    att_gate = jax.nn.sigmoid(projected[:, :, 3])
    pair_bias = project(att_normed, att_bias_weight).astype(jnp.bfloat16)
    key_all, value_all = (
        lax.all_gather(key_rows, ("col", "sub"), axis=1, tiled=True),
        lax.all_gather(value_rows, ("col", "sub"), axis=1, tiled=True),
    )
    bias_all_rows = lax.all_gather(pair_bias, "row", axis=0, tiled=True)
    bias_panel = lax.all_to_all(
        bias_all_rows, ("col", "sub"), split_axis=0, concat_axis=1, tiled=True
    )
    mask_row = (residue_live - 1.0) * mask_penalty
    head_bias = jnp.transpose(bias_panel.astype(jnp.float32), (2, 0, 1)) + mask_row[None, None, :]
    block_rows = math.gcd(rows_here, max(1, 512 // cols_here))
    blocks = rows_here // block_rows

    def attend(block_items):
        query_block, key_block, value_block = block_items
        scores = (
            jnp.einsum(
                "ijhd,ikhd->ihjk", query_block, key_block, preferred_element_type=jnp.float32
            )
            + head_bias[None]
        )
        row_max = jnp.max(scores, axis=-1, keepdims=True)
        raised = jnp.exp(scores - row_max)
        weights = (raised / jnp.sum(raised, axis=-1, keepdims=True)).astype(jnp.bfloat16)
        return jnp.einsum(
            "ihjk,ikhd->ijhd", weights, value_block, preferred_element_type=jnp.float32
        )

    attended = lax.map(
        attend,
        (
            queries.reshape(blocks, block_rows, cols_here, heads_here, head_size),
            key_all.reshape(blocks, block_rows, residues, heads_here, head_size),
            value_all.reshape(blocks, block_rows, residues, heads_here, head_size),
        ),
    )
    gated = (attended.reshape(rows_here, cols_here, head_width) * att_gate).astype(jnp.bfloat16)
    return pair_mid + project(gated, att_out_weight)


def dot_nn(a, b):
    return lax.dot_general(a, b, (((1,), (0,)), ((), ())), preferred_element_type=f32)


def dot_nt(a, b):
    return lax.dot_general(a, b, (((1,), (1,)), ((), ())), preferred_element_type=f32)


kernel_params = pltpu.CompilerParams(vmem_limit_bytes=16 << 20)


def near(v):
    return pltpu.with_memory_space_constraint(v, pltpu.VMEM)


def afar(v):
    return pltpu.with_memory_space_constraint(v, pltpu.HBM)


def split_weight(w_ref, w_scratch):
    rows, mats, out = w_ref.shape
    w_scratch[...] = w_ref[...].astype(f32).reshape(rows * mats, out)
    return [w_scratch[pl.ds(p, rows, stride=mats), :] for p in range(mats)]


def live_lanes(live_ref):
    live = live_ref[...].astype(f32)
    return jnp.concatenate([live, jnp.zeros((1, LANES - live.shape[1]), f32)], axis=1)


def factors_kernel(
    devices,
    pair_ref,
    gain_ref,
    w_ref,
    live_ref,
    lr_ref,
    normed_ref,
    lanes_ref,
    kept_ref,
    w_scratch,
):
    cells, _ = pair_ref.shape
    kept_ref[...] = pair_ref[...]
    lanes_ref[...] = live_lanes(live_ref)
    hidden = w_ref.shape[2]
    own = hidden // devices
    normed = norm_last(pair_ref[...], gain_ref[...]).astype(bf16)
    normed_ref[...] = normed
    w = [w.astype(bf16) for w in split_weight(w_ref, w_scratch)]
    spare = (-cells) % LANES
    tiles = (cells + spare) // LANES
    if spare:
        tail = normed[:spare]
        rows_left = jnp.concatenate([normed, tail], axis=0)
        rows_right = jnp.concatenate([tail, normed], axis=0)
    else:
        rows_left = rows_right = normed
    left = jnp.transpose(sigmoid(dot_nn(rows_left, w[0])) * dot_nn(rows_left, w[1]))
    right = jnp.transpose(sigmoid(dot_nn(rows_right, w[2])) * dot_nn(rows_right, w[3]))
    panels = [left[:, t * LANES : (t + 1) * LANES] for t in range(tiles)]
    right_panels = [right[:, t * LANES : (t + 1) * LANES] for t in range(tiles)]
    if spare:
        lane = lax.broadcasted_iota(jnp.int32, (hidden, LANES), 1)
        panels[-1] = jnp.where(lane < LANES - spare, panels[-1], right_panels[0])
        panels += right_panels[1:]
    else:
        panels += right_panels
    for t, panel in enumerate(panels):
        lr_ref[:, t] = panel.reshape(devices, own, LANES).astype(bf16)


def segment(panels, start, target):
    tile, at = divmod(start, LANES)
    here = panels[tile]
    if at and tile + 1 < len(panels):
        lane = lax.broadcasted_iota(jnp.int32, here.shape, 1)
        here = jnp.where(lane >= at, here, panels[tile + 1])
    shift = (target - at) % LANES
    return pltpu.roll(here, shift, 1) if shift else here


def triangle_kernel(
    rows_here, cols_here, live_ref, lr_ref, sum_ref, left_scratch, right_scratch, sum_scratch
):
    _, panels_in, own, _ = lr_ref.shape
    residues = left_scratch.shape[0] // own
    cols = residues // cols_here
    rows = residues // rows_here
    cells = rows_here * cols_here
    lane = lax.broadcasted_iota(jnp.int32, (own, LANES), 1)
    for r in range(rows):
        parts = [
            [lr_ref[r * cols + c, t].astype(f32) for t in range(panels_in)] for c in range(cols)
        ]
        for side, scratch in ((0, left_scratch), (1, right_scratch)):
            for i in range(rows_here):
                start = side * cells + i * cols_here
                line = segment(parts[0], start, 0)
                for c in range(1, cols):
                    moved = segment(parts[c], start, c * cols_here)
                    line = jnp.where(lane < c * cols_here, line, moved)
                scratch[pl.ds((r * rows_here + i) * own, own), :] = line
    live_wide = live_ref[...]
    live_square = jnp.broadcast_to(live_wide, (LANES, LANES))
    both = live_square * jnp.transpose(live_square)
    both = both[:residues]
    keep = live_wide > 0
    for h in range(own):
        left = jnp.where(keep, left_scratch[pl.ds(h, residues, stride=own), :], 0.0).astype(bf16)
        right = right_scratch[pl.ds(h, residues, stride=own), :].astype(bf16)
        right = jnp.concatenate([right, jnp.zeros((LANES - residues, LANES), bf16)], axis=0)
        sum_scratch[pl.ds(h, residues, stride=own), :] = dot_nt(left, right) * both
    tiles = sum_ref.shape[1]
    for r in range(rows):
        lines = [
            sum_scratch[pl.ds((r * rows_here + i) * own, own), :] for i in range(rows_here)
        ]
        for c in range(cols):
            for t in range(tiles):
                panel = None
                for i in range(rows_here):
                    low, high = i * cols_here - t * LANES, (i + 1) * cols_here - t * LANES
                    if high <= 0 or low >= LANES:
                        continue
                    shift = (low - c * cols_here) % LANES
                    line = pltpu.roll(lines[i], shift, 1) if shift else lines[i]
                    panel = line if panel is None else jnp.where(lane >= low, line, panel)
                sum_ref[r * cols + c, t] = panel.astype(bf16)


def middle_kernel(
    pair_ref,
    normed_ref,
    sum_ref,
    out_gain_ref,
    att_gain_ref,
    out_w_ref,
    gate_w_ref,
    bias_w_ref,
    mid_ref,
    att_ref,
    bias_ref,
):
    devices, tiles, own, _ = sum_ref.shape
    cells, _ = pair_ref.shape
    hidden = devices * own
    gain_col = jnp.transpose(jnp.broadcast_to(out_gain_ref[...], (LANES, hidden)))
    gate = sigmoid(dot_nn(normed_ref[...], gate_w_ref[...]))
    bias_w = bias_w_ref[...]
    hidden_rows = []
    for t in range(tiles):
        total = sum_ref[:, t].astype(f32).reshape(hidden, LANES)
        center = jnp.mean(total, axis=0, keepdims=True)
        centered = total - center
        variance = jnp.mean(centered * centered, axis=0, keepdims=True)
        hidden_normed = centered * lax.rsqrt(variance + epsilon) * gain_col
        hidden_rows.append(jnp.transpose(hidden_normed).astype(bf16))
    hidden_rows = jnp.concatenate(hidden_rows, axis=0)[:cells]
    mid = pair_ref[...] + gate * dot_nn(hidden_rows, out_w_ref[...])
    mid_ref[...] = mid
    att = norm_last(mid, att_gain_ref[...]).astype(bf16)
    att_ref[...] = att
    bias_ref[0] = dot_nt(bias_w, att).astype(bf16)


def own_kernel(heads, att_ref, w_ref, q_ref, k_ref, v_ref, gate_ref, kv_w_ref, w_scratch):
    rows_here, cols_here, chan = att_ref.shape
    width = w_ref.shape[2]
    shape = (rows_here, cols_here, width)
    att = att_ref[...].reshape(rows_here * cols_here, chan)
    w = [m.astype(bf16) for m in split_weight(w_ref, w_scratch)]
    kv_w_ref[0], kv_w_ref[1] = w[1], w[2]
    q_ref[...] = (dot_nn(att, w[0]) * (width // heads) ** (-0.5)).astype(bf16).reshape(shape)
    k_ref[...] = dot_nn(att, w[1]).astype(bf16).reshape(shape)
    v_ref[...] = dot_nn(att, w[2]).astype(bf16).reshape(shape)
    gate_ref[...] = sigmoid(dot_nn(att, w[3])).reshape(shape)


def fetch_plan():
    trips, codes = ([], []), [0] * 16
    for h in range(2):
        for x in range(2):
            for p in range(2):
                for b in range(2):
                    chips = [t for t in range(4) if (t in FIRST[h][x]) == (b == p)]
                    for n, target in enumerate(chips):
                        source_core = n ^ TURNED[2 * h + b][x][p]
                        core = x ^ (target in SWAPPED[h])
                        source = ((2 * h + b) * 2 + source_core) * 2 + x
                        device = (target * 2 + core) * 2 + h
                        trips[p].append((source, device))
                        codes[device] |= (b if p == 0 else 0) | source_core << (1 + p)
                        codes[device] |= (x == h) << 3
    return trips, codes


FIRST = (((0, 1), (0, 2)), ((0, 1), (1, 2)))
SWAPPED = ((1,), (0, 1, 2, 3))
TURNED = (((1, 0), (1, 0)), ((0, 1), (1, 1)), ((1, 0), (0, 0)), ((0, 1), (0, 0)))


def fetch_code(codes, row, col):
    index = row * 2 + col
    code = jnp.int32(0)
    for device, entry in enumerate(codes):
        code = jnp.where(index == device, jnp.int32(entry), code)
    return [jnp.bitwise_and(lax.shift_right_logical(code, jnp.int32(n)), 1) for n in range(4)]


def head_bias_half(ref, scratch, rows_here, cols_here, code, target):
    blocks, heads, cells = ref.shape
    first, *cores, _ = code
    pad = (-cells) % LANES
    for m in range(blocks):
        p, n = m // 2, m % 2
        block = 2 * jnp.bitwise_xor(first, p) + jnp.bitwise_xor(n, cores[p])
        v = ref[m].astype(f32)
        v = jnp.concatenate([v, jnp.zeros((heads, pad), f32)], axis=1) if pad else v
        panels = [v[:, t * LANES : (t + 1) * LANES] for t in range((cells + pad) // LANES)]
        for j in range(rows_here):
            line = segment(panels, j * cols_here, target)
            scratch[pl.ds((block * rows_here + j) * heads, heads), :] = line
    return jnp.concatenate(
        [scratch[pl.ds(h, cols_here, stride=heads), :] for h in range(heads)], axis=0
    )


def scores_kernel(
    codes,
    live_ref,
    fetched_ref,
    q_ref,
    k_ref,
    far_ref,
    v_ref,
    kv_w_ref,
    scores_ref,
    v_all_ref,
    bias_ref,
    bias_scratch,
):
    rows_here, cols_here, width = q_ref.shape
    heads = fetched_ref.shape[1]
    far = far_ref[...].reshape(rows_here * cols_here, width)
    k_far = dot_nn(far, kv_w_ref[0]).astype(bf16).reshape(q_ref.shape)
    v_far = dot_nn(far, kv_w_ref[1]).astype(bf16).reshape(q_ref.shape)
    row, col = lax.axis_index("row"), lax.axis_index(("col", "sub"))
    code = fetch_code(codes, row, col)
    own_first = code[3] == 1

    def in_order(own, other):
        return jnp.concatenate(
            [jnp.where(own_first, own, other), jnp.where(own_first, other, own)], axis=0
        )

    head_of = lax.broadcasted_iota(jnp.int32, (cols_here, width), 1) // (width // heads)
    for i in range(rows_here):
        q = q_ref[i]
        q_heads = jnp.concatenate(
            [jnp.where(head_of == h, q, jnp.zeros_like(q)) for h in range(heads)], axis=0
        )
        scores_ref[i] = dot_nt(q_heads, in_order(k_ref[i], k_far[i]))
        v_all_ref[i] = in_order(v_ref[i], v_far[i])
    lane_row = lax.broadcasted_iota(jnp.int32, (1, LANES), 1)
    live = live_ref[...]
    swapped = jnp.where(
        lane_row < cols_here,
        pltpu.roll(live, LANES - cols_here, 1),
        pltpu.roll(live, cols_here, 1),
    )
    natural = (col == 0) == own_first
    penalty = (jnp.where(natural, live, swapped) - 1.0) * mask_penalty
    half = head_bias_half(fetched_ref, bias_scratch, rows_here, cols_here, code, 0)
    bias_ref[...] = jnp.where(lane_row < cols_here, half, 0.0) + penalty


def attention_kernel(
    codes,
    bias_ref,
    swapped_ref,
    scores_ref,
    v_all_ref,
    gate_ref,
    mid_ref,
    out_w_ref,
    out_ref,
    bias_scratch,
    result,
    done,
):
    rows_here, cols_here, width = gate_ref.shape
    chunks = done.shape[0]
    heads = swapped_ref.shape[1]
    residues = 2 * cols_here
    row, col = lax.axis_index("row"), lax.axis_index(("col", "sub"))
    code = fetch_code(codes, jnp.bitwise_xor(row, 1), col)
    half = head_bias_half(swapped_ref, bias_scratch, rows_here, cols_here, code, cols_here)
    lane_row = lax.broadcasted_iota(jnp.int32, (1, LANES), 1)
    head_bias = (bias_ref[...] + jnp.where(lane_row < cols_here, 0.0, half))[:, :residues]
    head_of = lax.broadcasted_iota(jnp.int32, (cols_here, width), 1) // (width // heads)
    ones = jnp.ones((residues, width), bf16)
    chunk = rows_here // chunks
    copies = []
    for c in range(chunks):
        gated = []
        for i in range(c * chunk, (c + 1) * chunk):
            scores = scores_ref[i] + head_bias
            raised = jnp.exp(scores - jnp.max(scores, axis=-1, keepdims=True)).astype(bf16)
            mixed = dot_nn(raised, jnp.concatenate([v_all_ref[i], ones], axis=1))
            attended = mixed[:cols_here]
            for h in range(1, heads):
                part = mixed[h * cols_here : (h + 1) * cols_here]
                attended = jnp.where(jnp.tile(head_of, (1, 2)) == h, part, attended)
            attended = attended[:, :width] / attended[:, width:]
            gated.append((attended * gate_ref[i]).astype(bf16))
        update = dot_nn(jnp.concatenate(gated, axis=0), out_w_ref[...])
        at = slice(c * chunk, (c + 1) * chunk)
        result[at] = mid_ref[at] + update.reshape(chunk, cols_here, width)
        copies.append(pltpu.make_async_copy(result.at[at], out_ref.at[at], done.at[c]))
        copies[-1].start()
    for copy in copies:
        copy.wait()


def body_channels(
    pair,
    residue_mask,
    tri_norm_gain,
    tri_in_weight,
    tri_gate_weight,
    tri_out_norm_gain,
    tri_out_weight,
    att_norm_gain,
    att_proj_weight,
    att_bias_weight,
    att_out_weight,
):
    rows_here, cols_here, chan = pair.shape
    rows, cols = lax.axis_size("row"), lax.axis_size(("col", "sub"))
    group = ("row", "col", "sub")
    devices = rows * cols
    residues = cols_here * cols
    cells = rows_here * cols_here
    hidden = tri_in_weight.shape[2]
    own = hidden // devices
    heads = att_bias_weight.shape[1]
    tiles = -(-cells // LANES)
    lr_panels = -(-2 * cells // LANES) if (-cells) % LANES * 2 == LANES else 2 * tiles
    flat = pair.reshape(cells, chan)
    live = residue_mask.reshape(1, residues)

    lr, normed, lanes, kept = pl.pallas_call(
        functools.partial(factors_kernel, devices),
        out_shape=(
            pltpu.VMEM((devices, lr_panels, own, LANES), bf16),
            pltpu.VMEM((cells, chan), bf16),
            pltpu.VMEM((1, LANES), f32),
            pltpu.VMEM((cells, chan), f32),
        ),
        scratch_shapes=[pltpu.VMEM((chan * tri_in_weight.shape[1], hidden), f32)],
        compiler_params=kernel_params,
        name="factors",
    )(
        *map(
            afar,
            (
                flat,
                tri_norm_gain.reshape(1, chan),
                tri_in_weight,
                live,
            ),
        )
    )
    lr = lax.all_to_all(lr, group, 0, 0, tiled=True)
    sums = pl.pallas_call(
        functools.partial(triangle_kernel, rows_here, cols_here),
        out_shape=pltpu.VMEM((devices, tiles, own, LANES), bf16),
        scratch_shapes=[pltpu.VMEM((residues * own, LANES), f32) for _ in range(3)],
        compiler_params=kernel_params,
        name="triangle",
    )(near(lanes), near(lr))
    sums = lax.all_to_all(sums, group, 0, 0, tiled=True)
    shape = (rows_here, cols_here, chan)
    chunks = math.gcd(rows_here, 2)
    mid, att, bias = pl.pallas_call(
        middle_kernel,
        out_shape=(
            pltpu.VMEM((cells, chan), f32),
            pltpu.VMEM((cells, chan), bf16),
            pltpu.VMEM((1, heads, cells), bf16),
        ),
        compiler_params=kernel_params,
        name="middle",
    )(
        *map(
            near,
            (
                kept,
                normed,
                sums,
                tri_out_norm_gain.reshape(1, hidden),
                att_norm_gain.reshape(1, chan),
                tri_out_weight,
                tri_gate_weight,
                att_bias_weight.T,
            ),
        )
    )
    att, mid = att.reshape(shape), mid.reshape(shape)

    def swap(v):
        return lax.ppermute(v, "row", [(r, r ^ 1) for r in range(rows)])

    trips, codes = fetch_plan()
    joined = swap(bias)
    bias = jnp.concatenate([bias, joined], axis=0)
    fetched = []
    for p in range(2):
        fetched.append(lax.ppermute(bias, group, trips[p]))
    far = lax.ppermute(att, ("col", "sub"), [(c, c ^ 1) for c in range(cols)])
    queries, keys, values, gate, kv_weight = pl.pallas_call(
        functools.partial(own_kernel, heads),
        out_shape=(
            pltpu.VMEM(shape, bf16),
            pltpu.VMEM(shape, bf16),
            pltpu.VMEM(shape, bf16),
            pltpu.VMEM(shape, f32),
            pltpu.VMEM((2, chan, chan), bf16),
        ),
        scratch_shapes=[pltpu.VMEM((chan * att_proj_weight.shape[1], chan), f32)],
        compiler_params=kernel_params,
        name="own",
    )(near(att), near(att_proj_weight))
    fetched = jnp.concatenate(fetched, axis=0)
    swapped = swap(fetched)
    scores, values, bias = pl.pallas_call(
        functools.partial(scores_kernel, codes),
        out_shape=(
            pltpu.VMEM((rows_here, heads * cols_here, residues), f32),
            pltpu.VMEM((rows_here, residues, chan), bf16),
            pltpu.VMEM((heads * cols_here, LANES), f32),
        ),
        scratch_shapes=[pltpu.VMEM((cols_here * heads, LANES), f32)],
        compiler_params=kernel_params,
        name="scores",
    )(*map(near, (lanes, fetched, queries, keys, far, values, kv_weight)))
    return pl.pallas_call(
        functools.partial(attention_kernel, codes),
        out_shape=jax.ShapeDtypeStruct(shape, f32),
        out_specs=pl.BlockSpec(memory_space=pltpu.HBM),
        scratch_shapes=[
            pltpu.VMEM((cols_here * heads, LANES), f32),
            pltpu.VMEM(shape, f32),
            pltpu.SemaphoreType.DMA((chunks,)),
        ],
        compiler_params=kernel_params,
        name="attention",
    )(*map(near, (bias, swapped, scores, values, gate, mid, att_out_weight)))


def solution(mesh):
    placed = (
        P(("parts", "row"), ("col", "sub"), None),
        P("parts"),
        P(),
        P(),
        P(),
        P(),
        P(),
        P(),
        P(),
        P(),
        P(),
    )

    def body(pair, residue_mask, tri_norm_gain, tri_in_weight, *others):
        rows, cols = mesh.shape["row"], mesh.shape["col"] * mesh.shape["sub"]
        hidden = tri_in_weight.shape[2]
        fits = (
            cols == 2
            and rows == 8
            and hidden % (8 * rows * cols) == 0
            and hidden == pair.shape[2] == LANES
            and residue_mask.shape[0] <= LANES
            and pair.shape[0] * cols * pair.shape[1] % 16 == 0
        )
        chosen = body_channels if fits else body_general
        return chosen(pair, residue_mask, tri_norm_gain, tri_in_weight, *others)

    return jax.shard_map(
        body,
        mesh=mesh,
        in_specs=placed,
        out_specs=P(("parts", "row"), ("col", "sub"), None),
        check_vma=False,
    )
```
